128 devices in a mesh: tok: 8 (over y, z_lo), hid: 16 (over z_hi, x, core).
Axes of the slice: x: 4, y: 4, z: 4 (z_hi: 2, z_lo: 2; z = z_hi * 2 + z_lo), core: 2. Of those that a mesh axis runs over, the one named last changes fastest.
Arguments:
- tokens: bfloat16 [12288, 6144], P('tok', 'hid'), may hold values from -6 to 6
- cotangent: bfloat16 [12288, 6144], P('tok', 'hid'), may hold values from -6 to 6
- expert_choice: int32 [12288, 2], P('tok'), may hold values from 0 to 7, as said below
- router: bfloat16 [8, 6144], replicated, may hold values from -0.078125 to 0.078125
- gate_up: bfloat16 [6144, 2, 8192], P('tok', None, 'hid'), may hold values from -0.109375 to 0.109375
- w_down: bfloat16 [6144, 8192], P('tok', 'hid'), may hold values from -0.0625 to 0.0625
Outputs:
- grad_tokens: bfloat16 [12288, 6144], P('tok', 'hid')
- d_combine: float32 [12288, 2], P('tok')
- d_gate_up: float32 [6144, 2, 8192], P('tok', None, 'hid')
- d_down: float32 [6144, 8192], P('tok', 'hid')
The draws below stay inside these ranges and needn't reach their ends.
Inputs may be any that keep to these rules, and one draw needn't show every extreme that they name: `expert_choice`: each row names 2 different experts. In every aligned block of 1536 rows at most 432 rows name expert 0 and at least half of 432 do; some block has exactly 432.
All inputs are finite; a program needn't handle non-finite values.
Results may differ from the reference program's by a relative error of at most 0.017.
Values may be sent and summed in bfloat16 or wider, within the bound.
A program may use at most 128 MiB of HBM per device.

```python
import jax
import jax.numpy as jnp
from jax import lax

D = 6144
FF = 8192
EXPERTS = 8
TOK_GROUP = 1536
CAP = 432
TOKENS = 12288
N_TOK = 8


def draw_expert_choice(key, part):
    streams = jax.random.split(jax.random.fold_in(key, 17), 6)
    blocks = TOKENS // TOK_GROUP
    counts = jax.random.randint(streams[0], (blocks,), CAP // 2, CAP + 1)
    fullest = jax.random.randint(streams[1], (), 0, blocks)
    counts = jnp.where(jnp.arange(blocks) == fullest, CAP, counts)
    orders = jax.vmap(lambda block_key: jax.random.permutation(block_key, TOK_GROUP))(jax.random.split(streams[2], blocks))
    chosen = (orders < counts[:, None]).reshape(TOKENS)
    leading = jax.random.randint(streams[3], (TOKENS,), 1, EXPERTS)
    offset = jax.random.randint(streams[4], (TOKENS,), 1, EXPERTS - 1)
    trailing = 1 + (leading - 1 + offset) % (EXPERTS - 1)
    column = jax.random.randint(streams[5], (TOKENS,), 0, 2)
    left_entry = jnp.where(chosen, jnp.where(column == 0, 0, leading), leading)
    right_entry = jnp.where(chosen, jnp.where(column == 0, leading, 0), trailing)
    return jnp.stack([left_entry, right_entry], axis=1).astype(jnp.int32)


def raised(result, key, source, target, shards_of, factor):
    owner, partner = [(jnp.arange(result.shape[position]) // (result.shape[position] // shards_of)).reshape([-1 if axis == position else 1 for axis in range(result.ndim)]) for position in (source, target)]
    chosen = jax.random.permutation(key, shards_of)[partner]
    strong = (owner == chosen) | (owner == (partner + shards_of // 2) % shards_of)
    return jnp.where(strong, factor * result, result)


def levels(rng, dims, pieces, low, high):
    def one(axis_at, blocks):
        steps = jax.random.uniform(jax.random.fold_in(jax.random.fold_in(rng, 6), axis_at), (blocks,), jnp.float32, low / len(pieces), high / len(pieces))
        return jnp.repeat(jnp.exp(steps), dims[axis_at] // blocks).reshape((-1,) + (1,) * (len(dims) - axis_at - 1))

    gain = one(*pieces[0])
    for cut in pieces[1:]:
        gain = gain * one(*cut)
    return gain


def normal_values(key, shape, width, bound, cuts=(), kind=jnp.bfloat16):
    entries = width * jax.random.normal(key, shape, jnp.float32)
    if cuts:
        entries = entries * levels(key, shape, cuts, -0.22, 0.18)
    return jnp.clip(entries, -bound, bound).astype(kind)


def noise_with(rng, shape, deviation, bound, cuts, heavy, kind=jnp.bfloat16):
    drawn = deviation * jax.random.normal(rng, shape, jnp.float32)
    if cuts:
        drawn = drawn * levels(rng, shape, cuts, -0.22, 0.18)
    return jnp.clip(raised(drawn, jax.random.fold_in(rng, 3), *heavy), -bound, bound).astype(kind)


def setup_inputs(seed: int = 0) -> dict:
    seeds = jax.random.split(jax.random.key(seed), 7)
    tokens = noise_with(seeds[0], (TOKENS, D), 1.0, 6.0, ((0, 8), (1, 16)), (0, 1, 16, 2.0))
    cotangent = noise_with(seeds[1], (TOKENS, D), 1.0, 6.0, ((0, 8), (1, 16)), (0, 1, 16, 2.0))
    expert_choice = draw_expert_choice(jax.random.fold_in(seeds[6], 71), 0)
    router = normal_values(seeds[3], (EXPERTS, D), D ** -0.5, 0.078125)
    gate_up = noise_with(seeds[4], (D, 2, FF), D ** -0.5, 0.109375, ((0, 8), (2, 16)), (2, 0, 16, 2.0))
    w_down = normal_values(seeds[5], (D, FF), FF ** -0.5, 0.0625, ((0, 8), (1, 16)))
    return dict(tokens=tokens, cotangent=cotangent, expert_choice=expert_choice, router=router, gate_up=gate_up, w_down=w_down)


def silu_pair(pre):
    sigma = jax.nn.sigmoid(pre)
    return pre * sigma, sigma * (1.0 + pre * (1.0 - sigma))


def rounded_add(total, term):
    return total + lax.optimization_barrier(term.astype(jnp.bfloat16)).astype(jnp.float32)


def reference(tokens, cotangent, expert_choice, router, gate_up, w_down):
    logits = jnp.dot(tokens, router.T, preferred_element_type=jnp.float32)
    first = expert_choice[:, 0]
    second = expert_choice[:, 1]
    in_first = first == 0
    in_second = second == 0
    routed = jnp.logical_or(in_first, in_second)
    other = first + second
    labels = jnp.arange(EXPERTS, dtype=jnp.int32)
    other_logit = jnp.sum(jnp.where(other[:, None] == labels[None, :], logits, 0.0), axis=1)
    gating = jnp.where(routed, jax.nn.sigmoid(logits[:, 0] - other_logit), 0.0)
    flags = routed.astype(jnp.int32).reshape(N_TOK, TOK_GROUP)
    slot_rank = jnp.cumsum(flags, axis=1) - flags
    slot_ids = jnp.arange(CAP, dtype=jnp.int32)
    placed = jnp.logical_and(flags[:, None, :] > 0, slot_rank[:, None, :] == slot_ids[None, :, None])
    dispatch = placed.astype(jnp.float32)
    grouped_in = tokens.astype(jnp.float32).reshape(N_TOK, TOK_GROUP, D)
    grouped_cot = cotangent.astype(jnp.float32).reshape(N_TOK, TOK_GROUP, D)
    expert_in = jnp.einsum("kcr,krd->kcd", dispatch, grouped_in, precision=lax.Precision.HIGHEST).astype(jnp.bfloat16)
    expert_cot = jnp.einsum("kcr,krd->kcd", dispatch, grouped_cot, precision=lax.Precision.HIGHEST).astype(jnp.bfloat16)
    slot_gate = jnp.sum(dispatch * gating.reshape(N_TOK, 1, TOK_GROUP), axis=2)
    weights_in = gate_up.reshape(D, 2 * FF)
    grad_in = jnp.zeros((D, 2 * FF), jnp.float32)
    grad_out = jnp.zeros((D, FF), jnp.float32)
    back_rows = []
    score_rows = []
    for group in range(N_TOK):
        rows_in = expert_in[group]
        rows_cot = expert_cot[group]
        scale = slot_gate[group][:, None]
        joined = jnp.dot(rows_in, weights_in, preferred_element_type=jnp.float32)
        gate_pre = joined[:, :FF]
        up_pre = joined[:, FF:]
        raw = jnp.dot(rows_cot, w_down, preferred_element_type=jnp.float32)
        active, slope = silu_pair(gate_pre)
        product = active * up_pre
        scaled = (scale * product).astype(jnp.bfloat16)
        score_rows.append(jnp.sum(product * raw, axis=1))
        upstream = scale * raw
        grads_mid = jnp.concatenate([(upstream * up_pre * slope).astype(jnp.bfloat16), (upstream * active).astype(jnp.bfloat16)], axis=1)
        grad_in = rounded_add(grad_in, jnp.dot(rows_in.T, grads_mid, preferred_element_type=jnp.float32))
        grad_out = rounded_add(grad_out, jnp.dot(rows_cot.T, scaled, preferred_element_type=jnp.float32))
        back_rows.append(jnp.dot(grads_mid, weights_in.T, preferred_element_type=jnp.float32))
    back = jnp.stack(back_rows)
    scores = jnp.stack(score_rows)
    safe = jnp.minimum(slot_rank, CAP - 1).astype(jnp.int32)
    picked = jax.vmap(lambda rows, index: jnp.take(rows, index, axis=0))(back, safe).reshape(TOKENS, D)
    routed_flat = flags.reshape(TOKENS) > 0
    grad_tokens = jnp.where(routed_flat[:, None], picked, 0.0).astype(jnp.bfloat16)
    picked_score = jax.vmap(lambda rows, index: jnp.take(rows, index, axis=0))(scores, safe).reshape(TOKENS)
    token_score = jnp.where(routed, picked_score, 0.0)
    d_combine = jnp.stack([jnp.where(in_first, token_score, 0.0), jnp.where(in_second, token_score, 0.0)], axis=1)
    return grad_tokens, d_combine, grad_in.reshape(D, 2, FF), grad_out
```

```python
import jax
import jax.numpy as jnp
from jax import lax
from jax.sharding import Mesh
from jax.sharding import PartitionSpec as P

CAP = 432
TOK = ("y", "zl")
ALL = ("y", "zl", "hid")


def swap_pairs():
    pairs = []
    for y in range(4):
        for zl in range(2):
            for h in range(16):
                to_y, to_h = h // 4, y * 4 + h % 4
                pairs.append(((y * 2 + zl) * 16 + h, (to_y * 2 + zl) * 16 + to_h))
    return pairs


def silu_pair(pre):
    sigma = jax.nn.sigmoid(pre)
    return (pre * sigma, sigma * (1.0 + pre * (1.0 - sigma)))


def dot_f32(left, right, dims):
    return lax.dot_general(left, right, ((dims[0], dims[1]), ((), ())), preferred_element_type=jnp.float32)


def local(tokens, cotangent, expert_choice, router, gate_up, w_down):
    cols = tokens.shape[1]
    rows_own, hid = w_down.shape
    zl = lax.axis_index("zl")
    first = expert_choice[:, 0]
    second = expert_choice[:, 1]
    in_first = first == 0
    in_second = second == 0
    routed = jnp.logical_or(in_first, in_second)
    flags = routed.astype(jnp.int32)
    slot_rank = jnp.cumsum(flags) - flags
    slot_ids = jnp.arange(CAP, dtype=jnp.int32)
    placed = jnp.logical_and(routed[None, :], slot_rank[None, :] == slot_ids[:, None])
    select = placed.astype(jnp.bfloat16)

    weights = jnp.concatenate([gate_up.reshape(rows_own, 2 * hid), w_down], axis=1)
    other_weights = lax.ppermute(weights, "zl", [(0, 1), (1, 0)])

    dispatched = dot_f32(select, jnp.concatenate([tokens, cotangent], axis=1), ((1,), (0,)))
    moved = lax.ppermute(dispatched.astype(jnp.bfloat16), ALL, swap_pairs())
    gathered = lax.all_gather(moved, "hid", axis=0)

    router_cols = lax.dynamic_slice_in_dim(router, lax.axis_index("hid") * cols, cols, 1)
    logits = dot_f32(tokens, router_cols, ((1,), (1,)))
    other = first + second
    labels = jnp.arange(logits.shape[1], dtype=jnp.int32)
    other_logit = jnp.sum(jnp.where(other[:, None] == labels[None, :], logits, 0.0), axis=1)
    margin_part = jnp.sum(jnp.where(placed, (logits[:, 0] - other_logit)[None, :], 0.0), axis=1)
    margin = lax.psum(margin_part, "hid")
    filled = jnp.any(placed, axis=1)
    slot_gate = jnp.where(filled, jax.nn.sigmoid(margin), 0.0)

    parts = gathered.reshape(4, 4, CAP, 2, cols).transpose(3, 0, 2, 1, 4)
    parts = parts.reshape(2, 4 * CAP, 4 * cols)
    rows_in, rows_cot = parts[0], parts[1]

    low = jnp.where(zl == 0, weights, other_weights)
    high = jnp.where(zl == 0, other_weights, weights)
    both = jnp.concatenate([low, high], axis=0)
    w_gu = both[:, : 2 * hid]
    w_d = both[:, 2 * hid :]

    pre = jnp.concatenate(
        [
            dot_f32(rows_in, w_gu, ((1,), (0,))).astype(jnp.bfloat16),
            dot_f32(rows_cot, w_d, ((1,), (0,))).astype(jnp.bfloat16),
        ],
        axis=1,
    )
    pre = lax.psum_scatter(pre, "y", scatter_dimension=0, tiled=True).astype(jnp.float32)
    gate_pre, up_pre, raw = pre[:, :hid], pre[:, hid : 2 * hid], pre[:, 2 * hid :]
    active, slope = silu_pair(gate_pre)
    product = active * up_pre
    scale = slot_gate[:, None]
    score_part = jnp.sum(product * raw, axis=1)
    upstream = scale * raw
    mids = jnp.concatenate(
        [
            (upstream * up_pre * slope).astype(jnp.bfloat16),
            (upstream * active).astype(jnp.bfloat16),
            (scale * product).astype(jnp.bfloat16),
        ],
        axis=1,
    )
    mids = lax.all_gather(mids, "y", axis=0, tiled=True)
    mid_gu, mid_d = mids[:, : 2 * hid], mids[:, 2 * hid :]
    scores = lax.psum(score_part, "hid")

    back = dot_f32(mid_gu, w_gu, ((1,), (1,))).astype(jnp.bfloat16)
    back = back.reshape(4, CAP, 4, cols).transpose(0, 2, 1, 3).reshape(16, CAP, cols)
    back = lax.psum_scatter(back, "hid", scatter_dimension=0, tiled=False)

    def grads_of(rows):
        return jnp.concatenate(
            [
                dot_f32(lax.dynamic_slice_in_dim(rows_in, rows, rows_own, 1), mid_gu, ((0,), (0,))),
                dot_f32(lax.dynamic_slice_in_dim(rows_cot, rows, rows_own, 1), mid_d, ((0,), (0,))),
            ],
            axis=1,
        )

    sent = grads_of((1 - zl) * rows_own).astype(jnp.bfloat16)
    arrived = lax.ppermute(sent, "zl", [(0, 1), (1, 0)])
    grads = grads_of(zl * rows_own) + arrived.astype(jnp.float32)

    back = lax.ppermute(back, ALL, swap_pairs())
    grad_tokens = dot_f32(select, back, ((0,), (0,))).astype(jnp.bfloat16)
    token_score = jnp.sum(jnp.where(placed, scores[:, None], 0.0), axis=0)
    d_combine = jnp.stack(
        [jnp.where(in_first, token_score, 0.0), jnp.where(in_second, token_score, 0.0)], axis=1
    )
    d_gate_up = grads[:, : 2 * hid].reshape(rows_own, 2, hid)
    d_down = grads[:, 2 * hid :]
    return (grad_tokens, d_combine, d_gate_up, d_down)


def solution(mesh):
    split = Mesh(mesh.devices.reshape(4, 2, mesh.shape["hid"]), ("y", "zl", "hid"))
    return jax.shard_map(
        local,
        mesh=split,
        in_specs=(
            P(TOK, "hid"),
            P(TOK, "hid"),
            P(TOK, None),
            P(),
            P(TOK, None, "hid"),
            P(TOK, "hid"),
        ),
        out_specs=(P(TOK, "hid"), P(TOK, None), P(TOK, None, "hid"), P(TOK, "hid")),
        check_vma=False,
    )
```

```python
import functools

import jax
import jax.numpy as jnp
from jax import lax
from jax.experimental import pallas as pl
from jax.experimental.pallas import tpu as pltpu
from jax.sharding import Mesh
from jax.sharding import PartitionSpec as P

CAP = 432
SUB = 384
PART = 128
TOK = ("y", "zl")
HID = ("zh", "x", "c")
ALL = TOK + HID
MESH = pl.DeviceIdType.MESH
F32 = jnp.float32
BF16 = jnp.bfloat16


def swap_pairs():
    pairs = []
    for y in range(4):
        for zl in range(2):
            for h in range(16):
                to_y, to_h = h // 4, y * 4 + h % 4
                pairs.append(((y * 2 + zl) * 16 + h, (to_y * 2 + zl) * 16 + to_h))
    return pairs


def dot_f32(left, right, dims):
    return lax.dot_general(left, right, ((dims[0], dims[1]), ((), ())), preferred_element_type=F32)


def kernel(
    xin, win, router, other,
    back_out, score_out, dgu_out, dd_out,
    rows, wgt, psend, pown, prelay, precv, lsend, lrecv, gate, sacc, mids,
    gsend, grecv, bsend, bown, brecv, xrelay, xrecv, zsend, zrecv, srow, srecv,
    ssem, rsem,
):
    y, zl, zh, x, c = (lax.axis_index(a) for a in ALL)
    yr, yl, yo = (y + 1) % 4, (y + 3) % 4, (y + 2) % 4
    xr, xl, xo = (x + 1) % 4, (x + 3) % 4, (x + 2) % 4
    D = rows.shape[2]
    own = D // 2

    number = {}
    started = []

    def copy(key, src, dst, **to):
        i = number.setdefault(key, len(number))
        return pltpu.make_async_remote_copy(
            src_ref=src, dst_ref=dst, send_sem=ssem.at[i], recv_sem=rsem.at[i],
            device_id=to, device_id_type=MESH,
        )

    def start(cp):
        cp.start()
        started.append(cp)
        return cp

    barrier = pltpu.get_barrier_semaphore()
    peers = (
        dict(y=yr), dict(y=yl), dict(y=yo), dict(zl=1 - zl), dict(zh=1 - zh),
        dict(x=xr), dict(x=xl), dict(x=xo), dict(c=1 - c),
    )
    for peer in peers:
        pl.semaphore_signal(barrier, inc=1, device_id=peer, device_id_type=MESH)
    pl.semaphore_wait(barrier, len(peers))

    def place(zh_, x_, c_):
        row = pl.multiple_of((2 * zh_ + x_ // 2) * CAP, 16)
        col = pl.multiple_of((2 * (x_ % 2) + c_) * SUB, 128)
        return rows.at[:, pl.ds(row, CAP), pl.ds(col, SUB)]

    def weights(sub, zl_):
        return wgt.at[sub, pl.ds(pl.multiple_of(zl_ * own, 16), own), :]

    here = place(zh, x, c)
    to_zh = start(copy("zh", xin, here, zh=1 - zh))
    from_l0 = start(copy("xr0", xin, here, x=xr))
    from_r0 = start(copy("xl0", xin, here, x=xl))
    cores = [start(copy("c0", xin, here, c=1 - c))]
    for sub in range(4):
        start(copy(("w", sub), win.at[sub], weights(sub, zl), zl=1 - zl))
    here[...] = xin[...]

    def put_weights(i, carry):
        for sub in range(4):
            at = pl.multiple_of(zl * own + i * 96, 16)
            wgt[sub, pl.ds(at, 96), :] = win[sub, pl.ds(pl.multiple_of(i * 96, 16), 96), :]
        return carry

    lax.fori_loop(0, own // 96, put_weights, 0)

    to_zh.wait_recv()
    there = place(1 - zh, x, c)
    from_l1 = start(copy("xr1", there, there, x=xr))
    from_r1 = start(copy("xl1", there, there, x=xl))
    cores.append(start(copy("c1", there, there, c=1 - c)))

    from_l0.wait_recv()
    at = place(zh, xl, c)
    from_lo = start(copy("xro", at, at, x=xr))
    cores.append(start(copy("c2", at, at, c=1 - c)))
    from_r0.wait_recv()
    at = place(zh, xr, c)
    cores.append(start(copy("c3", at, at, c=1 - c)))
    from_r1.wait_recv()
    at = place(1 - zh, xr, c)
    from_ro = start(copy("xlo", at, at, x=xl))
    cores.append(start(copy("c4", at, at, c=1 - c)))
    from_l1.wait_recv()
    at = place(1 - zh, xl, c)
    cores.append(start(copy("c5", at, at, c=1 - c)))
    from_lo.wait_recv()
    at = place(zh, xo, c)
    cores.append(start(copy("c6", at, at, c=1 - c)))
    from_ro.wait_recv()
    at = place(1 - zh, xo, c)
    cores.append(start(copy("c7", at, at, c=1 - c)))
    for cp in cores:
        cp.wait_recv()

    def block_of(ref, which, t):
        return ref[which, pl.ds(pl.multiple_of(t * CAP, 16), CAP), :]

    def rs(key, j):
        kind, half = key
        side = {
            "far_r": lambda: (psend.at[j, 0, half], prelay.at[j, 0], yr),
            "far_l": lambda: (psend.at[j, 0, half], prelay.at[j, 1], yl),
            "near_r": lambda: (psend.at[j, 1, half], precv.at[j, 0, half], yr),
            "near_l": lambda: (psend.at[j, 2, half], precv.at[j, 1, half], yl),
        }[kind]
        src, dst, to = side()
        return copy(("rs", key, j), src, dst, y=to)

    def logit(r):
        to = (yo, yr, yl)[r]
        return copy(("lg", r), lsend.at[r], lrecv.at[r], y=to)

    def pre_of(j):
        def one(r, carry):
            t = (y + jnp.where(r == 0, 2, jnp.where(r == 1, 1, jnp.where(r == 2, 3, 0)))) % 4
            x_in = block_of(rows, 0, t)
            x_cot = block_of(rows, 1, t)
            g0 = dot_f32(x_in, wgt[2 * j, :, : 2 * PART], ((1,), (0,)))
            g1 = dot_f32(x_in, wgt[2 * j + 1, :, : 2 * PART], ((1,), (0,)))
            w_d = jnp.concatenate([wgt[2 * j, :, 2 * PART :], wgt[2 * j + 1, :, 2 * PART :]], axis=1)
            d = dot_f32(x_cot, w_d, ((1,), (0,)))

            @pl.when(r < 3)
            def _():
                psend[j, r, 0, :, : 2 * PART] = g0.astype(BF16)
                psend[j, r, 1, :, : 2 * PART] = g1.astype(BF16)
                psend[j, r, 0, :, 2 * PART :] = d[:, :PART].astype(BF16)
                psend[j, r, 1, :, 2 * PART :] = d[:, PART:].astype(BF16)

            @pl.when(r == 3)
            def _():
                pown[j, 0, :, : 2 * PART] = g0
                pown[j, 1, :, : 2 * PART] = g1
                pown[j, 0, :, 2 * PART :] = d[:, :PART]
                pown[j, 1, :, 2 * PART :] = d[:, PART:]

            if j == 0:
                lsend[r, :, :CAP] = dot_f32(router[...], x_in, ((1,), (1,)))

            @pl.when(r == 0)
            def _():
                rs(("far_r", 0), j).start()
                rs(("far_l", 1), j).start()
                if j == 0:
                    logit(0).start()

            @pl.when(r == 1)
            def _():
                rs(("near_r", 1), j).start()
                if j == 0:
                    logit(1).start()

            @pl.when(r == 2)
            def _():
                rs(("near_l", 0), j).start()
                if j == 0:
                    logit(2).start()

            return carry

        lax.fori_loop(0, 4, one, 0)
        for key in (("far_r", 0), ("far_l", 1), ("near_r", 1), ("near_l", 0)):
            started.append(rs(key, j))
        if j == 0:
            for r in range(3):
                started.append(logit(r))

    def add_relays(j):
        for side, slot, half, kind in ((0, 1, 0, "far_r"), (1, 2, 1, "far_l")):
            rs((kind, half), j).wait_recv()

            def add(i, carry):
                at = pl.ds(pl.multiple_of(i * 144, 16), 144)
                total = psend[j, slot, half, at, :].astype(F32) + prelay[j, side, at, :].astype(F32)
                psend[j, slot, half, at, :] = total.astype(BF16)
                return carry

            lax.fori_loop(0, 3, add, 0)
            start(rs(("near_r" if side == 0 else "near_l", half), j))

    def gates():
        for r in range(3):
            logit(r).wait_recv()
        logits = (lsend[3] + lrecv[0]) + (lrecv[1] + lrecv[2])
        experts = lax.broadcasted_iota(jnp.int32, (8, 512), 0)
        picked = jnp.sum(jnp.where(other[...] == experts, logits[:8], 0.0), axis=0, keepdims=True)
        margin = logits[:1] - picked
        row = jnp.where(other[:1] >= 0, jax.nn.sigmoid(margin), 0.0)
        gate[...] = jnp.transpose(jnp.broadcast_to(row, (PART, 512)))
        sacc[...] = jnp.zeros_like(sacc)

    def gather(key, j):
        kind, half = key
        sub = 2 * j + half
        t, to = {"own_r": (y, yr), "own_l": (y, yl), "fwd_r": (yl, yr), "fwd_l": (yr, yl)}[kind]
        at = mids.at[sub, pl.ds(pl.multiple_of(t * CAP, 16), CAP), :]
        return copy(("ag", key, j), at, at, y=to)

    def pointwise(j):
        for half in range(2):
            for kind in ("near_r", "near_l"):
                rs((kind, half), j).wait_recv()
        for half in range(2):
            sub = 2 * j + half

            def one(i, carry):
                at = pl.ds(pl.multiple_of(i * 48, 16), 48)
                pre = pown[j, half, at, :] + (
                    precv[j, 0, half, at, :].astype(F32) + precv[j, 1, half, at, :].astype(F32)
                )
                g, up, raw = pre[:, :PART], pre[:, PART : 2 * PART], pre[:, 2 * PART :]
                sigma = jax.nn.sigmoid(g)
                active = g * sigma
                slope = sigma * (1.0 + g * (1.0 - sigma))
                product = active * up
                scale = gate[at, :]
                sacc[at, :] += product * raw
                upstream = scale * raw
                to = pl.ds(pl.multiple_of(y * CAP + i * 48, 16), 48)
                mids[sub, to, :PART] = (upstream * up * slope).astype(BF16)
                mids[sub, to, PART : 2 * PART] = (upstream * active).astype(BF16)
                mids[sub, to, 2 * PART :] = (scale * product).astype(BF16)
                return carry

            lax.fori_loop(0, CAP // 48, one, 0)
            for kind in (("own_r", half), ("own_l", half)):
                start(gather(kind, j))

    def forward(j):
        gather(("own_r", 0), j).wait_recv()
        start(gather(("fwd_r", 0), j))
        gather(("own_l", 1), j).wait_recv()
        start(gather(("fwd_l", 1), j))

    def gathered(j):
        for key in (("own_r", 1), ("own_l", 0), ("fwd_r", 0), ("fwd_l", 1)):
            gather(key, j).wait_recv()

    def exchange(j):
        return copy(("gz", j), gsend.at[j], grecv.at[j], zl=1 - zl)

    def grads_of(j):
        def tile(at):
            left = rows[0, :, pl.ds(at, 256)]
            mid_gu = jnp.concatenate([mids[2 * j, :, : 2 * PART], mids[2 * j + 1, :, : 2 * PART]], axis=1)
            gu = dot_f32(left, mid_gu, ((0,), (0,)))
            left = rows[1, :, pl.ds(at, 256)]
            mid_d = jnp.concatenate([mids[2 * j, :, 2 * PART :], mids[2 * j + 1, :, 2 * PART :]], axis=1)
            return gu, dot_f32(left, mid_d, ((0,), (0,)))

        def one(i, carry):
            mine = i >= own // 256
            k = i % (own // 256)
            half = jnp.where(mine, zl, 1 - zl)
            gu, d = tile(pl.multiple_of(half * own + k * 256, 256))
            to = pl.ds(pl.multiple_of(k * 256, 256), 256)

            @pl.when(jnp.logical_not(mine))
            def _():
                for s in range(2):
                    gsend[j, s, to, : 2 * PART] = gu[:, 2 * PART * s : 2 * PART * (s + 1)].astype(BF16)
                    gsend[j, s, to, 2 * PART :] = d[:, PART * s : PART * (s + 1)].astype(BF16)

            @pl.when(mine)
            def _():
                for s in range(2):
                    sub = 2 * j + s
                    dgu_out[to, sub * PART : (sub + 1) * PART] = gu[:, 2 * PART * s : 2 * PART * s + PART]
                    dgu_out[to, 512 + sub * PART : 512 + (sub + 1) * PART] = gu[
                        :, 2 * PART * s + PART : 2 * PART * (s + 1)
                    ]
                    dd_out[to, sub * PART : (sub + 1) * PART] = d[:, PART * s : PART * (s + 1)]

            @pl.when(i == own // 256 - 1)
            def _():
                exchange(j).start()

            return carry

        lax.fori_loop(0, 2 * (own // 256), one, 0)
        started.append(exchange(j))

    def add_grads(j):
        exchange(j).wait_recv()

        def one(i, carry):
            at = pl.ds(pl.multiple_of(i * 64, 16), 64)
            for s in range(2):
                sub = 2 * j + s
                got = grecv[j, s, at, :].astype(F32)
                dgu_out[at, sub * PART : (sub + 1) * PART] += got[:, :PART]
                dgu_out[at, 512 + sub * PART : 512 + (sub + 1) * PART] += got[:, PART : 2 * PART]
                dd_out[at, sub * PART : (sub + 1) * PART] += got[:, 2 * PART :]
            return carry

        lax.fori_loop(0, own // 64, one, 0)

    def score(key):
        src, dst, to = {
            "c": (0, 0, dict(c=1 - c)), "zh": (1, 1, dict(zh=1 - zh)),
            "x0": (2, 2, dict(x=xr)), "x1": (2, 3, dict(x=xl)), "x2": (2, 4, dict(x=xo)),
        }[key]
        return copy(("sc", key), srow.at[src], srecv.at[dst], **to)

    def scores():
        total = jnp.sum(jnp.transpose(sacc[...]), axis=0, keepdims=True)
        srow[0] = jnp.broadcast_to(total, (8, 512))
        start(score("c"))

    def scores_zh():
        score("c").wait_recv()
        srow[1] = srow[0] + srecv[0]
        start(score("zh"))

    def scores_x():
        score("zh").wait_recv()
        srow[2] = srow[1] + srecv[1]
        for key in ("x0", "x1", "x2"):
            start(score(key))

    def scores_end():
        for key in ("x0", "x1", "x2"):
            score(key).wait_recv()
        score_out[...] = (srow[2] + srecv[2]) + (srecv[3] + srecv[4])

    def pair(k, r):
        return copy(("bc", k, r), bsend.at[r, k], brecv.at[r, k], c=1 - c)

    def ring(key):
        kind, half = key
        src, dst, to = {
            "far_r": lambda: (bown.at[0, half], xrelay.at[0], xr),
            "far_l": lambda: (bown.at[0, half], xrelay.at[1], xl),
            "near_r": lambda: (bown.at[1, half], xrecv.at[0, half], xr),
            "near_l": lambda: (bown.at[2, half], xrecv.at[1, half], xl),
        }[kind]()
        return copy(("bx", key), src, dst, x=to)

    def last():
        return copy("bz", zsend, zrecv, zh=1 - zh)

    def add_tiles(out, a, b, also=None):
        def one(i, carry):
            at = pl.ds(pl.multiple_of(i * 144, 16), 144)
            total = a[at, :].astype(F32) + b[at, :].astype(F32)
            if also is not None:
                total = total + also[at, :].astype(F32)
            out[at, :] = total.astype(out.dtype)
            return carry

        lax.fori_loop(0, 3, one, 0)

    def back():
        for r, x_ in enumerate((xo, xr, xl, x)):

            def one(k, carry):
                t = 2 * k + x_ // 2
                col = pl.multiple_of((x_ % 2) * 2 * SUB, 128)
                acc = None
                for sub in range(4):
                    m = mids[sub, pl.ds(pl.multiple_of(t * CAP, 16), CAP), : 2 * PART]
                    w = wgt[sub, pl.ds(col, 2 * SUB), : 2 * PART]
                    part = dot_f32(m, w, ((1,), (1,)))
                    acc = part if acc is None else acc + part
                low, high = acc[:, :SUB], acc[:, SUB:]
                bown[r, k] = jnp.where(c == 0, low, high).astype(BF16)
                bsend[r, k] = jnp.where(c == 0, high, low).astype(BF16)
                return carry

            lax.fori_loop(0, 2, one, 0)
            for k in range(2):
                start(pair(k, r))

    def back_ring():
        for r in range(4):
            for k in range(2):
                pair(k, r).wait_recv()
                add_tiles(bown.at[r, k], bown.at[r, k], brecv.at[r, k])
            if r == 0:
                start(ring(("far_r", 0)))
                start(ring(("far_l", 1)))
            if r == 1:
                start(ring(("near_r", 1)))
            if r == 2:
                start(ring(("near_l", 0)))
        ring(("far_r", 0)).wait_recv()
        add_tiles(bown.at[1, 0], bown.at[1, 0], xrelay.at[0])
        start(ring(("near_r", 0)))
        ring(("far_l", 1)).wait_recv()
        add_tiles(bown.at[2, 1], bown.at[2, 1], xrelay.at[1])
        start(ring(("near_l", 1)))

    def back_end():
        for half in range(2):
            for kind in ("near_r", "near_l"):
                ring((kind, half)).wait_recv()
        add_tiles(zsend, bown.at[3, 1 - zh], xrecv.at[0, 1 - zh], xrecv.at[1, 1 - zh])
        start(last())
        last().wait_recv()
        add_tiles(zsend_own := bown.at[3, zh], bown.at[3, zh], xrecv.at[0, zh], xrecv.at[1, zh])
        add_tiles(back_out, zsend_own, zrecv)

    for sub in range(2):
        copy(("w", sub), win.at[sub], weights(sub, zl), zl=1 - zl).wait_recv()
    pre_of(0)
    for sub in range(2, 4):
        copy(("w", sub), win.at[sub], weights(sub, zl), zl=1 - zl).wait_recv()
    pre_of(1)
    add_relays(0)
    gates()
    add_relays(1)
    pointwise(0)
    pointwise(1)
    scores()
    forward(0)
    scores_zh()
    gathered(0)
    scores_x()
    grads_of(0)
    forward(1)
    scores_end()
    gathered(1)
    back()
    back_ring()
    grads_of(1)
    add_grads(0)
    back_end()
    add_grads(1)
    for cp in started:
        cp.wait_send()


def exchange_and_compute(xin, win, router, other):
    own = win.shape[1]
    rows_all = 4 * CAP
    vm = pltpu.VMEM
    piece = (CAP, SUB)
    flops = 2 * rows_all * 2 * own * 4 * SUB * 8 // 3
    return pl.pallas_call(
        kernel,
        out_shape=(
            jax.ShapeDtypeStruct(piece, BF16),
            jax.ShapeDtypeStruct((8, 512), F32),
            jax.ShapeDtypeStruct((own, 1024), F32),
            jax.ShapeDtypeStruct((own, 512), F32),
        ),
        in_specs=[pl.BlockSpec(memory_space=vm)] * 4,
        out_specs=[pl.BlockSpec(memory_space=vm)] * 4,
        scratch_shapes=[
            vm((2, rows_all, 2 * own), BF16),
            vm((4, 2 * own, SUB), BF16),
            vm((2, 3, 2) + piece, BF16),
            vm((2, 2) + piece, F32),
            vm((2, 2) + piece, BF16),
            vm((2, 2, 2) + piece, BF16),
            vm((4, 16, 512), F32),
            vm((3, 16, 512), F32),
            vm((512, PART), F32),
            vm((512, PART), F32),
            vm((4, rows_all, SUB), BF16),
            vm((2, 2, own, SUB), BF16),
            vm((2, 2, own, SUB), BF16),
            vm((4, 2) + piece, BF16),
            vm((4, 2) + piece, BF16),
            vm((4, 2) + piece, BF16),
            vm((2,) + piece, BF16),
            vm((2, 2) + piece, BF16),
            vm(piece, BF16),
            vm(piece, BF16),
            vm((3, 8, 512), F32),
            vm((5, 8, 512), F32),
            pltpu.SemaphoreType.DMA((80,)),
            pltpu.SemaphoreType.DMA((80,)),
        ],
        cost_estimate=pl.CostEstimate(flops=flops, bytes_accessed=20 << 20, transcendentals=CAP * 512),
        compiler_params=pltpu.CompilerParams(
            collective_id=0, has_side_effects=True, vmem_limit_bytes=67043328
        ),
    )(xin, win, router, other)


def local(tokens, cotangent, expert_choice, router, gate_up, w_down):
    own, hid = w_down.shape
    first = expert_choice[:, 0]
    second = expert_choice[:, 1]
    in_first = first == 0
    in_second = second == 0
    routed = jnp.logical_or(in_first, in_second)
    flags = routed.astype(jnp.int32)
    slot_rank = jnp.cumsum(flags) - flags
    slot_ids = jnp.arange(CAP, dtype=jnp.int32)
    placed = jnp.logical_and(routed[None, :], slot_rank[None, :] == slot_ids[:, None])
    select = placed.astype(BF16)

    picked = [dot_f32(select, a, ((1,), (0,))).astype(BF16) for a in (tokens, cotangent)]
    xin = lax.ppermute(jnp.stack(picked), ALL, swap_pairs())

    win = jnp.stack(
        [
            jnp.concatenate(
                [
                    gate_up[:, 0, PART * s : PART * (s + 1)],
                    gate_up[:, 1, PART * s : PART * (s + 1)],
                    w_down[:, PART * s : PART * (s + 1)],
                ],
                axis=1,
            )
            for s in range(hid // PART)
        ]
    )
    router_cols = lax.dynamic_slice_in_dim(router, lax.axis_index("y") * 2 * own, 2 * own, 1)
    router_cols = jnp.pad(router_cols, ((0, 8), (0, 0)))
    other = jnp.sum(jnp.where(placed, (first + second + 1)[None, :], 0), axis=1) - 1
    other = jnp.pad(other, (0, 512 - CAP), constant_values=-1)
    other = jnp.broadcast_to(other[None, :], (8, 512))

    back, score, d_gu, d_down = exchange_and_compute(xin, win, router_cols, other)

    back = lax.ppermute(back, ALL, swap_pairs())
    grad_tokens = dot_f32(select, back, ((0,), (0,))).astype(BF16)
    token_score = jnp.sum(jnp.where(placed, score[0, :CAP, None], 0.0), axis=0)
    d_combine = jnp.stack(
        [jnp.where(in_first, token_score, 0.0), jnp.where(in_second, token_score, 0.0)], axis=1
    )
    return (grad_tokens, d_combine, d_gu.reshape(own, 2, hid), d_down)


def solution(mesh):
    split = Mesh(mesh.devices.reshape(4, 2, 2, 4, 2), ALL)
    return jax.shard_map(
        local,
        mesh=split,
        in_specs=(
            P(TOK, HID),
            P(TOK, HID),
            P(TOK, None),
            P(),
            P(TOK, None, HID),
            P(TOK, HID),
        ),
        out_specs=(P(TOK, HID), P(TOK, None), P(TOK, None, HID), P(TOK, HID)),
        check_vma=False,
    )
```

```python
import jax
import jax.numpy as jnp
from jax import lax
from jax.experimental import pallas as pl
from jax.experimental.pallas import tpu as pltpu
from jax.sharding import Mesh
from jax.sharding import PartitionSpec as P

CAP = 432
SUB = 384
PART = 128
TOK = ("y", "zl")
HID = ("zh", "x", "c")
ALL = TOK + HID
MESH = pl.DeviceIdType.MESH
F32 = jnp.float32
BF16 = jnp.bfloat16


def dot_f32(left, right, dims):
    return lax.dot_general(left, right, ((dims[0], dims[1]), ((), ())), preferred_element_type=F32)


def kernel(
    tokens, cotangent, win, router, meta,
    gtok_out, score_out, dgu_out, dd_out,
    select, xin, rows, wgt, psend, pown, prelay, precv, lsend, lrecv, gate, sacc, mids,
    gsend, grecv, bown, brecv, xrelay, xrecv, zsend, zrecv, fsend, fin, srow, srecv, labels,
    ssem, rsem,
):
    y, zl, zh, x, c = (lax.axis_index(a) for a in ALL)
    yr, yl, yo = (y + 1) % 4, (y + 3) % 4, (y + 2) % 4
    xr, xl, xo = (x + 1) % 4, (x + 3) % 4, (x + 2) % 4
    D = rows.shape[2]
    own = D // 2
    swap_y, swap_zh, swap_x = 2 * zh + x // 2, y // 2, 2 * (y % 2) + x % 2
    fixed = swap_y == y
    swap = dict(y=swap_y, zh=swap_zh, x=swap_x)

    number = {}
    started = []

    def index(key, n=1):
        if key not in number:
            number[key] = number.get("next", 0)
            number["next"] = number[key] + n
        return number[key]

    def copy_at(i, src, dst, **to):
        return pltpu.make_async_remote_copy(
            src_ref=src, dst_ref=dst, send_sem=ssem.at[i], recv_sem=rsem.at[i],
            device_id=to, device_id_type=MESH,
        )

    def copy(key, src, dst, **to):
        return copy_at(index(key), src, dst, **to)

    def start(cp):
        cp.start()
        started.append(cp)
        return cp

    barrier = pltpu.get_barrier_semaphore()
    peers = (
        dict(y=yr), dict(y=yl), dict(y=yo), dict(zl=1 - zl), dict(zh=1 - zh),
        dict(x=xr), dict(x=xl), dict(x=xo), dict(c=1 - c),
    )
    for peer in peers:
        pl.semaphore_signal(barrier, inc=1, device_id=peer, device_id_type=MESH)

    @pl.when(jnp.logical_not(fixed))
    def _():
        pl.semaphore_signal(barrier, inc=1, device_id=swap, device_id_type=MESH)
        pl.semaphore_wait(barrier, len(peers) + 1)

    @pl.when(fixed)
    def _():
        pl.semaphore_wait(barrier, len(peers))

    def place(zh_, x_, c_):
        row = pl.multiple_of((2 * zh_ + x_ // 2) * CAP, 16)
        col = pl.multiple_of((2 * (x_ % 2) + c_) * SUB, 128)
        return rows.at[:, pl.ds(row, CAP), pl.ds(col, SUB)]

    def weights(sub):
        at = wgt.at[sub, pl.ds(pl.multiple_of(zl * own, 16), own), :]
        return copy(("w", sub), win.at[sub], at, zl=1 - zl)

    here = place(zh, x, c)
    start(weights(0))
    start(weights(1))

    slots = lax.broadcasted_iota(jnp.int32, (CAP, tokens.shape[0]), 0)
    select[...] = jnp.where(slots == meta[0:1, :], 1.0, 0.0).astype(BF16)

    def move():
        return copy("move", xin, place(swap_zh, swap_x, c), **swap)

    xin[0] = dot_f32(select[...], tokens[...], ((1,), (0,))).astype(BF16)
    xin[1] = dot_f32(select[...], cotangent[...], ((1,), (0,))).astype(BF16)

    @pl.when(fixed)
    def _():
        here[...] = xin[...]

    @pl.when(jnp.logical_not(fixed))
    def _():
        move().start()

    def put_weights(i, carry):
        for sub in range(4):
            at = pl.multiple_of(zl * own + i * 96, 16)
            wgt[sub, pl.ds(at, 96), :] = win[sub, pl.ds(pl.multiple_of(i * 96, 16), 96), :]
        return carry

    lax.fori_loop(0, own // 96, put_weights, 0)
    named = jnp.broadcast_to(meta[1:2, :].astype(F32).astype(BF16), (16, tokens.shape[0]))
    labels[:, :CAP] = dot_f32(named, select[...], ((1,), (1,)))

    @pl.when(jnp.logical_not(fixed))
    def _():
        move().wait_recv()

    to_zh = start(copy("zh", here, here, zh=1 - zh))
    from_l0 = start(copy("xr0", here, here, x=xr))
    from_r0 = start(copy("xl0", here, here, x=xl))
    cores = {}

    def other_core(n, at):
        cores[n] = start(copy(("core", n), at, at, c=1 - c))

    other_core(0, here)
    start(weights(2))
    start(weights(3))

    def block_of(which, t):
        return rows[which, pl.ds(pl.multiple_of(t * CAP, 16), CAP), :]

    def ps(j, slot, half):
        return (j * 3 + slot) * 2 + half

    def rs(kind, half, j):
        src, dst, to = {
            "far_r": lambda: (psend.at[ps(j, 0, half)], prelay.at[j, 0], yr),
            "far_l": lambda: (psend.at[ps(j, 0, half)], prelay.at[j, 1], yl),
            "near_r": lambda: (psend.at[ps(j, 1, half)], precv.at[j, 0, half], yr),
            "near_l": lambda: (psend.at[ps(j, 2, half)], precv.at[j, 1, half], yl),
        }[kind]()
        return copy(("rs", kind, half, j), src, dst, y=to)

    def logit(r):
        to = (yo, yr, yl)[r]
        return copy(("lg", r), lsend.at[r], lrecv.at[r], y=to)

    def pre_block(j, t):
        r = (t - y + 4) % 4
        slot = jnp.where(r == 2, 0, jnp.where(r == 1, 1, jnp.where(r == 3, 2, 3)))
        x_in = block_of(0, t)
        x_cot = block_of(1, t)
        g0 = dot_f32(x_in, wgt[2 * j, :, : 2 * PART], ((1,), (0,)))
        g1 = dot_f32(x_in, wgt[2 * j + 1, :, : 2 * PART], ((1,), (0,)))
        w_d = jnp.concatenate([wgt[2 * j, :, 2 * PART :], wgt[2 * j + 1, :, 2 * PART :]], axis=1)
        d = dot_f32(x_cot, w_d, ((1,), (0,)))

        @pl.when(r != 0)
        def _():
            at = ps(j, slot, 0)
            psend[at, :, : 2 * PART] = g0.astype(BF16)
            psend[at + 1, :, : 2 * PART] = g1.astype(BF16)
            psend[at, :, 2 * PART :] = d[:, :PART].astype(BF16)
            psend[at + 1, :, 2 * PART :] = d[:, PART:].astype(BF16)

        @pl.when(r == 0)
        def _():
            pown[j, 0, :, : 2 * PART] = g0
            pown[j, 1, :, : 2 * PART] = g1
            pown[j, 0, :, 2 * PART :] = d[:, :PART]
            pown[j, 1, :, 2 * PART :] = d[:, PART:]

        @pl.when(r == 2)
        def _():
            rs("far_r", 0, j).start()
            rs("far_l", 1, j).start()

        @pl.when(r == 1)
        def _():
            rs("near_r", 1, j).start()

        @pl.when(r == 3)
        def _():
            rs("near_l", 0, j).start()

    def logits_of(r, carry):
        t = (y + jnp.where(r == 0, 2, jnp.where(r == 1, 1, jnp.where(r == 2, 3, 0)))) % 4
        cols = router[:, pl.ds(pl.multiple_of(y * D, 128), D)]
        lsend[r, :, :CAP] = dot_f32(cols, block_of(0, t), ((1,), (1,)))
        for k in range(3):

            @pl.when(r == k)
            def _():
                logit(k).start()

        return carry

    from_l0.wait_recv()
    at = place(zh, xl, c)
    from_lo = start(copy("xro", at, at, x=xr))
    other_core(2, at)
    from_r0.wait_recv()
    other_core(3, place(zh, xr, c))
    weights(0).wait_recv()
    weights(1).wait_recv()
    for n in (0, 2, 3):
        cores[n].wait_recv()
    pre_block(0, 2 * zh + x // 2)
    to_zh.wait_recv()
    there = place(1 - zh, x, c)
    from_l1 = start(copy("xr1", there, there, x=xr))
    from_r1 = start(copy("xl1", there, there, x=xl))
    other_core(1, there)
    from_lo.wait_recv()
    other_core(6, place(zh, xo, c))
    cores[6].wait_recv()
    pre_block(0, 2 * zh + 1 - x // 2)
    from_r1.wait_recv()
    at = place(1 - zh, xr, c)
    from_ro = start(copy("xlo", at, at, x=xl))
    other_core(4, at)
    from_l1.wait_recv()
    other_core(5, place(1 - zh, xl, c))
    for n in (1, 4, 5):
        cores[n].wait_recv()
    pre_block(0, 2 * (1 - zh) + x // 2)
    from_ro.wait_recv()
    other_core(7, place(1 - zh, xo, c))
    cores[7].wait_recv()
    pre_block(0, 2 * (1 - zh) + 1 - x // 2)

    def add_relays(j):
        for side, slot, half in ((0, 1, 0), (1, 2, 1)):
            rs(("far_r", "far_l")[side], half, j).wait_recv()
            mine = ps(j, slot, half)

            def add(i, carry):
                at = pl.ds(pl.multiple_of(i * 144, 16), 144)
                total = psend[mine, at, :].astype(F32) + prelay[j, side, at, :].astype(F32)
                psend[mine, at, :] = total.astype(BF16)
                return carry

            lax.fori_loop(0, 3, add, 0)
            rs(("near_r", "near_l")[side], half, j).start()

    def gates():
        for r in range(3):
            logit(r).wait_recv()
        logits = (lsend[3] + lrecv[0]) + (lrecv[1] + lrecv[2])
        label = labels[:8] - 1.0
        experts = lax.broadcasted_iota(jnp.int32, (8, 512), 0).astype(F32)
        picked = jnp.sum(jnp.where(label == experts, logits, 0.0), axis=0, keepdims=True)
        margin = logits[:1] - picked
        row = jnp.where(label[:1] > -0.5, jax.nn.sigmoid(margin), 0.0)
        gate[...] = jnp.transpose(jnp.broadcast_to(row, (PART, 512)))
        sacc[...] = jnp.zeros_like(sacc)

    def gather(kind, half, j):
        sub = 2 * j + half
        t, to = {"own_r": (y, yr), "own_l": (y, yl), "fwd_r": (yl, yr), "fwd_l": (yr, yl)}[kind]
        at = mids.at[sub, pl.ds(pl.multiple_of(t * CAP, 16), CAP), :]
        return copy(("ag", kind, half, j), at, at, y=to)

    def pointwise(j):
        for half in range(2):
            for kind in ("near_r", "near_l"):
                rs(kind, half, j).wait_recv()
        for half in range(2):
            sub = 2 * j + half

            def one(i, carry):
                at = pl.ds(pl.multiple_of(i * 48, 16), 48)
                pre = pown[j, half, at, :] + (
                    precv[j, 0, half, at, :].astype(F32) + precv[j, 1, half, at, :].astype(F32)
                )
                g, up, raw = pre[:, :PART], pre[:, PART : 2 * PART], pre[:, 2 * PART :]
                sigma = jax.nn.sigmoid(g)
                active = g * sigma
                slope = sigma * (1.0 + g * (1.0 - sigma))
                product = active * up
                scale = gate[at, :]
                sacc[at, :] += product * raw
                upstream = scale * raw
                to = pl.ds(pl.multiple_of(y * CAP + i * 48, 16), 48)
                mids[sub, to, :PART] = (upstream * up * slope).astype(BF16)
                mids[sub, to, PART : 2 * PART] = (upstream * active).astype(BF16)
                mids[sub, to, 2 * PART :] = (scale * product).astype(BF16)
                return carry

            lax.fori_loop(0, CAP // 48, one, 0)
            for kind in ("own_r", "own_l"):
                start(gather(kind, half, j))

    def forward(j):
        gather("own_r", 0, j).wait_recv()
        start(gather("fwd_r", 0, j))
        gather("own_l", 1, j).wait_recv()
        start(gather("fwd_l", 1, j))

    def near(j):
        gather("own_r", 1, j).wait_recv()
        gather("own_l", 0, j).wait_recv()

    def far(j):
        gather("fwd_r", 0, j).wait_recv()
        gather("fwd_l", 1, j).wait_recv()

    def exchange(j, s):
        return copy(("gz", j, s), gsend.at[j, s], grecv.at[j, s], zl=1 - zl)

    def out_rows(first, count, sub, g):
        return pl.ds(first * 8 + 2 * sub + g, count, stride=8)

    def grads_tile(j, at):
        mid_gu = jnp.concatenate([mids[2 * j, :, : 2 * PART], mids[2 * j + 1, :, : 2 * PART]], axis=1)
        gu = dot_f32(rows[0, :, pl.ds(at, 256)], mid_gu, ((0,), (0,)))
        mid_d = jnp.concatenate([mids[2 * j, :, 2 * PART :], mids[2 * j + 1, :, 2 * PART :]], axis=1)
        return gu, dot_f32(rows[1, :, pl.ds(at, 256)], mid_d, ((0,), (0,)))

    def grads_theirs(j):
        def one(i, carry):
            gu, d = grads_tile(j, pl.multiple_of((1 - zl) * own + i * 256, 256))
            to = pl.ds(pl.multiple_of(i * 256, 256), 256)
            for s in range(2):
                gsend[j, s, to, : 2 * PART] = gu[:, 2 * PART * s : 2 * PART * (s + 1)].astype(BF16)
                gsend[j, s, to, 2 * PART :] = d[:, PART * s : PART * (s + 1)].astype(BF16)
            return carry

        lax.fori_loop(0, own // 256, one, 0)

    def grads_mine(j):
        def one(i, carry):
            gu, d = grads_tile(j, pl.multiple_of(zl * own + i * 256, 256))
            to = pl.ds(pl.multiple_of(i * 256, 256), 256)
            for s in range(2):
                sub = 2 * j + s
                for g in range(2):
                    dgu_out[out_rows(i * 256, 256, sub, g), :] = gu[:, PART * (2 * s + g) : PART * (2 * s + g + 1)]
                dd_out[to, sub * PART : (sub + 1) * PART] = d[:, PART * s : PART * (s + 1)]
            return carry

        lax.fori_loop(0, own // 256, one, 0)

    def add_grads(j, s):
        exchange(j, s).wait_recv()
        sub = 2 * j + s

        def one(i, carry):
            at = pl.ds(pl.multiple_of(i * 64, 16), 64)
            got = grecv[j, s, at, :].astype(F32)
            for g in range(2):
                to = out_rows(i * 64, 64, sub, g)
                dgu_out[to, :] = dgu_out[to, :] + got[:, PART * g : PART * (g + 1)]
            dd_out[at, sub * PART : (sub + 1) * PART] += got[:, 2 * PART :]
            return carry

        lax.fori_loop(0, own // 64, one, 0)

    def score(key):
        src, dst, to = {
            "c": (0, 0, dict(c=1 - c)), "zh": (1, 1, dict(zh=1 - zh)),
            "x0": (2, 2, dict(x=xr)), "x1": (2, 3, dict(x=xl)), "x2": (2, 4, dict(x=xo)),
        }[key]
        return copy(("sc", key), srow.at[src], srecv.at[dst], **to)

    def scores():
        total = jnp.sum(jnp.transpose(sacc[...]), axis=0, keepdims=True)
        srow[0] = jnp.broadcast_to(total, (8, 512))
        start(score("c"))

    def scores_zh():
        score("c").wait_recv()
        srow[1] = srow[0] + srecv[0]
        start(score("zh"))

    def scores_x():
        score("zh").wait_recv()
        srow[2] = srow[1] + srecv[1]
        for key in ("x0", "x1", "x2"):
            start(score(key))

    def scores_end():
        for key in ("x0", "x1", "x2"):
            score(key).wait_recv()
        score_out[...] = (srow[2] + srecv[2]) + (srecv[3] + srecv[4])

    pair_base = index("pair", 8)

    def pair(i):
        return copy_at(pair_base + i, psend.at[i], brecv.at[i], c=1 - c)

    def ring(kind, half):
        src, dst, to = {
            "far_r": lambda: (bown.at[xo, half], xrelay.at[0], xr),
            "far_l": lambda: (bown.at[xo, half], xrelay.at[1], xl),
            "near_r": lambda: (bown.at[xr, half], xrecv.at[0, half], xr),
            "near_l": lambda: (bown.at[xl, half], xrecv.at[1, half], xl),
        }[kind]()
        return copy(("bx", kind, half), src, dst, x=to)

    def last():
        return copy("bz", zsend, zrecv, zh=1 - zh)

    def home():
        return copy("home", fsend, fin, **swap)

    def add_tiles(outs, refs):
        def one(i, carry):
            at = pl.ds(pl.multiple_of(i * 144, 16), 144)
            total = refs[0][at, :].astype(F32)
            for ref in refs[1:]:
                total = total + ref[at, :].astype(F32)
            for out in outs:
                out[at, :] = total.astype(out.dtype)
            return carry

        lax.fori_loop(0, 3, one, 0)

    def back_block(t):
        k = t // 2

        def one(b, carry):
            x_ = 2 * (t % 2) + b
            col = pl.multiple_of(b * 2 * SUB, 128)
            acc = None
            for sub in range(4):
                m = mids[sub, pl.ds(pl.multiple_of(t * CAP, 16), CAP), : 2 * PART]
                w = wgt[sub, pl.ds(col, 2 * SUB), : 2 * PART]
                part = dot_f32(m, w, ((1,), (1,)))
                acc = part if acc is None else acc + part
            low, high = acc[:, :SUB], acc[:, SUB:]
            i = x_ * 2 + k
            bown[x_, k] = jnp.where(c == 0, low, high).astype(BF16)
            psend[i] = jnp.where(c == 0, high, low).astype(BF16)
            pair(i).start()
            return carry

        lax.fori_loop(0, 2, one, 0)

    def back_sum(t):
        k = t // 2

        def one(b, carry):
            x_ = 2 * (t % 2) + b
            i = x_ * 2 + k
            r = (x_ - x + 4) % 4
            pair(i).wait_recv()
            add_tiles([bown.at[x_, k]], [bown.at[x_, k], brecv.at[i]])
            for r_, k_, kind in ((2, 0, "far_r"), (2, 1, "far_l"), (1, 1, "near_r"), (3, 0, "near_l")):

                @pl.when(jnp.logical_and(r == r_, k == k_))
                def _():
                    ring(kind, k_).start()

            return carry

        lax.fori_loop(0, 2, one, 0)

    weights(2).wait_recv()
    weights(3).wait_recv()

    def pre_one(n, carry):
        pre_block(1, (y + 2 + jnp.where(n == 0, 0, jnp.where(n == 1, 3, jnp.where(n == 2, 1, 2)))) % 4)
        return carry

    lax.fori_loop(0, 4, pre_one, 0)
    add_relays(0)
    lax.fori_loop(0, 4, logits_of, 0)
    add_relays(1)
    gates()
    pointwise(0)
    forward(0)
    pointwise(1)
    scores()
    for j in range(2):
        for kind in ("far_r", "far_l", "near_r", "near_l"):
            for half in range(2):
                if ("rs", kind, half, j) in number:
                    rs(kind, half, j).wait_send()
    back_block(y)
    scores_zh()
    near(0)
    far(0)
    grads_theirs(0)
    start(exchange(0, 0))
    start(exchange(0, 1))
    forward(1)
    grads_mine(0)
    scores_x()
    back_sum(y)
    near(1)
    back_block(yr)
    back_block(yl)
    back_sum(yr)
    back_sum(yl)
    scores_end()
    far(1)
    back_block(yo)
    grads_theirs(1)
    start(exchange(1, 0))
    back_sum(yo)
    grads_mine(1)
    ring("far_r", 0).wait_recv()
    add_tiles([bown.at[xr, 0]], [bown.at[xr, 0], xrelay.at[0]])
    ring("near_r", 0).start()
    ring("far_l", 1).wait_recv()
    add_tiles([bown.at[xl, 1]], [bown.at[xl, 1], xrelay.at[1]])
    ring("near_l", 1).start()
    add_grads(0, 0)
    add_grads(0, 1)
    for half in range(2):
        for kind in ("near_r", "near_l"):
            ring(kind, half).wait_recv()
    add_tiles([zsend], [bown.at[x, 1 - zh], xrecv.at[0, 1 - zh], xrecv.at[1, 1 - zh]])
    start(last())
    start(exchange(1, 1))
    add_grads(1, 0)
    last().wait_recv()
    add_tiles([fsend], [bown.at[x, zh], xrecv.at[0, zh], xrecv.at[1, zh], zrecv])

    @pl.when(fixed)
    def _():
        fin[...] = fsend[...]

    @pl.when(jnp.logical_not(fixed))
    def _():
        home().start()
        home().wait_recv()

    def put_tokens(i, carry):
        at = pl.ds(pl.multiple_of(i * 256, 256), 256)
        gtok_out[at, :] = dot_f32(select[:, at], fin[...], ((0,), (0,))).astype(BF16)
        return carry

    lax.fori_loop(0, tokens.shape[0] // 256, put_tokens, 0)
    add_grads(1, 1)

    @pl.when(jnp.logical_not(fixed))
    def _():
        move().wait_send()
        home().wait_send()

    for r in range(3):
        logit(r).wait_send()
    for kind in ("far_r", "far_l", "near_r", "near_l"):
        for half in range(2):
            if ("bx", kind, half) in number:
                ring(kind, half).wait_send()
    for i in range(8):
        pair(i).wait_send()
    for cp in started:
        cp.wait_send()


def exchange_and_compute(tokens, cotangent, win, router, meta):
    own = win.shape[1]
    rows_all = 4 * CAP
    vm = pltpu.VMEM
    piece = (CAP, SUB)
    flops = 2 * rows_all * 2 * own * 4 * SUB * 8 // 3
    return pl.pallas_call(
        kernel,
        out_shape=(
            jax.ShapeDtypeStruct(tokens.shape, BF16),
            jax.ShapeDtypeStruct((8, 512), F32),
            jax.ShapeDtypeStruct((own * 8, PART), F32),
            jax.ShapeDtypeStruct((own, 512), F32),
        ),
        in_specs=[pl.BlockSpec(memory_space=vm)] * 5,
        out_specs=[pl.BlockSpec(memory_space=vm)] * 4,
        scratch_shapes=[
            vm((CAP, tokens.shape[0]), BF16),
            vm((2,) + piece, BF16),
            vm((2, rows_all, 2 * own), BF16),
            vm((4, 2 * own, SUB), BF16),
            vm((12,) + piece, BF16),
            vm((2, 2) + piece, F32),
            vm((2, 2) + piece, BF16),
            vm((2, 2, 2) + piece, BF16),
            vm((4, 8, 512), F32),
            vm((3, 8, 512), F32),
            vm((512, PART), F32),
            vm((512, PART), F32),
            vm((4, rows_all, SUB), BF16),
            vm((2, 2, own, SUB), BF16),
            vm((2, 2, own, SUB), BF16),
            vm((4, 2) + piece, BF16),
            vm((8,) + piece, BF16),
            vm((2,) + piece, BF16),
            vm((2, 2) + piece, BF16),
            vm(piece, BF16),
            vm(piece, BF16),
            vm(piece, BF16),
            vm(piece, BF16),
            vm((3, 8, 512), F32),
            vm((5, 8, 512), F32),
            vm((16, 512), F32),
            pltpu.SemaphoreType.DMA((96,)),
            pltpu.SemaphoreType.DMA((96,)),
        ],
        cost_estimate=pl.CostEstimate(flops=flops, bytes_accessed=20 << 20, transcendentals=CAP * 512),
        compiler_params=pltpu.CompilerParams(
            collective_id=0, has_side_effects=True, vmem_limit_bytes=67043328
        ),
    )(tokens, cotangent, win, router, meta)


def local(tokens, cotangent, expert_choice, router, gate_up, w_down):
    own, hid = w_down.shape
    first = expert_choice[:, 0]
    second = expert_choice[:, 1]
    in_first = first == 0
    in_second = second == 0
    routed = jnp.logical_or(in_first, in_second)
    flags = routed.astype(jnp.int32)
    slot_rank = jnp.where(routed, jnp.cumsum(flags) - flags, -1)
    meta = jnp.stack([slot_rank, first + second + 1] + [flags] * 6)

    win = jnp.stack(
        [
            jnp.concatenate(
                [
                    gate_up[:, 0, PART * s : PART * (s + 1)],
                    gate_up[:, 1, PART * s : PART * (s + 1)],
                    w_down[:, PART * s : PART * (s + 1)],
                ],
                axis=1,
            )
            for s in range(hid // PART)
        ]
    )
    grad_tokens, score, d_gu, d_down = exchange_and_compute(tokens, cotangent, win, router, meta)

    slot_ids = jnp.arange(CAP, dtype=jnp.int32)
    placed = slot_rank[None, :] == slot_ids[:, None]
    token_score = jnp.sum(jnp.where(placed, score[0, :CAP, None], 0.0), axis=0)
    d_combine = jnp.stack(
        [jnp.where(in_first, token_score, 0.0), jnp.where(in_second, token_score, 0.0)], axis=1
    )
    d_gate_up = d_gu.reshape(own, hid // PART, 2, PART).transpose(0, 2, 1, 3).reshape(own, 2, hid)
    return (grad_tokens, d_combine, d_gate_up, d_down)


def solution(mesh):
    split = Mesh(mesh.devices.reshape(4, 2, 2, 4, 2), ALL)
    return jax.shard_map(
        local,
        mesh=split,
        in_specs=(
            P(TOK, HID),
            P(TOK, HID),
            P(TOK, None),
            P(),
            P(TOK, None, HID),
            P(TOK, HID),
        ),
        out_specs=(P(TOK, HID), P(TOK, None), P(TOK, None, HID), P(TOK, HID)),
        check_vma=False,
    )
```

```python
import jax
import jax.numpy as jnp
from jax import lax
from jax.experimental import pallas as pl
from jax.experimental.pallas import tpu as pltpu
from jax.sharding import Mesh
from jax.sharding import PartitionSpec as P

CAP = 432
SUB = 384
PART = 128
TOK = ("y", "zl")
HID = ("zh", "x", "c")
ALL = TOK + HID
MESH = pl.DeviceIdType.MESH
F32 = jnp.float32
BF16 = jnp.bfloat16


def dot_f32(left, right, dims):
    return lax.dot_general(left, right, ((dims[0], dims[1]), ((), ())), preferred_element_type=F32)


P0, PN = (0, 224), (224, 208)
Q0, QN = (0, 112, 224, 336), (112, 112, 112, 96)
RS_KINDS = ("far_r", "far_l", "nr_raw", "nl_raw", "nr_rel", "nl_rel")
AG_KINDS = ("own_r0", "own_l1", "own_r1", "own_l0", "fwd_r", "fwd_l")


def kernel(
    tokens, cotangent, gate_w, up_w, down_w, router, meta,
    fin, score_out, dgu_out, dd_out,
    select, xin, rows, wgt, psend, pown, prelay, precv, lsend, lrecv, gate, sacc, mids,
    gsend, grecv, bown, brecv, xrelay, xrecv, zsend, zrecv, fsend, stage, zstage, srow, srecv, labels,
    ssem, rsem,
):
    y, zl, zh, x, c = (lax.axis_index(a) for a in ALL)
    yr, yl, yo = (y + 1) % 4, (y + 3) % 4, (y + 2) % 4
    xr, xl, xo = (x + 1) % 4, (x + 3) % 4, (x + 2) % 4
    D = rows.shape[2]
    own = D // 2
    swap_y, swap_zh, swap_x = 2 * zh + x // 2, y // 2, 2 * (y % 2) + x % 2
    fixed = swap_y == y
    moves = jnp.logical_not(fixed)
    swap = dict(y=swap_y, zh=swap_zh, x=swap_x)

    number = {}
    started = []

    def index(key, n=1):
        if key not in number:
            number[key] = number.get("next", 0)
            number["next"] = number[key] + n
        return number[key]

    def copy_at(i, src, dst, **to):
        return pltpu.make_async_remote_copy(
            src_ref=src, dst_ref=dst, send_sem=ssem.at[i], recv_sem=rsem.at[i],
            device_id=to, device_id_type=MESH,
        )

    def copy(key, src, dst, **to):
        return copy_at(index(key), src, dst, **to)

    def start(cp):
        cp.start()
        started.append(cp)
        return cp

    barrier = pltpu.get_barrier_semaphore()
    peers = (
        dict(y=yr), dict(y=yl), dict(y=yo), dict(zl=1 - zl), dict(zh=1 - zh),
        dict(x=xr), dict(x=xl), dict(x=xo), dict(c=1 - c), dict(zl=1 - zl, zh=1 - zh),
    )
    for peer in peers:
        pl.semaphore_signal(barrier, inc=1, device_id=peer, device_id_type=MESH)

    @pl.when(moves)
    def _():
        pl.semaphore_signal(barrier, inc=1, device_id=swap, device_id_type=MESH)

    def place(p, zh_, x_, c_):
        row = pl.multiple_of((2 * zh_ + x_ // 2) * CAP + P0[p], 16)
        col = pl.multiple_of((2 * (x_ % 2) + c_) * SUB, 128)
        return rows.at[:, pl.ds(row, PN[p]), pl.ds(col, SUB)]

    def weights(sub):
        at = wgt.at[sub, pl.ds(pl.multiple_of(zl * own, 16), own), :]
        return copy(("w", sub), at, at, zl=1 - zl)

    def part(p):
        return pl.ds(P0[p], PN[p])

    def quarter(q):
        return pl.ds(Q0[q], QN[q])

    def move(p):
        return copy(("move", p), xin.at[:, part(p), :], place(p, swap_zh, swap_x, c), **swap)

    for p in range(2):
        slots = lax.broadcasted_iota(jnp.int32, (PN[p], tokens.shape[0]), 0) + P0[p]
        select[part(p), :] = jnp.where(slots == meta[0:1, :], 1.0, 0.0).astype(BF16)
        xin[0, part(p), :] = dot_f32(select[part(p), :], tokens[...], ((1,), (0,))).astype(BF16)
        xin[1, part(p), :] = dot_f32(select[part(p), :], cotangent[...], ((1,), (0,))).astype(BF16)

    def put_weights(i, carry):
        at = pl.ds(pl.multiple_of(zl * own + i * 96, 16), 96)
        of = pl.ds(pl.multiple_of(i * 96, 16), 96)
        for sub in range(4):
            for n, ref in enumerate((gate_w, up_w, down_w)):
                wgt[sub, at, PART * n : PART * (n + 1)] = ref[of, PART * sub : PART * (sub + 1)]
        return carry

    lax.fori_loop(0, own // 96, put_weights, 0)

    @pl.when(moves)
    def _():
        pl.semaphore_wait(barrier, len(peers) + 1)

    @pl.when(fixed)
    def _():
        pl.semaphore_wait(barrier, len(peers))

    for p in range(2):

        @pl.when(fixed)
        def _():
            place(p, zh, x, c)[...] = xin[:, part(p), :]

        @pl.when(moves)
        def _():
            move(p).start()

    start(weights(0))
    named = jnp.broadcast_to(meta[1:2, :].astype(F32).astype(BF16), (16, tokens.shape[0]))
    labels[:, :CAP] = dot_f32(named, select[...], ((1,), (1,)))

    steps = {
        "za": (lambda p: (place(p, zh, x, c), stage.at[:, part(p), :]), dict(zl=1 - zl)),
        "zb": (lambda p: (stage.at[:, part(p), :], place(p, zh, x, c)), dict(zl=1 - zl, zh=1 - zh)),
        "xr0": (lambda p: place(p, zh, x, c), dict(x=xr)),
        "xl0": (lambda p: place(p, zh, x, c), dict(x=xl)),
        "xro": (lambda p: place(p, zh, xl, c), dict(x=xr)),
        "xr1": (lambda p: place(p, 1 - zh, x, c), dict(x=xr)),
        "xl1": (lambda p: place(p, 1 - zh, x, c), dict(x=xl)),
        "xlo": (lambda p: place(p, 1 - zh, xr, c), dict(x=xl)),
        "c_own": (lambda p: place(p, zh, x, c), dict(c=1 - c)),
        "c_zh": (lambda p: place(p, 1 - zh, x, c), dict(c=1 - c)),
        "c_xr0": (lambda p: place(p, zh, xl, c), dict(c=1 - c)),
        "c_xl0": (lambda p: place(p, zh, xr, c), dict(c=1 - c)),
        "c_xr1": (lambda p: place(p, 1 - zh, xl, c), dict(c=1 - c)),
        "c_xl1": (lambda p: place(p, 1 - zh, xr, c), dict(c=1 - c)),
        "c_xro": (lambda p: place(p, zh, xo, c), dict(c=1 - c)),
        "c_xlo": (lambda p: place(p, 1 - zh, xo, c), dict(c=1 - c)),
    }

    def hop(name, p):
        at, to = steps[name]
        ends = at(p)
        src, dst = ends if isinstance(ends, tuple) else (ends, ends)
        return copy((name, p), src, dst, **to)

    def arrive(name, p, *then):
        hop(name, p).wait_recv()
        for follow in then:
            start(hop(follow, p))

    def all_cores(p):
        for name in steps:
            if name.startswith("c_"):
                hop(name, p).wait_recv()

    for p in range(2):

        @pl.when(moves)
        def _():
            move(p).wait_recv()

        for name in ("za", "xr0", "xl0", "c_own"):
            start(hop(name, p))
        start(weights(p + 1))
    start(weights(3))

    rs_base = index("rs", 48)
    ag_base = index("ag", 48)

    def rs(kind, p, s):
        q = 2 * p + (kind in ("far_l", "nr_raw", "nl_rel"))
        at = quarter(q)
        src, dst, to = {
            "fa": lambda: (psend.at[0, s, at, :], prelay.at[s, at, :], yr if kind == "far_r" else yl),
            "nr": lambda: (psend.at[1, s, at, :], precv.at[0, s, at, :], yr),
            "nl": lambda: (psend.at[2, s, at, :], precv.at[1, s, at, :], yl),
        }[kind[:2]]()
        return copy_at(rs_base + (p * 4 + s) * 6 + RS_KINDS.index(kind), src, dst, y=to)

    def logit(r):
        to = (yo, yr, yl)[r]
        return copy(("lg", r), lsend.at[r], lrecv.at[r], y=to)

    def pre(p, j):
        s0, s1 = 2 * j, 2 * j + 1

        def one(n, carry):
            r = jnp.where(n == 0, 2, jnp.where(n == 1, 1, jnp.where(n == 2, 3, 0)))
            t = (y + r) % 4
            at = pl.ds(pl.multiple_of(t * CAP + P0[p], 16), PN[p])
            x_in = rows[0, at, :]
            g0 = dot_f32(x_in, wgt[s0, :, : 2 * PART], ((1,), (0,)))
            g1 = dot_f32(x_in, wgt[s1, :, : 2 * PART], ((1,), (0,)))
            w_d = jnp.concatenate([wgt[s0, :, 2 * PART :], wgt[s1, :, 2 * PART :]], axis=1)
            d = dot_f32(rows[1, at, :], w_d, ((1,), (0,)))

            @pl.when(n < 3)
            def _():
                psend[n, s0, part(p), : 2 * PART] = g0.astype(BF16)
                psend[n, s1, part(p), : 2 * PART] = g1.astype(BF16)
                psend[n, s0, part(p), 2 * PART :] = d[:, :PART].astype(BF16)
                psend[n, s1, part(p), 2 * PART :] = d[:, PART:].astype(BF16)

            @pl.when(n == 3)
            def _():
                pown[s0, part(p), : 2 * PART] = g0
                pown[s1, part(p), : 2 * PART] = g1
                pown[s0, part(p), 2 * PART :] = d[:, :PART]
                pown[s1, part(p), 2 * PART :] = d[:, PART:]

            for m, kinds in ((0, ("far_r", "far_l")), (1, ("nr_raw",)), (2, ("nl_raw",))):

                @pl.when(n == m)
                def _():
                    for s in (s0, s1):
                        for kind in kinds:
                            rs(kind, p, s).start()

            return carry

        lax.fori_loop(0, 4, one, 0)

    def logits():
        cols = router[:, pl.ds(pl.multiple_of(y * D, 128), D)]

        def one(n, carry):
            t = (y + jnp.where(n == 0, 2, jnp.where(n == 1, 1, jnp.where(n == 2, 3, 0)))) % 4
            at = pl.ds(pl.multiple_of(t * CAP, 16), CAP)
            lsend[n, :, :CAP] = dot_f32(cols, rows[0, at, :], ((1,), (1,)))
            return carry

        lax.fori_loop(0, 4, one, 0)
        for r in range(3):
            start(logit(r))

    def relay(p, s):
        for side, slot, rel in (("far_r", 1, "nr_rel"), ("far_l", 2, "nl_rel")):
            at = quarter(2 * p + (side == "far_l"))
            rs(side, p, s).wait_recv()
            total = psend[slot, s, at, :].astype(F32) + prelay[s, at, :].astype(F32)
            psend[slot, s, at, :] = total.astype(BF16)
            rs(rel, p, s).start()

    def gates():
        for r in range(3):
            logit(r).wait_recv()
        total = (lsend[3] + lrecv[0]) + (lrecv[1] + lrecv[2])
        label = labels[:8] - 1.0
        experts = lax.broadcasted_iota(jnp.int32, (8, 512), 0).astype(F32)
        picked = jnp.sum(jnp.where(label == experts, total, 0.0), axis=0, keepdims=True)
        margin = total[:1] - picked
        row = jnp.where(label[:1] > -0.5, jax.nn.sigmoid(margin), 0.0)
        gate[...] = jnp.transpose(jnp.broadcast_to(row, (PART, 512)))
        sacc[...] = jnp.zeros_like(sacc)

    def ag(kind, p, s):
        q = 2 * p + (kind in ("own_r1", "own_l1", "fwd_l"))
        t = {"own": y, "fwd": yl if kind == "fwd_r" else yr}[kind[:3]]
        to = yr if kind[4] == "r" else yl
        at = mids.at[s, pl.ds(pl.multiple_of(t * CAP + Q0[q], 16), QN[q]), :]
        return copy_at(ag_base + (p * 4 + s) * 6 + AG_KINDS.index(kind), at, at, y=to)

    def pointwise(p, s):
        for kind in RS_KINDS[2:]:
            rs(kind, p, s).wait_recv()
        for q in (2 * p, 2 * p + 1):
            at = quarter(q)
            near = precv[0, s, at, :].astype(F32) + precv[1, s, at, :].astype(F32)
            now = pown[s, at, :] + near
            g, up, raw = now[:, :PART], now[:, PART : 2 * PART], now[:, 2 * PART :]
            sigma = jax.nn.sigmoid(g)
            active = g * sigma
            slope = sigma * (1.0 + g * (1.0 - sigma))
            product = active * up
            scale = gate[at, :]
            sacc[at, :] += product * raw
            upstream = scale * raw
            to = pl.ds(pl.multiple_of(y * CAP + Q0[q], 16), QN[q])
            mids[s, to, :PART] = (upstream * up * slope).astype(BF16)
            mids[s, to, PART : 2 * PART] = (upstream * active).astype(BF16)
            mids[s, to, 2 * PART :] = (scale * product).astype(BF16)
        for kind in AG_KINDS[:4]:
            ag(kind, p, s).start()

    def forward(p, s):
        for kind, fwd in (("own_r0", "fwd_r"), ("own_l1", "fwd_l")):
            ag(kind, p, s).wait_recv()
            ag(fwd, p, s).start()

    def near(p, s):
        ag("own_r1", p, s).wait_recv()
        ag("own_l0", p, s).wait_recv()

    def far(p, s):
        ag("fwd_r", p, s).wait_recv()
        ag("fwd_l", p, s).wait_recv()

    def exchange(s, half=None):
        at = pl.ds(0, own) if half is None else pl.ds(half * (own // 2), own // 2)
        return copy(("gz", s, half), gsend.at[s, at, :], grecv.at[s, at, :], zl=1 - zl)

    def out_rows(first, count, sub, g):
        return pl.ds(first * 8 + 2 * sub + g, count, stride=8)

    def grads_tile(s, at):
        gu = dot_f32(rows[0, :, pl.ds(at, 256)], mids[s, :, : 2 * PART], ((0,), (0,)))
        return gu, dot_f32(rows[1, :, pl.ds(at, 256)], mids[s, :, 2 * PART :], ((0,), (0,)))

    def grads_theirs(s):
        def one(i, carry):
            gu, d = grads_tile(s, pl.multiple_of((1 - zl) * own + i * 256, 256))
            to = pl.ds(pl.multiple_of(i * 256, 256), 256)
            gsend[s, to, : 2 * PART] = gu.astype(BF16)
            gsend[s, to, 2 * PART :] = d.astype(BF16)
            return carry

        lax.fori_loop(0, own // 256, one, 0)

    def grads_mine(s):
        def one(i, carry):
            gu, d = grads_tile(s, pl.multiple_of(zl * own + i * 256, 256))
            for g in range(2):
                dgu_out[out_rows(i * 256, 256, s, g), :] = gu[:, PART * g : PART * (g + 1)]
            to = pl.ds(pl.multiple_of(i * 256, 256), 256)
            dd_out[to, s * PART : (s + 1) * PART] = d
            return carry

        lax.fori_loop(0, own // 256, one, 0)

    def add_grads(s, half=None):
        exchange(s, half).wait_recv()

        def one(i, carry):
            at = pl.ds(pl.multiple_of(i * 64, 16), 64)
            got = grecv[s, at, :].astype(F32)
            for g in range(2):
                to = out_rows(i * 64, 64, s, g)
                dgu_out[to, :] = dgu_out[to, :] + got[:, PART * g : PART * (g + 1)]
            dd_out[at, s * PART : (s + 1) * PART] += got[:, 2 * PART :]
            return carry

        count = own // 64
        if half is None:
            lax.fori_loop(0, count, one, 0)
        else:
            lax.fori_loop(half * (count // 2), (half + 1) * (count // 2), one, 0)

    def score(key):
        src, dst, to = {
            "c": (0, 0, dict(c=1 - c)), "zh": (1, 1, dict(zh=1 - zh)),
            "x0": (2, 2, dict(x=xr)), "x1": (2, 3, dict(x=xl)), "x2": (2, 4, dict(x=xo)),
        }[key]
        return copy(("sc", key), srow.at[src], srecv.at[dst], **to)

    def scores():
        total = jnp.sum(jnp.transpose(sacc[...]), axis=0, keepdims=True)
        srow[0] = jnp.broadcast_to(total, (8, 512))
        start(score("c"))

    def scores_zh():
        score("c").wait_recv()
        srow[1] = srow[0] + srecv[0]
        start(score("zh"))

    def scores_x():
        score("zh").wait_recv()
        srow[2] = srow[1] + srecv[1]
        for key in ("x0", "x1", "x2"):
            start(score(key))

    def scores_end():
        for key in ("x0", "x1", "x2"):
            score(key).wait_recv()
        score_out[...] = (srow[2] + srecv[2]) + (srecv[3] + srecv[4])

    pair_base = index("pair", 16)

    def pair(p, i):
        src = psend.at[i // 4, i % 4, part(p), :]
        return copy_at(pair_base + p * 8 + i, src, brecv.at[i, part(p), :], c=1 - c)

    def ring(kind, half, p):
        at = part(p)
        src, dst, to = {
            "far_r": lambda: (bown.at[xo, half, at, :], xrelay.at[0, at, :], xr),
            "far_l": lambda: (bown.at[xo, half, at, :], xrelay.at[1, at, :], xl),
            "near_r": lambda: (bown.at[xr, half, at, :], xrecv.at[0, half, at, :], xr),
            "near_l": lambda: (bown.at[xl, half, at, :], xrecv.at[1, half, at, :], xl),
        }[kind]()
        return copy(("bx", kind, half, p), src, dst, x=to)

    def last_a(p):
        return copy(("bza", p), zsend.at[part(p), :], zstage.at[part(p), :], zl=1 - zl)

    def last_b(p):
        return copy(("bzb", p), zstage.at[part(p), :], zrecv.at[part(p), :], zl=1 - zl, zh=1 - zh)

    def last_relay(p):
        last_a(p).wait_recv()
        start(last_b(p))

    def home(p):
        return copy(("home", p), fsend.at[part(p), :], fin.at[part(p), :], **swap)

    def add_rows(p, out, refs):
        for q in (2 * p, 2 * p + 1):
            at = quarter(q)
            total = refs[0][at, :].astype(F32)
            for ref in refs[1:]:
                total = total + ref[at, :].astype(F32)
            out[at, :] = total.astype(out.dtype)

    def back_block(p, t):
        k = t // 2

        def one(b, carry):
            x_ = 2 * (t % 2) + b
            col = pl.multiple_of(b * 2 * SUB, 128)
            acc = None
            for sub in range(4):
                m = mids[sub, pl.ds(pl.multiple_of(t * CAP + P0[p], 16), PN[p]), : 2 * PART]
                w = wgt[sub, pl.ds(col, 2 * SUB), : 2 * PART]
                piece = dot_f32(m, w, ((1,), (1,)))
                acc = piece if acc is None else acc + piece
            low, high = acc[:, :SUB], acc[:, SUB:]
            i = x_ * 2 + k
            bown[x_, k, part(p), :] = jnp.where(c == 0, low, high).astype(BF16)
            psend[i // 4, i % 4, part(p), :] = jnp.where(c == 0, high, low).astype(BF16)
            pair(p, i).start()
            return carry

        lax.fori_loop(0, 2, one, 0)

    def back_sum(p, t):
        k = t // 2

        def one(b, carry):
            x_ = 2 * (t % 2) + b
            i = x_ * 2 + k
            r = (x_ - x + 4) % 4
            pair(p, i).wait_recv()
            add_rows(p, bown.at[x_, k], [bown.at[x_, k], brecv.at[i]])
            for r_, k_, kind in ((2, 0, "far_r"), (2, 1, "far_l"), (1, 1, "near_r"), (3, 0, "near_l")):

                @pl.when(jnp.logical_and(r == r_, k == k_))
                def _():
                    ring(kind, k_, p).start()

            return carry

        lax.fori_loop(0, 2, one, 0)

    def ring_relay(p):
        ring("far_r", 0, p).wait_recv()
        add_rows(p, bown.at[xr, 0], [bown.at[xr, 0], xrelay.at[0]])
        ring("near_r", 0, p).start()
        ring("far_l", 1, p).wait_recv()
        add_rows(p, bown.at[xl, 1], [bown.at[xl, 1], xrelay.at[1]])
        ring("near_l", 1, p).start()

    def ring_end(p):
        for half in range(2):
            for kind in ("near_r", "near_l"):
                ring(kind, half, p).wait_recv()
        add_rows(p, zsend, [bown.at[x, 1 - zh], xrecv.at[0, 1 - zh], xrecv.at[1, 1 - zh]])
        start(last_a(p))

    def go_home(p):
        last_b(p).wait_recv()
        add_rows(p, fsend, [bown.at[x, zh], xrecv.at[0, zh], xrecv.at[1, zh], zrecv])

        @pl.when(fixed)
        def _():
            fin[part(p), :] = fsend[part(p), :]

        @pl.when(moves)
        def _():
            home(p).start()

    arrive("xr0", 0, "xro", "c_xr0")
    arrive("xl0", 0, "c_xl0")
    arrive("za", 0, "zb")
    arrive("zb", 0, "xr1", "xl1", "c_zh")
    arrive("xr0", 1, "xro", "c_xr0")
    arrive("xl0", 1, "c_xl0")
    arrive("za", 1, "zb")
    arrive("xl1", 0, "xlo", "c_xl1")
    arrive("zb", 1, "xr1", "xl1", "c_zh")
    arrive("xro", 0, "c_xro")
    arrive("xr1", 0, "c_xr1")
    arrive("xl1", 1, "xlo", "c_xl1")
    arrive("xlo", 0, "c_xlo")
    weights(0).wait_recv()
    weights(1).wait_recv()
    all_cores(0)
    pre(0, 0)
    arrive("xro", 1, "c_xro")
    arrive("xr1", 1, "c_xr1")
    arrive("xlo", 1, "c_xlo")
    all_cores(1)
    pre(1, 0)
    relay(0, 0)
    relay(0, 1)
    logits()
    weights(2).wait_recv()
    weights(3).wait_recv()
    pre(0, 1)
    relay(1, 0)
    relay(1, 1)
    pre(1, 1)
    gates()
    pointwise(0, 0)
    pointwise(1, 0)
    relay(0, 2)
    relay(0, 3)
    pointwise(0, 1)
    pointwise(1, 1)
    relay(1, 2)
    relay(1, 3)
    forward(0, 0)
    forward(1, 0)
    pointwise(0, 2)
    pointwise(0, 3)
    forward(0, 1)
    forward(1, 1)
    pointwise(1, 2)
    pointwise(1, 3)
    scores()
    near(0, 0)
    near(1, 0)
    far(0, 0)
    far(1, 0)
    scores_zh()
    grads_theirs(0)
    start(exchange(0))
    forward(0, 2)
    forward(0, 3)
    for kind in RS_KINDS:
        for p in range(2):
            for s in range(4):
                rs(kind, p, s).wait_send()
    back_block(0, y)
    near(0, 1)
    near(1, 1)
    far(0, 1)
    far(1, 1)
    grads_theirs(1)
    start(exchange(1))
    near(0, 2)
    near(0, 3)
    back_block(0, yr)
    forward(1, 2)
    forward(1, 3)
    back_block(0, yl)
    far(0, 2)
    far(0, 3)
    back_block(0, yo)
    back_block(1, y)
    back_sum(0, y)
    back_sum(0, yr)
    back_sum(0, yl)
    back_sum(0, yo)
    near(1, 2)
    near(1, 3)
    back_block(1, yr)
    back_block(1, yl)
    far(1, 2)
    far(1, 3)
    back_block(1, yo)
    ring_relay(0)
    back_sum(1, y)
    back_sum(1, yr)
    back_sum(1, yl)
    back_sum(1, yo)
    grads_theirs(2)
    start(exchange(2))
    ring_end(0)
    grads_theirs(3)
    start(exchange(3, 0))
    ring_relay(1)
    last_relay(0)
    grads_mine(0)
    ring_end(1)
    start(exchange(3, 1))
    scores_x()
    go_home(0)
    last_relay(1)
    grads_mine(1)
    add_grads(0)
    add_grads(1)
    go_home(1)
    grads_mine(2)
    grads_mine(3)
    scores_end()
    add_grads(2)

    @pl.when(moves)
    def _():
        home(0).wait_recv()
        home(1).wait_recv()

    add_grads(3, 0)
    add_grads(3, 1)

    @pl.when(moves)
    def _():
        for p in range(2):
            move(p).wait_send()
            home(p).wait_send()

    for kind in AG_KINDS:
        for p in range(2):
            for s in range(4):
                ag(kind, p, s).wait_send()
    for key in number:
        if key[0] == "bx":
            ring(*key[1:]).wait_send()
    for p in range(2):
        for i in range(8):
            pair(p, i).wait_send()
    for cp in started:
        cp.wait_send()


def finish(meta, fin, score, d_gu, d_down):
    total = meta.shape[1]
    steps = 6
    tile = total // steps
    vm = pltpu.VMEM

    def body(meta_ref, fin_ref, score_ref, gu_ref, down_ref, gtok_ref, comb_ref, gu_out, down_out):
        gu_out[...] = gu_ref[...]
        down_out[...] = down_ref[...]
        slots = lax.broadcasted_iota(jnp.int32, (CAP, tile), 0)
        select = jnp.where(slots == meta_ref[0:1, :], 1.0, 0.0).astype(BF16)
        gtok_ref[...] = dot_f32(select, fin_ref[...], ((0,), (0,))).astype(BF16)
        exact = score_ref[0:1, :CAP]
        high = exact.astype(BF16)
        rest = exact - high.astype(F32)
        middle = rest.astype(BF16)
        low = (rest - middle.astype(F32)).astype(BF16)
        at = lax.broadcasted_iota(jnp.int32, (16, CAP), 0)
        split = jnp.where(at == 0, high.astype(F32), jnp.where(at == 1, middle.astype(F32), low.astype(F32)))
        split = jnp.where(at < 3, split, 0.0).astype(BF16)
        parts = dot_f32(split, select, ((1,), (0,)))
        value = parts[0:1] + (parts[1:2] + parts[2:3])
        column = lax.broadcasted_iota(jnp.int32, (8, tile), 0)
        chosen = jnp.where(column == 0, meta_ref[2:3, :], meta_ref[3:4, :])
        comb_ref[...] = jnp.where(chosen > 0, value, 0.0)

    whole = lambda a: pl.BlockSpec(a.shape, lambda i: (0, 0))
    rows = lambda a: pl.BlockSpec((a.shape[0] // steps, a.shape[1]), lambda i: (i, 0))
    cols = pl.BlockSpec((8, tile), lambda i: (0, i))
    return pl.pallas_call(
        body,
        grid=(steps,),
        out_shape=(
            jax.ShapeDtypeStruct((total, SUB), BF16),
            jax.ShapeDtypeStruct((8, total), F32),
            jax.ShapeDtypeStruct(d_gu.shape, F32),
            jax.ShapeDtypeStruct(d_down.shape, F32),
        ),
        in_specs=[cols, whole(fin), whole(score), rows(d_gu), rows(d_down)],
        out_specs=[pl.BlockSpec((tile, SUB), lambda i: (i, 0)), cols, rows(d_gu), rows(d_down)],
        cost_estimate=pl.CostEstimate(flops=2 * total * CAP * SUB, bytes_accessed=12 << 20, transcendentals=0),
    )(meta, fin, score, d_gu, d_down)


def exchange_and_compute(tokens, cotangent, gate_w, up_w, down_w, router, meta):
    own = down_w.shape[0]
    rows_all = 4 * CAP
    vm = pltpu.VMEM
    piece = (CAP, SUB)
    flops = 2 * rows_all * 2 * own * 4 * SUB * 8 // 3
    return pl.pallas_call(
        kernel,
        out_shape=(
            jax.ShapeDtypeStruct(piece, BF16),
            jax.ShapeDtypeStruct((8, 512), F32),
            jax.ShapeDtypeStruct((own * 8, PART), F32),
            jax.ShapeDtypeStruct((own, 512), F32),
        ),
        in_specs=[pl.BlockSpec(memory_space=vm)] * 7,
        out_specs=[pl.BlockSpec(memory_space=vm)] * 4,
        scratch_shapes=[
            vm((CAP, tokens.shape[0]), BF16),
            vm((2,) + piece, BF16),
            vm((2, rows_all, 2 * own), BF16),
            vm((4, 2 * own, SUB), BF16),
            vm((3, 4) + piece, BF16),
            vm((4,) + piece, F32),
            vm((4,) + piece, BF16),
            vm((2, 4) + piece, BF16),
            vm((4, 8, 512), F32),
            vm((3, 8, 512), F32),
            vm((512, PART), F32),
            vm((512, PART), F32),
            vm((4, rows_all, SUB), BF16),
            vm((4, own, SUB), BF16),
            vm((4, own, SUB), BF16),
            vm((4, 2) + piece, BF16),
            vm((8,) + piece, BF16),
            vm((2,) + piece, BF16),
            vm((2, 2) + piece, BF16),
            vm(piece, BF16),
            vm(piece, BF16),
            vm(piece, BF16),
            vm((2,) + piece, BF16),
            vm(piece, BF16),
            vm((3, 8, 512), F32),
            vm((5, 8, 512), F32),
            vm((16, 512), F32),
            pltpu.SemaphoreType.DMA((192,)),
            pltpu.SemaphoreType.DMA((192,)),
        ],
        cost_estimate=pl.CostEstimate(flops=flops, bytes_accessed=20 << 20, transcendentals=CAP * 512),
        compiler_params=pltpu.CompilerParams(
            collective_id=0, has_side_effects=True, vmem_limit_bytes=67043328
        ),
    )(tokens, cotangent, gate_w, up_w, down_w, router, meta)


def local(tokens, cotangent, expert_choice, router, gate_up, w_down):
    own, hid = w_down.shape
    first = expert_choice[:, 0]
    second = expert_choice[:, 1]
    in_first = first == 0
    in_second = second == 0
    routed = jnp.logical_or(in_first, in_second)
    flags = routed.astype(jnp.int32)
    slot_rank = jnp.where(routed, jnp.cumsum(flags) - flags, -1)
    meta = [slot_rank, first + second + 1, in_first.astype(jnp.int32), in_second.astype(jnp.int32)]
    meta = jnp.stack(meta + [flags] * 4)
    fin, score, d_gu, d_down = exchange_and_compute(
        tokens, cotangent, gate_up[:, 0, :], gate_up[:, 1, :], w_down, router, meta
    )
    grad_tokens, combine, d_gu, d_down = finish(meta, fin, score, d_gu, d_down)
    d_gate_up = d_gu.reshape(own, hid // PART, 2, PART).transpose(0, 2, 1, 3).reshape(own, 2, hid)
    return (grad_tokens, combine[:2].T, d_gate_up, d_down)


def solution(mesh):
    split = Mesh(mesh.devices.reshape(4, 2, 2, 4, 2), ALL)
    return jax.shard_map(
        local,
        mesh=split,
        in_specs=(
            P(TOK, HID),
            P(TOK, HID),
            P(TOK, None),
            P(),
            P(TOK, None, HID),
            P(TOK, HID),
        ),
        out_specs=(P(TOK, HID), P(TOK, None), P(TOK, None, HID), P(TOK, HID)),
        check_vma=False,
    )
```

```python
import jax
import jax.numpy as jnp
from jax import lax
from jax.experimental import pallas as pl
from jax.experimental.pallas import tpu as pltpu
from jax.sharding import Mesh
from jax.sharding import PartitionSpec as P

CAP = 432
SUB = 384
PART = 128
TOK = ("y", "zl")
HID = ("zh", "x", "c")
ALL = TOK + HID
MESH = pl.DeviceIdType.MESH
F32 = jnp.float32
BF16 = jnp.bfloat16


def dot_f32(left, right, dims):
    return lax.dot_general(left, right, ((dims[0], dims[1]), ((), ())), preferred_element_type=F32)


P0, PN = (0, 224), (224, 208)
Q0, QN = (0, 112, 224, 336), (112, 112, 112, 96)
RS_KINDS = ("far_r", "far_l", "nr_raw", "nl_raw", "nr_rel", "nl_rel")
AG_KINDS = ("own_r0", "own_l1", "own_r1", "own_l0", "fwd_r", "fwd_l")


def kernel(
    tokens, cotangent, gate_up, down_w, router, choice,
    fin, comb_out, rank_out, dgu_out, dd_out,
    select, xin, rows, wgt, psend, pown, prelay, precv, lsend, lrecv, gate, sacc, mids,
    gsend, grecv, bown, brecv, xrelay, xrecv, zsend, zrecv, fsend, srow, srecv, labels, meta, flags,
    ssem, rsem,
):
    y, zl, zh, x, c = (lax.axis_index(a) for a in ALL)
    yr, yl, yo = (y + 1) % 4, (y + 3) % 4, (y + 2) % 4
    xr, xl, xo = (x + 1) % 4, (x + 3) % 4, (x + 2) % 4
    D = rows.shape[2]
    own = D // 2
    swap_y, swap_zh, swap_x = 2 * zh + x // 2, y // 2, 2 * (y % 2) + x % 2
    fixed = swap_y == y
    moves = jnp.logical_not(fixed)
    swap = dict(y=swap_y, zh=swap_zh, x=swap_x)

    number = {}
    started = []

    def index(key, n=1):
        if key not in number:
            number[key] = number.get("next", 0)
            number["next"] = number[key] + n
        return number[key]

    def copy_at(i, src, dst, **to):
        return pltpu.make_async_remote_copy(
            src_ref=src, dst_ref=dst, send_sem=ssem.at[i], recv_sem=rsem.at[i],
            device_id=to, device_id_type=MESH,
        )

    def copy(key, src, dst, **to):
        return copy_at(index(key), src, dst, **to)

    def start(cp):
        cp.start()
        started.append(cp)
        return cp

    barrier = pltpu.get_barrier_semaphore()
    peers = (
        dict(y=yr), dict(y=yl), dict(y=yo), dict(zl=1 - zl), dict(zh=1 - zh),
        dict(x=xr), dict(x=xl), dict(x=xo), dict(c=1 - c),
    )
    for peer in peers:
        pl.semaphore_signal(barrier, inc=1, device_id=peer, device_id_type=MESH)

    @pl.when(moves)
    def _():
        pl.semaphore_signal(barrier, inc=1, device_id=swap, device_id_type=MESH)

    def place(p, zh_, x_, c_):
        row = pl.multiple_of((2 * zh_ + x_ // 2) * CAP + P0[p], 16)
        col = pl.multiple_of((2 * (x_ % 2) + c_) * SUB, 128)
        return rows.at[:, pl.ds(row, PN[p]), pl.ds(col, SUB)]

    def weights(sub):
        at = wgt.at[sub, pl.ds(pl.multiple_of(zl * own, 16), own), :]
        return copy(("w", sub), at, at, zl=1 - zl)

    def part(p):
        return pl.ds(P0[p], PN[p])

    def quarter(q):
        return pl.ds(Q0[q], QN[q])

    def move(p):
        return copy(("move", p), xin.at[:, part(p), :], place(p, swap_zh, swap_x, c), **swap)

    total = tokens.shape[0]
    first, second = choice[0:1, :], choice[1:2, :]
    routed = jnp.logical_or(first == 0, second == 0)
    hits = jnp.where(routed, 1.0, 0.0)
    flags[...] = jnp.zeros_like(flags)
    for i in range(total // PART):
        flags[i : i + 1, :] = hits[:, PART * i : PART * (i + 1)]
    lane = lax.broadcasted_iota(jnp.int32, (PART, PART), 0)
    before = jnp.where(lane < lax.broadcasted_iota(jnp.int32, (PART, PART), 1), 1.0, 0.0)
    line = lax.broadcasted_iota(jnp.int32, (16, 16), 0)
    above = jnp.where(line > lax.broadcasted_iota(jnp.int32, (16, 16), 1), 1.0, 0.0)
    marks = flags[...].astype(BF16)
    within = dot_f32(marks, before.astype(BF16), ((1,), (0,)))
    counts = dot_f32(marks, jnp.ones((PART, PART), BF16), ((1,), (0,)))
    flags[...] = within + dot_f32(above.astype(BF16), counts.astype(BF16), ((1,), (0,)))
    for i in range(total // PART):
        at = slice(PART * i, PART * (i + 1))
        rank = flags[i : i + 1, :].astype(jnp.int32)
        meta[0:1, at] = jnp.where(routed[:, at], rank, -1)
    meta[1:2, :] = first + second + 1
    meta[2:3, :] = jnp.where(first == 0, 1, 0)
    meta[3:4, :] = jnp.where(second == 0, 1, 0)
    meta[4:8, :] = jnp.zeros((4, total), jnp.int32)
    rank_out[...] = meta[...]

    for p in range(2):
        slots = lax.broadcasted_iota(jnp.int32, (PN[p], tokens.shape[0]), 0) + P0[p]
        select[part(p), :] = jnp.where(slots == meta[0:1, :], 1.0, 0.0).astype(BF16)
        xin[0, part(p), :] = dot_f32(select[part(p), :], tokens[...], ((1,), (0,))).astype(BF16)
        xin[1, part(p), :] = dot_f32(select[part(p), :], cotangent[...], ((1,), (0,))).astype(BF16)

    def put_weights(i, carry):
        at = pl.ds(pl.multiple_of(zl * own + i * 96, 16), 96)
        of = pl.ds(pl.multiple_of(i * 96, 16), 96)
        for sub in range(4):
            for n, (ref, base) in enumerate(((gate_up, 0), (gate_up, 512), (down_w, 0))):
                wgt[sub, at, PART * n : PART * (n + 1)] = ref[of, base + PART * sub : base + PART * (sub + 1)]
        return carry

    lax.fori_loop(0, own // 96, put_weights, 0)

    @pl.when(moves)
    def _():
        pl.semaphore_wait(barrier, len(peers) + 1)

    @pl.when(fixed)
    def _():
        pl.semaphore_wait(barrier, len(peers))

    for p in range(2):

        @pl.when(fixed)
        def _():
            place(p, zh, x, c)[...] = xin[:, part(p), :]

        @pl.when(moves)
        def _():
            move(p).start()

    start(weights(0))
    named = jnp.broadcast_to(meta[1:2, :].astype(F32).astype(BF16), (16, tokens.shape[0]))
    labels[:, :CAP] = dot_f32(named, select[...], ((1,), (1,)))

    steps = {
        "zh": (lambda p: place(p, zh, x, c), dict(zh=1 - zh)),
        "xr0": (lambda p: place(p, zh, x, c), dict(x=xr)),
        "xl0": (lambda p: place(p, zh, x, c), dict(x=xl)),
        "xro": (lambda p: place(p, zh, xl, c), dict(x=xr)),
        "xr1": (lambda p: place(p, 1 - zh, x, c), dict(x=xr)),
        "xl1": (lambda p: place(p, 1 - zh, x, c), dict(x=xl)),
        "xlo": (lambda p: place(p, 1 - zh, xr, c), dict(x=xl)),
        "c_own": (lambda p: place(p, zh, x, c), dict(c=1 - c)),
        "c_zh": (lambda p: place(p, 1 - zh, x, c), dict(c=1 - c)),
        "c_xr0": (lambda p: place(p, zh, xl, c), dict(c=1 - c)),
        "c_xl0": (lambda p: place(p, zh, xr, c), dict(c=1 - c)),
        "c_xr1": (lambda p: place(p, 1 - zh, xl, c), dict(c=1 - c)),
        "c_xl1": (lambda p: place(p, 1 - zh, xr, c), dict(c=1 - c)),
        "c_xro": (lambda p: place(p, zh, xo, c), dict(c=1 - c)),
        "c_xlo": (lambda p: place(p, 1 - zh, xo, c), dict(c=1 - c)),
    }

    def hop(name, p):
        at, to = steps[name]
        return copy((name, p), at(p), at(p), **to)

    def arrive(name, p, *then):
        hop(name, p).wait_recv()
        for follow in then:
            start(hop(follow, p))

    def all_cores(p):
        for name in steps:
            if name.startswith("c_"):
                hop(name, p).wait_recv()

    for p in range(2):

        @pl.when(moves)
        def _():
            move(p).wait_recv()

        for name in ("zh", "xr0", "xl0", "c_own"):
            start(hop(name, p))
    for sub in range(1, 4):
        start(weights(sub))

    rs_base = index("rs", 48)
    ag_base = index("ag", 48)

    def rs(kind, p, s):
        q = 2 * p + (kind in ("far_l", "nr_raw", "nl_rel"))
        at = quarter(q)
        src, dst, to = {
            "fa": lambda: (psend.at[0, s, at, :], prelay.at[s, at, :], yr if kind == "far_r" else yl),
            "nr": lambda: (psend.at[1, s, at, :], precv.at[0, s, at, :], yr),
            "nl": lambda: (psend.at[2, s, at, :], precv.at[1, s, at, :], yl),
        }[kind[:2]]()
        return copy_at(rs_base + (p * 4 + s) * 6 + RS_KINDS.index(kind), src, dst, y=to)

    def logit(r):
        to = (yo, yr, yl)[r]
        return copy(("lg", r), lsend.at[r], lrecv.at[r], y=to)

    def pre(p, j):
        s0, s1 = 2 * j, 2 * j + 1

        def one(n, carry):
            r = jnp.where(n == 0, 2, jnp.where(n == 1, 1, jnp.where(n == 2, 3, 0)))
            t = (y + r) % 4
            at = pl.ds(pl.multiple_of(t * CAP + P0[p], 16), PN[p])
            x_in = rows[0, at, :]
            g0 = dot_f32(x_in, wgt[s0, :, : 2 * PART], ((1,), (0,)))
            g1 = dot_f32(x_in, wgt[s1, :, : 2 * PART], ((1,), (0,)))
            w_d = jnp.concatenate([wgt[s0, :, 2 * PART :], wgt[s1, :, 2 * PART :]], axis=1)
            d = dot_f32(rows[1, at, :], w_d, ((1,), (0,)))

            @pl.when(n < 3)
            def _():
                psend[n, s0, part(p), : 2 * PART] = g0.astype(BF16)
                psend[n, s1, part(p), : 2 * PART] = g1.astype(BF16)
                psend[n, s0, part(p), 2 * PART :] = d[:, :PART].astype(BF16)
                psend[n, s1, part(p), 2 * PART :] = d[:, PART:].astype(BF16)

            @pl.when(n == 3)
            def _():
                pown[s0, part(p), : 2 * PART] = g0
                pown[s1, part(p), : 2 * PART] = g1
                pown[s0, part(p), 2 * PART :] = d[:, :PART]
                pown[s1, part(p), 2 * PART :] = d[:, PART:]

            for m, kinds in ((0, ("far_r", "far_l")), (1, ("nr_raw",)), (2, ("nl_raw",))):

                @pl.when(n == m)
                def _():
                    for s in (s0, s1):
                        for kind in kinds:
                            rs(kind, p, s).start()

            return carry

        lax.fori_loop(0, 4, one, 0)

    def logits():
        cols = router[:, pl.ds(pl.multiple_of(y * D, 128), D)]

        def one(n, carry):
            t = (y + jnp.where(n == 0, 2, jnp.where(n == 1, 1, jnp.where(n == 2, 3, 0)))) % 4
            at = pl.ds(pl.multiple_of(t * CAP, 16), CAP)
            lsend[n, :, :CAP] = dot_f32(cols, rows[0, at, :], ((1,), (1,)))
            return carry

        lax.fori_loop(0, 4, one, 0)
        for r in range(3):
            start(logit(r))

    def relay(p, s):
        for side, slot, rel in (("far_r", 1, "nr_rel"), ("far_l", 2, "nl_rel")):
            at = quarter(2 * p + (side == "far_l"))
            rs(side, p, s).wait_recv()
            total = psend[slot, s, at, :].astype(F32) + prelay[s, at, :].astype(F32)
            psend[slot, s, at, :] = total.astype(BF16)
            rs(rel, p, s).start()

    def gates():
        for r in range(3):
            logit(r).wait_recv()
        total = (lsend[3] + lrecv[0]) + (lrecv[1] + lrecv[2])
        label = labels[:8] - 1.0
        experts = lax.broadcasted_iota(jnp.int32, (8, 512), 0).astype(F32)
        picked = jnp.sum(jnp.where(label == experts, total, 0.0), axis=0, keepdims=True)
        margin = total[:1] - picked
        row = jnp.where(label[:1] > -0.5, jax.nn.sigmoid(margin), 0.0)
        gate[...] = jnp.transpose(jnp.broadcast_to(row, (PART, 512)))
        sacc[...] = jnp.zeros_like(sacc)

    def ag(kind, p, s):
        q = 2 * p + (kind in ("own_r1", "own_l1", "fwd_l"))
        t = {"own": y, "fwd": yl if kind == "fwd_r" else yr}[kind[:3]]
        to = yr if kind[4] == "r" else yl
        at = mids.at[s, pl.ds(pl.multiple_of(t * CAP + Q0[q], 16), QN[q]), :]
        return copy_at(ag_base + (p * 4 + s) * 6 + AG_KINDS.index(kind), at, at, y=to)

    def pointwise(p, s):
        for kind in RS_KINDS[2:]:
            rs(kind, p, s).wait_recv()
        for q in (2 * p, 2 * p + 1):
            at = quarter(q)
            near = precv[0, s, at, :].astype(F32) + precv[1, s, at, :].astype(F32)
            now = pown[s, at, :] + near
            g, up, raw = now[:, :PART], now[:, PART : 2 * PART], now[:, 2 * PART :]
            sigma = jax.nn.sigmoid(g)
            active = g * sigma
            slope = sigma * (1.0 + g * (1.0 - sigma))
            product = active * up
            scale = gate[at, :]
            sacc[at, :] += product * raw
            upstream = scale * raw
            to = pl.ds(pl.multiple_of(y * CAP + Q0[q], 16), QN[q])
            mids[s, to, :PART] = (upstream * up * slope).astype(BF16)
            mids[s, to, PART : 2 * PART] = (upstream * active).astype(BF16)
            mids[s, to, 2 * PART :] = (scale * product).astype(BF16)
        for kind in AG_KINDS[:4]:
            ag(kind, p, s).start()

    def forward(p, s):
        for kind, fwd in (("own_r0", "fwd_r"), ("own_l1", "fwd_l")):
            ag(kind, p, s).wait_recv()
            ag(fwd, p, s).start()

    def near(p, s):
        ag("own_r1", p, s).wait_recv()
        ag("own_l0", p, s).wait_recv()

    def far(p, s):
        ag("fwd_r", p, s).wait_recv()
        ag("fwd_l", p, s).wait_recv()

    def exchange(s, half=None):
        at = pl.ds(0, own) if half is None else pl.ds(half * (own // 2), own // 2)
        return copy(("gz", s, half), gsend.at[s, at, :], grecv.at[s, at, :], zl=1 - zl)

    def out_rows(first, count, sub, g):
        return pl.ds(first * 8 + 2 * sub + g, count, stride=8)

    def grads_tile(s, at):
        gu = dot_f32(rows[0, :, pl.ds(at, 256)], mids[s, :, : 2 * PART], ((0,), (0,)))
        return gu, dot_f32(rows[1, :, pl.ds(at, 256)], mids[s, :, 2 * PART :], ((0,), (0,)))

    def grads_theirs(s):
        def one(i, carry):
            gu, d = grads_tile(s, pl.multiple_of((1 - zl) * own + i * 256, 256))
            to = pl.ds(pl.multiple_of(i * 256, 256), 256)
            gsend[s, to, : 2 * PART] = gu.astype(BF16)
            gsend[s, to, 2 * PART :] = d.astype(BF16)
            return carry

        lax.fori_loop(0, own // 256, one, 0)

    def grads_mine(s):
        def one(i, carry):
            gu, d = grads_tile(s, pl.multiple_of(zl * own + i * 256, 256))
            for g in range(2):
                dgu_out[out_rows(i * 256, 256, s, g), :] = gu[:, PART * g : PART * (g + 1)]
            to = pl.ds(pl.multiple_of(i * 256, 256), 256)
            dd_out[to, s * PART : (s + 1) * PART] = d
            return carry

        lax.fori_loop(0, own // 256, one, 0)

    def add_grads(s, half=None):
        exchange(s, half).wait_recv()

        def one(i, carry):
            at = pl.ds(pl.multiple_of(i * 64, 16), 64)
            got = grecv[s, at, :].astype(F32)
            for g in range(2):
                to = out_rows(i * 64, 64, s, g)
                dgu_out[to, :] = dgu_out[to, :] + got[:, PART * g : PART * (g + 1)]
            dd_out[at, s * PART : (s + 1) * PART] += got[:, 2 * PART :]
            return carry

        count = own // 64
        if half is None:
            lax.fori_loop(0, count, one, 0)
        else:
            lax.fori_loop(half * (count // 2), (half + 1) * (count // 2), one, 0)

    def score(key):
        src, dst, to = {
            "c": (0, 0, dict(c=1 - c)), "zh": (1, 1, dict(zh=1 - zh)),
            "x0": (2, 2, dict(x=xr)), "x1": (2, 3, dict(x=xl)), "x2": (2, 4, dict(x=xo)),
        }[key]
        return copy(("sc", key), srow.at[src], srecv.at[dst], **to)

    def scores():
        summed = jnp.sum(jnp.transpose(sacc[...]), axis=0, keepdims=True)
        srow[0] = jnp.broadcast_to(summed, (8, 512))
        start(score("c"))

    def scores_zh():
        score("c").wait_recv()
        srow[1] = srow[0] + srecv[0]
        start(score("zh"))

    def scores_x():
        score("zh").wait_recv()
        srow[2] = srow[1] + srecv[1]
        for key in ("x0", "x1", "x2"):
            start(score(key))

    def scores_end():
        for key in ("x0", "x1", "x2"):
            score(key).wait_recv()
        exact = ((srow[2] + srecv[2]) + (srecv[3] + srecv[4]))[0:1, :CAP]
        high = exact.astype(BF16).astype(F32)
        middle = (exact - high).astype(BF16).astype(F32)
        at = lax.broadcasted_iota(jnp.int32, (16, CAP), 0)
        split = jnp.where(at == 0, high, jnp.where(at == 1, middle, exact - high - middle))
        split = jnp.where(at < 3, split, 0.0).astype(BF16)
        parts = dot_f32(split, select[...], ((1,), (0,)))
        value = parts[0:1] + (parts[1:2] + parts[2:3])
        column = lax.broadcasted_iota(jnp.int32, (8, total), 0)
        chosen = jnp.where(column == 0, meta[2:3, :], meta[3:4, :])
        comb_out[...] = jnp.where(chosen > 0, value, 0.0)

    pair_base = index("pair", 16)

    def pair(p, i):
        src = psend.at[i // 4, i % 4, part(p), :]
        return copy_at(pair_base + p * 8 + i, src, brecv.at[i, part(p), :], c=1 - c)

    def ring(kind, half, p):
        at = part(p)
        src, dst, to = {
            "far_r": lambda: (bown.at[xo, half, at, :], xrelay.at[0, at, :], xr),
            "far_l": lambda: (bown.at[xo, half, at, :], xrelay.at[1, at, :], xl),
            "near_r": lambda: (bown.at[xr, half, at, :], xrecv.at[0, half, at, :], xr),
            "near_l": lambda: (bown.at[xl, half, at, :], xrecv.at[1, half, at, :], xl),
        }[kind]()
        return copy(("bx", kind, half, p), src, dst, x=to)

    def last(p):
        return copy(("bz", p), zsend.at[part(p), :], zrecv.at[part(p), :], zh=1 - zh)

    def home(p):
        return copy(("home", p), fsend.at[part(p), :], fin.at[part(p), :], **swap)

    def add_rows(p, out, refs):
        for q in (2 * p, 2 * p + 1):
            at = quarter(q)
            total = refs[0][at, :].astype(F32)
            for ref in refs[1:]:
                total = total + ref[at, :].astype(F32)
            out[at, :] = total.astype(out.dtype)

    def back_block(p, t):
        k = t // 2

        def one(b, carry):
            x_ = 2 * (t % 2) + b
            col = pl.multiple_of(b * 2 * SUB, 128)
            acc = None
            for sub in range(4):
                m = mids[sub, pl.ds(pl.multiple_of(t * CAP + P0[p], 16), PN[p]), : 2 * PART]
                w = wgt[sub, pl.ds(col, 2 * SUB), : 2 * PART]
                piece = dot_f32(m, w, ((1,), (1,)))
                acc = piece if acc is None else acc + piece
            low, high = acc[:, :SUB], acc[:, SUB:]
            i = x_ * 2 + k
            bown[x_, k, part(p), :] = jnp.where(c == 0, low, high).astype(BF16)
            psend[i // 4, i % 4, part(p), :] = jnp.where(c == 0, high, low).astype(BF16)
            pair(p, i).start()
            return carry

        lax.fori_loop(0, 2, one, 0)

    def back_sum(p, t):
        k = t // 2

        def one(b, carry):
            x_ = 2 * (t % 2) + b
            i = x_ * 2 + k
            r = (x_ - x + 4) % 4
            pair(p, i).wait_recv()
            add_rows(p, bown.at[x_, k], [bown.at[x_, k], brecv.at[i]])
            for r_, k_, kind in ((2, 0, "far_r"), (2, 1, "far_l"), (1, 1, "near_r"), (3, 0, "near_l")):

                @pl.when(jnp.logical_and(r == r_, k == k_))
                def _():
                    ring(kind, k_, p).start()

            return carry

        lax.fori_loop(0, 2, one, 0)

    def ring_relay(p):
        ring("far_r", 0, p).wait_recv()
        add_rows(p, bown.at[xr, 0], [bown.at[xr, 0], xrelay.at[0]])
        ring("near_r", 0, p).start()
        ring("far_l", 1, p).wait_recv()
        add_rows(p, bown.at[xl, 1], [bown.at[xl, 1], xrelay.at[1]])
        ring("near_l", 1, p).start()

    def ring_end(p):
        for half in range(2):
            for kind in ("near_r", "near_l"):
                ring(kind, half, p).wait_recv()
        add_rows(p, zsend, [bown.at[x, 1 - zh], xrecv.at[0, 1 - zh], xrecv.at[1, 1 - zh]])
        start(last(p))

    def go_home(p):
        last(p).wait_recv()
        add_rows(p, fsend, [bown.at[x, zh], xrecv.at[0, zh], xrecv.at[1, zh], zrecv])

        @pl.when(fixed)
        def _():
            fin[part(p), :] = fsend[part(p), :]

        @pl.when(moves)
        def _():
            home(p).start()

    arrive("xr0", 0, "xro", "c_xr0")
    arrive("xl0", 0, "c_xl0")
    arrive("zh", 0, "xr1", "xl1", "c_zh")
    arrive("xr0", 1, "xro", "c_xr0")
    arrive("xl0", 1, "c_xl0")
    arrive("zh", 1, "xr1", "xl1", "c_zh")
    arrive("xl1", 0, "xlo", "c_xl1")
    arrive("xro", 0, "c_xro")
    arrive("xr1", 0, "c_xr1")
    arrive("xl1", 1, "xlo", "c_xl1")
    arrive("xlo", 0, "c_xlo")
    weights(0).wait_recv()
    weights(1).wait_recv()
    all_cores(0)
    pre(0, 0)
    arrive("xro", 1, "c_xro")
    arrive("xr1", 1, "c_xr1")
    arrive("xlo", 1, "c_xlo")
    all_cores(1)
    pre(1, 0)
    logits()
    relay(0, 0)
    relay(0, 1)
    weights(2).wait_recv()
    weights(3).wait_recv()
    pre(0, 1)
    relay(1, 0)
    relay(1, 1)
    pre(1, 1)
    gates()
    relay(0, 2)
    relay(0, 3)
    pointwise(0, 0)
    pointwise(1, 0)
    relay(1, 2)
    relay(1, 3)
    forward(0, 0)
    pointwise(0, 1)
    forward(1, 0)
    pointwise(1, 1)
    forward(0, 1)
    for p in range(2):
        near(p, 0)
        far(p, 0)
    pointwise(0, 2)
    forward(1, 1)
    grads_theirs(0)
    start(exchange(0))
    pointwise(0, 3)
    forward(0, 2)
    pointwise(1, 2)
    forward(0, 3)
    pointwise(1, 3)
    for kind in RS_KINDS:
        for p in range(2):
            for s in range(4):
                rs(kind, p, s).wait_send()
    back_block(0, y)
    scores()
    for p in range(2):
        near(p, 1)
        far(p, 1)
    grads_theirs(1)
    start(exchange(1))
    forward(1, 2)
    for s in range(2, 4):
        near(0, s)
    back_block(0, yr)
    forward(1, 3)
    back_block(0, yl)
    for s in range(2, 4):
        far(0, s)
    back_block(0, yo)
    back_sum(0, y)
    back_sum(0, yr)
    back_sum(0, yl)
    back_sum(0, yo)
    scores_zh()
    near(1, 2)
    far(1, 2)
    grads_theirs(2)
    start(exchange(2))
    back_block(1, y)
    near(1, 3)
    back_block(1, yr)
    ring_relay(0)
    back_block(1, yl)
    far(1, 3)
    back_block(1, yo)
    back_sum(1, y)
    back_sum(1, yr)
    back_sum(1, yl)
    back_sum(1, yo)
    grads_theirs(3)
    ring_end(0)
    start(exchange(3, 0))
    ring_relay(1)
    scores_x()
    grads_mine(0)
    add_grads(0)
    ring_end(1)
    start(exchange(3, 1))
    go_home(0)
    grads_mine(1)
    add_grads(1)
    grads_mine(2)
    go_home(1)
    grads_mine(3)
    add_grads(2)
    scores_end()

    @pl.when(moves)
    def _():
        home(0).wait_recv()
        home(1).wait_recv()

    add_grads(3, 0)
    add_grads(3, 1)

    @pl.when(moves)
    def _():
        for p in range(2):
            move(p).wait_send()
            home(p).wait_send()

    for kind in AG_KINDS:
        for p in range(2):
            for s in range(4):
                ag(kind, p, s).wait_send()
    for key in number:
        if key[0] == "bx":
            ring(*key[1:]).wait_send()
    for p in range(2):
        for i in range(8):
            pair(p, i).wait_send()
    for cp in started:
        cp.wait_send()


def finish(ranks, fin, d_gu, d_down):
    total = ranks.shape[1]
    steps = 3
    tile = total // steps

    def body(ranks_ref, fin_ref, gu_ref, down_ref, gtok_ref, gu_out, down_out):
        gu_out[...] = gu_ref[...]
        down_out[...] = down_ref[...]
        slots = lax.broadcasted_iota(jnp.int32, (CAP, tile), 0)
        select = jnp.where(slots == ranks_ref[0:1, :], 1.0, 0.0).astype(BF16)
        gtok_ref[...] = dot_f32(select, fin_ref[...], ((0,), (0,))).astype(BF16)

    whole = lambda a: pl.BlockSpec(a.shape, lambda i: (0, 0))
    rows = lambda a: pl.BlockSpec((a.shape[0] // steps, a.shape[1]), lambda i: (i, 0))
    return pl.pallas_call(
        body,
        grid=(steps,),
        out_shape=(
            jax.ShapeDtypeStruct((total, SUB), BF16),
            jax.ShapeDtypeStruct(d_gu.shape, F32),
            jax.ShapeDtypeStruct(d_down.shape, F32),
        ),
        in_specs=[pl.BlockSpec((8, tile), lambda i: (0, i)), whole(fin), rows(d_gu), rows(d_down)],
        out_specs=[pl.BlockSpec((tile, SUB), lambda i: (i, 0)), rows(d_gu), rows(d_down)],
        cost_estimate=pl.CostEstimate(flops=2 * total * CAP * SUB, bytes_accessed=12 << 20, transcendentals=0),
    )(ranks, fin, d_gu, d_down)


def exchange_and_compute(tokens, cotangent, gate_up, down_w, router, choice):
    own = down_w.shape[0]
    rows_all = 4 * CAP
    vm = pltpu.VMEM
    piece = (CAP, SUB)
    flops = 2 * rows_all * 2 * own * 4 * SUB * 8 // 3
    return pl.pallas_call(
        kernel,
        out_shape=(
            jax.ShapeDtypeStruct(piece, BF16),
            jax.ShapeDtypeStruct((8, tokens.shape[0]), F32),
            jax.ShapeDtypeStruct((8, tokens.shape[0]), jnp.int32),
            jax.ShapeDtypeStruct((own * 8, PART), F32),
            jax.ShapeDtypeStruct((own, 512), F32),
        ),
        in_specs=[pl.BlockSpec(memory_space=vm)] * 6,
        out_specs=[pl.BlockSpec(memory_space=vm)] * 5,
        scratch_shapes=[
            vm((CAP, tokens.shape[0]), BF16),
            vm((2,) + piece, BF16),
            vm((2, rows_all, 2 * own), BF16),
            vm((4, 2 * own, SUB), BF16),
            vm((3, 4) + piece, BF16),
            vm((4,) + piece, F32),
            vm((4,) + piece, BF16),
            vm((2, 4) + piece, BF16),
            vm((4, 8, 512), F32),
            vm((3, 8, 512), F32),
            vm((512, PART), F32),
            vm((512, PART), F32),
            vm((4, rows_all, SUB), BF16),
            vm((4, own, SUB), BF16),
            vm((4, own, SUB), BF16),
            vm((4, 2) + piece, BF16),
            vm((8,) + piece, BF16),
            vm((2,) + piece, BF16),
            vm((2, 2) + piece, BF16),
            vm(piece, BF16),
            vm(piece, BF16),
            vm(piece, BF16),
            vm((3, 8, 512), F32),
            vm((5, 8, 512), F32),
            vm((16, 512), F32),
            vm((8, tokens.shape[0]), jnp.int32),
            vm((16, PART), F32),
            pltpu.SemaphoreType.DMA((192,)),
            pltpu.SemaphoreType.DMA((192,)),
        ],
        cost_estimate=pl.CostEstimate(flops=flops, bytes_accessed=20 << 20, transcendentals=CAP * 512),
        compiler_params=pltpu.CompilerParams(
            collective_id=0, has_side_effects=True, vmem_limit_bytes=67043328
        ),
    )(tokens, cotangent, gate_up, down_w, router, choice)


def local(tokens, cotangent, expert_choice, router, gate_up, w_down):
    own, hid = w_down.shape
    fin, combine, ranks, d_gu, d_down = exchange_and_compute(
        tokens, cotangent, gate_up.reshape(own, 2 * hid), w_down, router, expert_choice.T
    )
    grad_tokens, d_gu, d_down = finish(ranks, fin, d_gu, d_down)
    d_gate_up = d_gu.reshape(own, hid // PART, 2, PART).transpose(0, 2, 1, 3).reshape(own, 2, hid)
    return (grad_tokens, combine[:2].T, d_gate_up, d_down)


def solution(mesh):
    split = Mesh(mesh.devices.reshape(4, 2, 2, 4, 2), ALL)
    return jax.shard_map(
        local,
        mesh=split,
        in_specs=(
            P(TOK, HID),
            P(TOK, HID),
            P(TOK, None),
            P(),
            P(TOK, None, HID),
            P(TOK, HID),
        ),
        out_specs=(P(TOK, HID), P(TOK, None), P(TOK, None, HID), P(TOK, HID)),
        check_vma=False,
    )
```

```python
import jax
import jax.numpy as jnp
from jax import lax
from jax.experimental import pallas as pl
from jax.experimental.pallas import tpu as pltpu
from jax.sharding import Mesh
from jax.sharding import PartitionSpec as P

CAP = 432
SUB = 384
PART = 128
TOK = ("y", "zl")
HID = ("zh", "x", "c")
ALL = TOK + HID
MESH = pl.DeviceIdType.MESH
F32 = jnp.float32
BF16 = jnp.bfloat16


def dot_f32(left, right, dims):
    return lax.dot_general(left, right, ((dims[0], dims[1]), ((), ())), preferred_element_type=F32)


P0, PN = (0, 224), (224, 208)
Q0, QN = (0, 112, 224, 336), (112, 112, 112, 96)
RS_KINDS = ("far_r", "far_l", "nr_raw", "nl_raw", "nr_rel", "nl_rel")
AG_KINDS = ("own_r0", "own_l1", "own_r1", "own_l0", "fwd_r", "fwd_l")


def kernel(
    tokens, cotangent, gate_up, down_w, router, choice,
    fin_out, comb_out, rank_out, acc_out,
    select, xin, rows, wgt, psend, pown, prelay, precv, lsend, lrecv, gate, sacc, mids,
    gsend, grecv, bown, brecv, xrelay, xrecv, zsend, zrecv, fsend, fin, srow, srecv, labels, meta, flags, comb, acc,
    ssem, rsem, osem,
):
    y, zl, zh, x, c = (lax.axis_index(a) for a in ALL)
    yr, yl, yo = (y + 1) % 4, (y + 3) % 4, (y + 2) % 4
    xr, xl, xo = (x + 1) % 4, (x + 3) % 4, (x + 2) % 4
    D = rows.shape[2]
    own = D // 2
    swap_y, swap_zh, swap_x = 2 * zh + x // 2, y // 2, 2 * (y % 2) + x % 2
    fixed = swap_y == y
    moves = jnp.logical_not(fixed)
    swap = dict(y=swap_y, zh=swap_zh, x=swap_x)

    number = {}
    started = []

    def index(key, n=1):
        if key not in number:
            number[key] = number.get("next", 0)
            number["next"] = number[key] + n
        return number[key]

    def copy_at(i, src, dst, **to):
        return pltpu.make_async_remote_copy(
            src_ref=src, dst_ref=dst, send_sem=ssem.at[i], recv_sem=rsem.at[i],
            device_id=to, device_id_type=MESH,
        )

    def copy(key, src, dst, **to):
        return copy_at(index(key), src, dst, **to)

    def start(cp):
        cp.start()
        started.append(cp)
        return cp

    barrier = pltpu.get_barrier_semaphore()
    peers = (
        dict(y=yr), dict(y=yl), dict(y=yo), dict(zl=1 - zl), dict(zh=1 - zh),
        dict(x=xr), dict(x=xl), dict(x=xo), dict(c=1 - c),
    )
    for peer in peers:
        pl.semaphore_signal(barrier, inc=1, device_id=peer, device_id_type=MESH)

    @pl.when(moves)
    def _():
        pl.semaphore_signal(barrier, inc=1, device_id=swap, device_id_type=MESH)

    def place(p, zh_, x_, c_):
        row = pl.multiple_of((2 * zh_ + x_ // 2) * CAP + P0[p], 16)
        col = pl.multiple_of((2 * (x_ % 2) + c_) * SUB, 128)
        return rows.at[:, pl.ds(row, PN[p]), pl.ds(col, SUB)]

    def weights(sub):
        at = wgt.at[sub, pl.ds(pl.multiple_of(zl * own, 16), own), :]
        return copy(("w", sub), at, at, zl=1 - zl)

    def part(p):
        return pl.ds(P0[p], PN[p])

    def quarter(q):
        return pl.ds(Q0[q], QN[q])

    def move(p):
        return copy(("move", p), xin.at[:, part(p), :], place(p, swap_zh, swap_x, c), **swap)

    total = tokens.shape[0]
    first, second = choice[0:1, :], choice[1:2, :]
    routed = jnp.logical_or(first == 0, second == 0)
    hits = jnp.where(routed, 1.0, 0.0)
    flags[...] = jnp.zeros_like(flags)
    for i in range(total // PART):
        flags[i : i + 1, :] = hits[:, PART * i : PART * (i + 1)]
    lane = lax.broadcasted_iota(jnp.int32, (PART, PART), 0)
    before = jnp.where(lane < lax.broadcasted_iota(jnp.int32, (PART, PART), 1), 1.0, 0.0)
    line = lax.broadcasted_iota(jnp.int32, (16, 16), 0)
    above = jnp.where(line > lax.broadcasted_iota(jnp.int32, (16, 16), 1), 1.0, 0.0)
    marks = flags[...].astype(BF16)
    within = dot_f32(marks, before.astype(BF16), ((1,), (0,)))
    counts = dot_f32(marks, jnp.ones((PART, PART), BF16), ((1,), (0,)))
    flags[...] = within + dot_f32(above.astype(BF16), counts.astype(BF16), ((1,), (0,)))
    for i in range(total // PART):
        at = slice(PART * i, PART * (i + 1))
        rank = flags[i : i + 1, :].astype(jnp.int32)
        meta[0:1, at] = jnp.where(routed[:, at], rank, -1)
    meta[1:2, :] = first + second + 1
    meta[2:3, :] = jnp.where(first == 0, 1, 0)
    meta[3:4, :] = jnp.where(second == 0, 1, 0)
    meta[4:8, :] = jnp.zeros((4, total), jnp.int32)
    leave = []

    def put_out(src, dst):
        cp = pltpu.make_async_copy(src, dst, osem.at[len(leave)])
        cp.start()
        leave.append(cp)

    put_out(meta, rank_out)

    def dispatch(p):
        slots = lax.broadcasted_iota(jnp.int32, (PN[p], total), 0) + P0[p]
        select[part(p), :] = jnp.where(slots == meta[0:1, :], 1.0, 0.0).astype(BF16)
        xin[0, part(p), :] = dot_f32(select[part(p), :], tokens[...], ((1,), (0,))).astype(BF16)
        xin[1, part(p), :] = dot_f32(select[part(p), :], cotangent[...], ((1,), (0,))).astype(BF16)

    def send(p):
        @pl.when(fixed)
        def _():
            place(p, zh, x, c)[...] = xin[:, part(p), :]

        @pl.when(moves)
        def _():
            move(p).start()

    dispatch(0)

    @pl.when(moves)
    def _():
        pl.semaphore_wait(barrier, len(peers) + 1)

    @pl.when(fixed)
    def _():
        pl.semaphore_wait(barrier, len(peers))

    send(0)
    dispatch(1)
    send(1)

    def put_weights(i, carry):
        at = pl.ds(pl.multiple_of(zl * own + i * 96, 16), 96)
        of = pl.ds(pl.multiple_of(i * 96, 16), 96)
        for sub in range(4):
            for n, (ref, base) in enumerate(((gate_up, 0), (gate_up, 512), (down_w, 0))):
                wgt[sub, at, PART * n : PART * (n + 1)] = ref[of, base + PART * sub : base + PART * (sub + 1)]
        return carry

    lax.fori_loop(0, own // 96, put_weights, 0)
    start(weights(0))
    named = jnp.broadcast_to(meta[1:2, :].astype(F32).astype(BF16), (16, tokens.shape[0]))
    labels[:, :CAP] = dot_f32(named, select[...], ((1,), (1,)))

    steps = {
        "zh": (lambda p: place(p, zh, x, c), dict(zh=1 - zh)),
        "xr0": (lambda p: place(p, zh, x, c), dict(x=xr)),
        "xl0": (lambda p: place(p, zh, x, c), dict(x=xl)),
        "xro": (lambda p: place(p, zh, xl, c), dict(x=xr)),
        "xr1": (lambda p: place(p, 1 - zh, x, c), dict(x=xr)),
        "xl1": (lambda p: place(p, 1 - zh, x, c), dict(x=xl)),
        "xlo": (lambda p: place(p, 1 - zh, xr, c), dict(x=xl)),
        "c_own": (lambda p: place(p, zh, x, c), dict(c=1 - c)),
        "c_zh": (lambda p: place(p, 1 - zh, x, c), dict(c=1 - c)),
        "c_xr0": (lambda p: place(p, zh, xl, c), dict(c=1 - c)),
        "c_xl0": (lambda p: place(p, zh, xr, c), dict(c=1 - c)),
        "c_xr1": (lambda p: place(p, 1 - zh, xl, c), dict(c=1 - c)),
        "c_xl1": (lambda p: place(p, 1 - zh, xr, c), dict(c=1 - c)),
        "c_xro": (lambda p: place(p, zh, xo, c), dict(c=1 - c)),
        "c_xlo": (lambda p: place(p, 1 - zh, xo, c), dict(c=1 - c)),
    }

    def hop(name, p):
        at, to = steps[name]
        return copy((name, p), at(p), at(p), **to)

    def arrive(name, p, *then):
        hop(name, p).wait_recv()
        for follow in then:
            start(hop(follow, p))

    def all_cores(p):
        for name in steps:
            if name.startswith("c_"):
                hop(name, p).wait_recv()

    for p in range(2):

        @pl.when(moves)
        def _():
            move(p).wait_recv()

        for name in ("zh", "xr0", "xl0", "c_own"):
            start(hop(name, p))
    for sub in range(1, 4):
        start(weights(sub))

    rs_base = index("rs", 48)
    ag_base = index("ag", 48)

    def rs(kind, p, s):
        q = 2 * p + (kind in ("far_l", "nr_raw", "nl_rel"))
        at = quarter(q)
        src, dst, to = {
            "fa": lambda: (psend.at[0, s, at, :], prelay.at[s, at, :], yr if kind == "far_r" else yl),
            "nr": lambda: (psend.at[1, s, at, :], precv.at[0, s, at, :], yr),
            "nl": lambda: (psend.at[2, s, at, :], precv.at[1, s, at, :], yl),
        }[kind[:2]]()
        return copy_at(rs_base + (p * 4 + s) * 6 + RS_KINDS.index(kind), src, dst, y=to)

    def logit(r):
        to = (yo, yr, yl)[r]
        return copy(("lg", r), lsend.at[r], lrecv.at[r], y=to)

    def pre(p, j):
        s0, s1 = 2 * j, 2 * j + 1

        def one(n, carry):
            r = jnp.where(n == 0, 2, jnp.where(n == 1, 1, jnp.where(n == 2, 3, 0)))
            t = (y + r) % 4
            at = pl.ds(pl.multiple_of(t * CAP + P0[p], 16), PN[p])
            x_in = rows[0, at, :]
            g0 = dot_f32(x_in, wgt[s0, :, : 2 * PART], ((1,), (0,)))
            g1 = dot_f32(x_in, wgt[s1, :, : 2 * PART], ((1,), (0,)))
            w_d = jnp.concatenate([wgt[s0, :, 2 * PART :], wgt[s1, :, 2 * PART :]], axis=1)
            d = dot_f32(rows[1, at, :], w_d, ((1,), (0,)))

            @pl.when(n < 3)
            def _():
                psend[n, s0, part(p), : 2 * PART] = g0.astype(BF16)
                psend[n, s1, part(p), : 2 * PART] = g1.astype(BF16)
                psend[n, s0, part(p), 2 * PART :] = d[:, :PART].astype(BF16)
                psend[n, s1, part(p), 2 * PART :] = d[:, PART:].astype(BF16)

            @pl.when(n == 3)
            def _():
                pown[s0, part(p), : 2 * PART] = g0
                pown[s1, part(p), : 2 * PART] = g1
                pown[s0, part(p), 2 * PART :] = d[:, :PART]
                pown[s1, part(p), 2 * PART :] = d[:, PART:]

            for m, kinds in ((0, ("far_r", "far_l")), (1, ("nr_raw",)), (2, ("nl_raw",))):

                @pl.when(n == m)
                def _():
                    for s in (s0, s1):
                        for kind in kinds:
                            rs(kind, p, s).start()

            return carry

        lax.fori_loop(0, 4, one, 0)

    def logits():
        cols = router[:, pl.ds(pl.multiple_of(y * D, 128), D)]

        def one(n, carry):
            t = (y + jnp.where(n == 0, 2, jnp.where(n == 1, 1, jnp.where(n == 2, 3, 0)))) % 4
            at = pl.ds(pl.multiple_of(t * CAP, 16), CAP)
            lsend[n, :, :CAP] = dot_f32(cols, rows[0, at, :], ((1,), (1,)))
            return carry

        lax.fori_loop(0, 4, one, 0)
        for r in range(3):
            start(logit(r))

    def relay(p, s):
        for side, slot, rel in (("far_r", 1, "nr_rel"), ("far_l", 2, "nl_rel")):
            at = quarter(2 * p + (side == "far_l"))
            rs(side, p, s).wait_recv()
            total = psend[slot, s, at, :].astype(F32) + prelay[s, at, :].astype(F32)
            psend[slot, s, at, :] = total.astype(BF16)
            rs(rel, p, s).start()

    def gates():
        for r in range(3):
            logit(r).wait_recv()
        total = (lsend[3] + lrecv[0]) + (lrecv[1] + lrecv[2])
        label = labels[:8] - 1.0
        experts = lax.broadcasted_iota(jnp.int32, (8, 512), 0).astype(F32)
        picked = jnp.sum(jnp.where(label == experts, total, 0.0), axis=0, keepdims=True)
        margin = total[:1] - picked
        row = jnp.where(label[:1] > -0.5, jax.nn.sigmoid(margin), 0.0)
        gate[...] = jnp.transpose(jnp.broadcast_to(row, (PART, 512)))
        sacc[...] = jnp.zeros_like(sacc)

    def ag(kind, p, s):
        q = 2 * p + (kind in ("own_r1", "own_l1", "fwd_l"))
        t = {"own": y, "fwd": yl if kind == "fwd_r" else yr}[kind[:3]]
        to = yr if kind[4] == "r" else yl
        at = mids.at[s, pl.ds(pl.multiple_of(t * CAP + Q0[q], 16), QN[q]), :]
        return copy_at(ag_base + (p * 4 + s) * 6 + AG_KINDS.index(kind), at, at, y=to)

    def pointwise(p, s):
        for kind in RS_KINDS[2:]:
            rs(kind, p, s).wait_recv()
        for q in (2 * p, 2 * p + 1):
            at = quarter(q)
            near = precv[0, s, at, :].astype(F32) + precv[1, s, at, :].astype(F32)
            now = pown[s, at, :] + near
            g, up, raw = now[:, :PART], now[:, PART : 2 * PART], now[:, 2 * PART :]
            sigma = jax.nn.sigmoid(g)
            active = g * sigma
            slope = sigma * (1.0 + g * (1.0 - sigma))
            product = active * up
            scale = gate[at, :]
            sacc[at, :] += product * raw
            upstream = scale * raw
            to = pl.ds(pl.multiple_of(y * CAP + Q0[q], 16), QN[q])
            mids[s, to, :PART] = (upstream * up * slope).astype(BF16)
            mids[s, to, PART : 2 * PART] = (upstream * active).astype(BF16)
            mids[s, to, 2 * PART :] = (scale * product).astype(BF16)
        for kind in AG_KINDS[:4]:
            ag(kind, p, s).start()

    def forward(p, s):
        for kind, fwd in (("own_r0", "fwd_r"), ("own_l1", "fwd_l")):
            ag(kind, p, s).wait_recv()
            ag(fwd, p, s).start()

    def near(p, s):
        ag("own_r1", p, s).wait_recv()
        ag("own_l0", p, s).wait_recv()

    def far(p, s):
        ag("fwd_r", p, s).wait_recv()
        ag("fwd_l", p, s).wait_recv()

    def exchange(s, half=None):
        at = pl.ds(0, own) if half is None else pl.ds(half * (own // 2), own // 2)
        return copy(("gz", s, half), gsend.at[s, at, :], grecv.at[s, at, :], zl=1 - zl)

    def grads_tile(s, at):
        gu = dot_f32(rows[0, :, pl.ds(at, 256)], mids[s, :, : 2 * PART], ((0,), (0,)))
        return gu, dot_f32(rows[1, :, pl.ds(at, 256)], mids[s, :, 2 * PART :], ((0,), (0,)))

    def grads_theirs(s):
        def one(i, carry):
            gu, d = grads_tile(s, pl.multiple_of((1 - zl) * own + i * 256, 256))
            to = pl.ds(pl.multiple_of(i * 256, 256), 256)
            gsend[s, to, : 2 * PART] = gu.astype(BF16)
            gsend[s, to, 2 * PART :] = d.astype(BF16)
            return carry

        lax.fori_loop(0, own // 256, one, 0)

    def grads_mine(s):
        def one(i, carry):
            gu, d = grads_tile(s, pl.multiple_of(zl * own + i * 256, 256))
            to = pl.ds(pl.multiple_of(i * 256, 256), 256)
            for g in range(2):
                acc[3 * s + g, to, :] = gu[:, PART * g : PART * (g + 1)]
            acc[3 * s + 2, to, :] = d
            return carry

        lax.fori_loop(0, own // 256, one, 0)

    def add_grads(s, half=None):
        exchange(s, half).wait_recv()

        def one(i, carry):
            at = pl.ds(pl.multiple_of(i * 64, 16), 64)
            got = grecv[s, at, :].astype(F32)
            for g in range(3):
                acc[3 * s + g, at, :] += got[:, PART * g : PART * (g + 1)]
            return carry

        count = own // 64
        if half is None:
            lax.fori_loop(0, count, one, 0)
        else:
            lax.fori_loop(half * (count // 2), (half + 1) * (count // 2), one, 0)
        at = pl.ds(0, own) if half is None else pl.ds(half * (own // 2), own // 2)
        put_out(acc.at[pl.ds(3 * s, 3), at, :], acc_out.at[pl.ds(3 * s, 3), at, :])

    def score(key):
        src, dst, to = {
            "c": (0, 0, dict(c=1 - c)), "zh": (1, 1, dict(zh=1 - zh)),
            "x0": (2, 2, dict(x=xr)), "x1": (2, 3, dict(x=xl)), "x2": (2, 4, dict(x=xo)),
        }[key]
        return copy(("sc", key), srow.at[src], srecv.at[dst], **to)

    def scores():
        summed = jnp.sum(jnp.transpose(sacc[...]), axis=0, keepdims=True)
        srow[0] = jnp.broadcast_to(summed, (8, 512))
        start(score("c"))

    def scores_zh():
        score("c").wait_recv()
        srow[1] = srow[0] + srecv[0]
        start(score("zh"))

    def scores_x():
        score("zh").wait_recv()
        srow[2] = srow[1] + srecv[1]
        for key in ("x0", "x1", "x2"):
            start(score(key))

    def scores_end():
        for key in ("x0", "x1", "x2"):
            score(key).wait_recv()
        exact = ((srow[2] + srecv[2]) + (srecv[3] + srecv[4]))[0:1, :CAP]
        high = exact.astype(BF16).astype(F32)
        middle = (exact - high).astype(BF16).astype(F32)
        at = lax.broadcasted_iota(jnp.int32, (16, CAP), 0)
        split = jnp.where(at == 0, high, jnp.where(at == 1, middle, exact - high - middle))
        split = jnp.where(at < 3, split, 0.0).astype(BF16)
        parts = dot_f32(split, select[...], ((1,), (0,)))
        value = parts[0:1] + (parts[1:2] + parts[2:3])
        column = lax.broadcasted_iota(jnp.int32, (8, total), 0)
        chosen = jnp.where(column == 0, meta[2:3, :], meta[3:4, :])
        comb[...] = jnp.where(chosen > 0, value, 0.0)
        put_out(comb, comb_out)

    pair_base = index("pair", 16)

    def pair(p, i):
        src = psend.at[i // 4, i % 4, part(p), :]
        return copy_at(pair_base + p * 8 + i, src, brecv.at[i, part(p), :], c=1 - c)

    def ring(kind, half, p):
        at = part(p)
        src, dst, to = {
            "far_r": lambda: (bown.at[xo, half, at, :], xrelay.at[0, at, :], xr),
            "far_l": lambda: (bown.at[xo, half, at, :], xrelay.at[1, at, :], xl),
            "near_r": lambda: (bown.at[xr, half, at, :], xrecv.at[0, half, at, :], xr),
            "near_l": lambda: (bown.at[xl, half, at, :], xrecv.at[1, half, at, :], xl),
        }[kind]()
        return copy(("bx", kind, half, p), src, dst, x=to)

    def last(p):
        return copy(("bz", p), zsend.at[part(p), :], zrecv.at[part(p), :], zh=1 - zh)

    def home(p):
        return copy(("home", p), fsend.at[part(p), :], fin.at[part(p), :], **swap)

    def add_rows(p, out, refs):
        for q in (2 * p, 2 * p + 1):
            at = quarter(q)
            total = refs[0][at, :].astype(F32)
            for ref in refs[1:]:
                total = total + ref[at, :].astype(F32)
            out[at, :] = total.astype(out.dtype)

    def back_block(p, t):
        k = t // 2

        def one(b, carry):
            x_ = 2 * (t % 2) + b
            col = pl.multiple_of(b * 2 * SUB, 128)
            acc = None
            for sub in range(4):
                m = mids[sub, pl.ds(pl.multiple_of(t * CAP + P0[p], 16), PN[p]), : 2 * PART]
                w = wgt[sub, pl.ds(col, 2 * SUB), : 2 * PART]
                piece = dot_f32(m, w, ((1,), (1,)))
                acc = piece if acc is None else acc + piece
            low, high = acc[:, :SUB], acc[:, SUB:]
            i = x_ * 2 + k
            bown[x_, k, part(p), :] = jnp.where(c == 0, low, high).astype(BF16)
            psend[i // 4, i % 4, part(p), :] = jnp.where(c == 0, high, low).astype(BF16)
            pair(p, i).start()
            return carry

        lax.fori_loop(0, 2, one, 0)

    def back_sum(p, t):
        k = t // 2

        def one(b, carry):
            x_ = 2 * (t % 2) + b
            i = x_ * 2 + k
            r = (x_ - x + 4) % 4
            pair(p, i).wait_recv()
            add_rows(p, bown.at[x_, k], [bown.at[x_, k], brecv.at[i]])
            for r_, k_, kind in ((2, 0, "far_r"), (2, 1, "far_l"), (1, 1, "near_r"), (3, 0, "near_l")):

                @pl.when(jnp.logical_and(r == r_, k == k_))
                def _():
                    ring(kind, k_, p).start()

            return carry

        lax.fori_loop(0, 2, one, 0)

    def ring_relay(p):
        ring("far_r", 0, p).wait_recv()
        add_rows(p, bown.at[xr, 0], [bown.at[xr, 0], xrelay.at[0]])
        ring("near_r", 0, p).start()
        ring("far_l", 1, p).wait_recv()
        add_rows(p, bown.at[xl, 1], [bown.at[xl, 1], xrelay.at[1]])
        ring("near_l", 1, p).start()

    def ring_end(p):
        for half in range(2):
            for kind in ("near_r", "near_l"):
                ring(kind, half, p).wait_recv()
        add_rows(p, zsend, [bown.at[x, 1 - zh], xrecv.at[0, 1 - zh], xrecv.at[1, 1 - zh]])
        start(last(p))

    def go_home(p):
        last(p).wait_recv()
        add_rows(p, fsend, [bown.at[x, zh], xrecv.at[0, zh], xrecv.at[1, zh], zrecv])

        @pl.when(fixed)
        def _():
            fin[part(p), :] = fsend[part(p), :]

        @pl.when(moves)
        def _():
            home(p).start()

    arrive("xr0", 0, "xro", "c_xr0")
    arrive("xl0", 0, "c_xl0")
    arrive("zh", 0, "xr1", "xl1", "c_zh")
    arrive("xr0", 1, "xro", "c_xr0")
    arrive("xl0", 1, "c_xl0")
    arrive("zh", 1, "xr1", "xl1", "c_zh")
    arrive("xl1", 0, "xlo", "c_xl1")
    arrive("xro", 0, "c_xro")
    arrive("xr1", 0, "c_xr1")
    arrive("xl1", 1, "xlo", "c_xl1")
    arrive("xlo", 0, "c_xlo")
    weights(0).wait_recv()
    weights(1).wait_recv()
    all_cores(0)
    pre(0, 0)
    arrive("xro", 1, "c_xro")
    arrive("xr1", 1, "c_xr1")
    arrive("xlo", 1, "c_xlo")
    all_cores(1)
    pre(1, 0)
    logits()
    for p in range(2):
        for s in range(2):
            relay(p, s)
    gates()
    pointwise(0, 0)
    pointwise(0, 1)
    weights(2).wait_recv()
    weights(3).wait_recv()
    pre(0, 1)
    pointwise(1, 0)
    pointwise(1, 1)
    forward(0, 0)
    forward(0, 1)
    pre(1, 1)
    relay(0, 2)
    relay(0, 3)
    forward(1, 0)
    forward(1, 1)
    relay(1, 2)
    relay(1, 3)
    for p in range(2):
        near(p, 0)
        far(p, 0)
    grads_theirs(0)
    start(exchange(0))
    pointwise(0, 2)
    for p in range(2):
        near(p, 1)
        far(p, 1)
    grads_theirs(1)
    start(exchange(1))
    pointwise(1, 2)
    forward(0, 2)
    pointwise(0, 3)
    forward(1, 2)
    pointwise(1, 3)
    for kind in RS_KINDS:
        for p in range(2):
            for s in range(4):
                rs(kind, p, s).wait_send()
    scores()
    grads_mine(0)
    back_block(0, y)
    forward(0, 3)
    grads_mine(1)
    scores_zh()
    for p in range(2):
        near(p, 2)
        far(p, 2)
    grads_theirs(2)
    start(exchange(2))
    forward(1, 3)
    near(0, 3)
    back_block(0, yr)
    back_block(0, yl)
    far(0, 3)
    back_block(0, yo)
    back_sum(0, y)
    back_sum(0, yr)
    back_sum(0, yl)
    back_sum(0, yo)
    back_block(1, y)
    near(1, 3)
    back_block(1, yr)
    back_block(1, yl)
    far(1, 3)
    back_block(1, yo)
    back_sum(1, y)
    back_sum(1, yr)
    back_sum(1, yl)
    back_sum(1, yo)
    ring_relay(0)
    grads_theirs(3)
    start(exchange(3, 0))
    ring_relay(1)
    ring_end(0)
    start(exchange(3, 1))
    scores_x()
    add_grads(0)
    add_grads(1)
    grads_mine(2)
    ring_end(1)
    go_home(0)
    grads_mine(3)
    add_grads(2)
    scores_end()
    go_home(1)

    @pl.when(moves)
    def _():
        home(0).wait_recv()
        home(1).wait_recv()

    put_out(fin, fin_out)

    add_grads(3, 0)
    add_grads(3, 1)

    @pl.when(moves)
    def _():
        for p in range(2):
            move(p).wait_send()
            home(p).wait_send()

    for kind in AG_KINDS:
        for p in range(2):
            for s in range(4):
                ag(kind, p, s).wait_send()
    for key in number:
        if key[0] == "bx":
            ring(*key[1:]).wait_send()
    for p in range(2):
        for i in range(8):
            pair(p, i).wait_send()
    for cp in started:
        cp.wait_send()
    for cp in leave:
        cp.wait()


def finish(ranks, fin, combine, sums):
    total, own = ranks.shape[1], sums.shape[1]
    steps = 4
    tile, deep = total // steps, own // steps

    def body(ranks_ref, fin_ref, comb_ref, sums_ref, gtok_ref, comb_out, gu_out, down_out):
        for s in range(4):
            for g in range(2):
                gu_out[pl.ds(2 * s + g, deep, stride=8), :] = sums_ref[3 * s + g]
            down_out[:, PART * s : PART * (s + 1)] = sums_ref[3 * s + 2]
        comb_out[...] = comb_ref[0:2, :]
        slots = lax.broadcasted_iota(jnp.int32, (CAP, tile), 0)
        select = jnp.where(slots == ranks_ref[0:1, :], 1.0, 0.0).astype(BF16)
        gtok_ref[...] = dot_f32(select, fin_ref[...], ((0,), (0,))).astype(BF16)

    cols = lambda n: pl.BlockSpec((n, tile), lambda i: (0, i))
    rows = lambda n, m: pl.BlockSpec((n, m), lambda i: (i, 0))
    return pl.pallas_call(
        body,
        grid=(steps,),
        out_shape=(
            jax.ShapeDtypeStruct((total, SUB), BF16),
            jax.ShapeDtypeStruct((2, total), F32),
            jax.ShapeDtypeStruct((own * 8, PART), F32),
            jax.ShapeDtypeStruct((own, 4 * PART), F32),
        ),
        in_specs=[
            cols(8),
            pl.BlockSpec(fin.shape, lambda i: (0, 0)),
            cols(8),
            pl.BlockSpec((12, deep, PART), lambda i: (0, i, 0)),
        ],
        out_specs=[rows(tile, SUB), cols(2), rows(deep * 8, PART), rows(deep, 4 * PART)],
        cost_estimate=pl.CostEstimate(flops=2 * total * CAP * SUB, bytes_accessed=12 << 20, transcendentals=0),
    )(ranks, fin, combine, sums)


def exchange_and_compute(tokens, cotangent, gate_up, down_w, router, choice):
    own = down_w.shape[0]
    rows_all = 4 * CAP
    vm = pltpu.VMEM
    piece = (CAP, SUB)
    flops = 2 * rows_all * 2 * own * 4 * SUB * 8 // 3
    return pl.pallas_call(
        kernel,
        out_shape=(
            jax.ShapeDtypeStruct(piece, BF16),
            jax.ShapeDtypeStruct((8, tokens.shape[0]), F32),
            jax.ShapeDtypeStruct((8, tokens.shape[0]), jnp.int32),
            jax.ShapeDtypeStruct((12, own, PART), F32),
        ),
        in_specs=[pl.BlockSpec(memory_space=vm)] * 6,
        out_specs=[pl.BlockSpec(memory_space=pl.ANY)] * 4,
        scratch_shapes=[
            vm((CAP, tokens.shape[0]), BF16),
            vm((2,) + piece, BF16),
            vm((2, rows_all, 2 * own), BF16),
            vm((4, 2 * own, SUB), BF16),
            vm((3, 4) + piece, BF16),
            vm((4,) + piece, F32),
            vm((4,) + piece, BF16),
            vm((2, 4) + piece, BF16),
            vm((4, 8, 512), F32),
            vm((3, 8, 512), F32),
            vm((512, PART), F32),
            vm((512, PART), F32),
            vm((4, rows_all, SUB), BF16),
            vm((4, own, SUB), BF16),
            vm((4, own, SUB), BF16),
            vm((4, 2) + piece, BF16),
            vm((8,) + piece, BF16),
            vm((2,) + piece, BF16),
            vm((2, 2) + piece, BF16),
            vm(piece, BF16),
            vm(piece, BF16),
            vm(piece, BF16),
            vm(piece, BF16),
            vm((3, 8, 512), F32),
            vm((5, 8, 512), F32),
            vm((16, 512), F32),
            vm((8, tokens.shape[0]), jnp.int32),
            vm((16, PART), F32),
            vm((8, tokens.shape[0]), F32),
            vm((12, own, PART), F32),
            pltpu.SemaphoreType.DMA((192,)),
            pltpu.SemaphoreType.DMA((192,)),
            pltpu.SemaphoreType.DMA((8,)),
        ],
        cost_estimate=pl.CostEstimate(flops=flops, bytes_accessed=20 << 20, transcendentals=CAP * 512),
        compiler_params=pltpu.CompilerParams(
            collective_id=0, has_side_effects=True, vmem_limit_bytes=67043328
        ),
    )(tokens, cotangent, gate_up, down_w, router, choice)


def local(tokens, cotangent, expert_choice, router, gate_up, w_down):
    own, hid = w_down.shape
    fin, combine, ranks, sums = exchange_and_compute(
        tokens, cotangent, gate_up.reshape(own, 2 * hid), w_down, router, expert_choice.T
    )
    grad_tokens, combine, d_gu, d_down = finish(ranks, fin, combine, sums)
    d_gate_up = d_gu.reshape(own, hid // PART, 2, PART).transpose(0, 2, 1, 3).reshape(own, 2, hid)
    return (grad_tokens, combine.T, d_gate_up, d_down)


def solution(mesh):
    split = Mesh(mesh.devices.reshape(4, 2, 2, 4, 2), ALL)
    return jax.shard_map(
        local,
        mesh=split,
        in_specs=(
            P(TOK, HID),
            P(TOK, HID),
            P(TOK, None),
            P(),
            P(TOK, None, HID),
            P(TOK, HID),
        ),
        out_specs=(P(TOK, HID), P(TOK, None), P(TOK, None, HID), P(TOK, HID)),
        check_vma=False,
    )
```

```python
import jax
import jax.numpy as jnp
from jax import lax
from jax.experimental import pallas as pl
from jax.experimental.pallas import tpu as pltpu
from jax.sharding import Mesh
from jax.sharding import PartitionSpec as P

CAP = 432
SUB = 384
PART = 128
TOK = ("y", "zl")
HID = ("zh", "x", "c")
ALL = TOK + HID
MESH = pl.DeviceIdType.MESH
F32 = jnp.float32
BF16 = jnp.bfloat16


def dot_f32(left, right, dims):
    return lax.dot_general(left, right, ((dims[0], dims[1]), ((), ())), preferred_element_type=F32)


P0, PN = (0, 224), (224, 208)
Q0, QN = (0, 112, 224, 336), (112, 112, 112, 96)
RS_KINDS = ("far_r", "far_l", "nr_raw", "nl_raw", "nr_rel", "nl_rel")
AG_KINDS = ("own_r0", "own_l1", "own_r1", "own_l0", "fwd_r", "fwd_l")


def kernel(
    tokens, cotangent, gate_up, down_w, router, choice,
    fin_out, comb_out, rank_out, acc_out,
    select, xin, rows, wgt, psend, pown, prelay, precv, lsend, lrecv, gate, sacc, mids,
    gsend, grecv, bown, brecv, xrelay, xrecv, zsend, zrecv, fsend, fin, srow, srecv, labels, meta, flags, comb, acc,
    ssem, rsem, osem,
):
    y, zl, zh, x, c = (lax.axis_index(a) for a in ALL)
    yr, yl, yo = (y + 1) % 4, (y + 3) % 4, (y + 2) % 4
    xr, xl, xo = (x + 1) % 4, (x + 3) % 4, (x + 2) % 4
    D = rows.shape[2]
    own = D // 2
    swap_y, swap_zh, swap_x = 2 * zh + x // 2, y // 2, 2 * (y % 2) + x % 2
    fixed = swap_y == y
    moves = jnp.logical_not(fixed)
    swap = dict(y=swap_y, zh=swap_zh, x=swap_x)

    number = {}
    started = []

    def index(key, n=1):
        if key not in number:
            number[key] = number.get("next", 0)
            number["next"] = number[key] + n
        return number[key]

    def copy_at(i, src, dst, **to):
        return pltpu.make_async_remote_copy(
            src_ref=src, dst_ref=dst, send_sem=ssem.at[i], recv_sem=rsem.at[i],
            device_id=to, device_id_type=MESH,
        )

    def copy(key, src, dst, **to):
        return copy_at(index(key), src, dst, **to)

    def start(cp):
        cp.start()
        started.append(cp)
        return cp

    barrier = pltpu.get_barrier_semaphore()
    peers = (
        dict(y=yr), dict(y=yl), dict(y=yo), dict(zl=1 - zl), dict(zh=1 - zh),
        dict(x=xr), dict(x=xl), dict(x=xo), dict(c=1 - c),
    )
    for peer in peers:
        pl.semaphore_signal(barrier, inc=1, device_id=peer, device_id_type=MESH)

    @pl.when(moves)
    def _():
        pl.semaphore_signal(barrier, inc=1, device_id=swap, device_id_type=MESH)

    def place(p, zh_, x_, c_):
        row = pl.multiple_of((2 * zh_ + x_ // 2) * CAP + P0[p], 16)
        col = pl.multiple_of((2 * (x_ % 2) + c_) * SUB, 128)
        return rows.at[:, pl.ds(row, PN[p]), pl.ds(col, SUB)]

    def weights(sub):
        at = wgt.at[sub, pl.ds(pl.multiple_of(zl * own, 16), own), :]
        return copy(("w", sub), at, at, zl=1 - zl)

    def part(p):
        return pl.ds(P0[p], PN[p])

    def quarter(q):
        return pl.ds(Q0[q], QN[q])

    def move(p):
        return copy(("move", p), xin.at[:, part(p), :], place(p, swap_zh, swap_x, c), **swap)

    total = tokens.shape[0]
    first, second = choice[0:1, :], choice[1:2, :]
    routed = jnp.logical_or(first == 0, second == 0)
    hits = jnp.where(routed, 1.0, 0.0)
    flags[...] = jnp.zeros_like(flags)
    for i in range(total // PART):
        flags[i : i + 1, :] = hits[:, PART * i : PART * (i + 1)]
    lane = lax.broadcasted_iota(jnp.int32, (PART, PART), 0)
    before = jnp.where(lane < lax.broadcasted_iota(jnp.int32, (PART, PART), 1), 1.0, 0.0)
    line = lax.broadcasted_iota(jnp.int32, (16, 16), 0)
    above = jnp.where(line > lax.broadcasted_iota(jnp.int32, (16, 16), 1), 1.0, 0.0)
    marks = flags[...].astype(BF16)
    within = dot_f32(marks, before.astype(BF16), ((1,), (0,)))
    counts = dot_f32(marks, jnp.ones((PART, PART), BF16), ((1,), (0,)))
    flags[...] = within + dot_f32(above.astype(BF16), counts.astype(BF16), ((1,), (0,)))
    for i in range(total // PART):
        at = slice(PART * i, PART * (i + 1))
        rank = flags[i : i + 1, :].astype(jnp.int32)
        meta[0:1, at] = jnp.where(routed[:, at], rank, -1)
    meta[1:2, :] = first + second + 1
    meta[2:3, :] = jnp.where(first == 0, 1, 0)
    meta[3:4, :] = jnp.where(second == 0, 1, 0)
    meta[4:8, :] = jnp.zeros((4, total), jnp.int32)
    leave = []

    def put_out(src, dst):
        cp = pltpu.make_async_copy(src, dst, osem.at[len(leave)])
        cp.start()
        leave.append(cp)

    put_out(meta, rank_out)

    def dispatch(p):
        slots = lax.broadcasted_iota(jnp.int32, (PN[p], total), 0) + P0[p]
        select[part(p), :] = jnp.where(slots == meta[0:1, :], 1.0, 0.0).astype(BF16)
        xin[0, part(p), :] = dot_f32(select[part(p), :], tokens[...], ((1,), (0,))).astype(BF16)
        xin[1, part(p), :] = dot_f32(select[part(p), :], cotangent[...], ((1,), (0,))).astype(BF16)

    def send(p):
        @pl.when(fixed)
        def _():
            place(p, zh, x, c)[...] = xin[:, part(p), :]

        @pl.when(moves)
        def _():
            move(p).start()

    dispatch(0)

    @pl.when(moves)
    def _():
        pl.semaphore_wait(barrier, len(peers) + 1)

    @pl.when(fixed)
    def _():
        pl.semaphore_wait(barrier, len(peers))

    send(0)
    dispatch(1)
    send(1)

    def put_weights(i, carry):
        at = pl.ds(pl.multiple_of(zl * own + i * 96, 16), 96)
        of = pl.ds(pl.multiple_of(i * 96, 16), 96)
        for sub in range(4):
            for n, (ref, base) in enumerate(((gate_up, 0), (gate_up, 512), (down_w, 0))):
                wgt[sub, at, PART * n : PART * (n + 1)] = ref[of, base + PART * sub : base + PART * (sub + 1)]
        return carry

    lax.fori_loop(0, own // 96, put_weights, 0)
    named = jnp.broadcast_to(meta[1:2, :].astype(F32).astype(BF16), (16, tokens.shape[0]))
    labels[:, :CAP] = dot_f32(named, select[...], ((1,), (1,)))

    steps = {
        "zh": (lambda p: place(p, zh, x, c), dict(zh=1 - zh)),
        "xr0": (lambda p: place(p, zh, x, c), dict(x=xr)),
        "xl0": (lambda p: place(p, zh, x, c), dict(x=xl)),
        "xro": (lambda p: place(p, zh, xl, c), dict(x=xr)),
        "xr1": (lambda p: place(p, 1 - zh, x, c), dict(x=xr)),
        "xl1": (lambda p: place(p, 1 - zh, x, c), dict(x=xl)),
        "xlo": (lambda p: place(p, 1 - zh, xr, c), dict(x=xl)),
        "c_own": (lambda p: place(p, zh, x, c), dict(c=1 - c)),
        "c_zh": (lambda p: place(p, 1 - zh, x, c), dict(c=1 - c)),
        "c_xr0": (lambda p: place(p, zh, xl, c), dict(c=1 - c)),
        "c_xl0": (lambda p: place(p, zh, xr, c), dict(c=1 - c)),
        "c_xr1": (lambda p: place(p, 1 - zh, xl, c), dict(c=1 - c)),
        "c_xl1": (lambda p: place(p, 1 - zh, xr, c), dict(c=1 - c)),
        "c_xro": (lambda p: place(p, zh, xo, c), dict(c=1 - c)),
        "c_xlo": (lambda p: place(p, 1 - zh, xo, c), dict(c=1 - c)),
    }

    def hop(name, p):
        at, to = steps[name]
        return copy((name, p), at(p), at(p), **to)

    def arrive(name, p, *then):
        hop(name, p).wait_recv()
        for follow in then:
            start(hop(follow, p))

    def all_cores(p):
        for name in steps:
            if name.startswith("c_"):
                hop(name, p).wait_recv()

    for p in range(2):

        @pl.when(moves)
        def _():
            move(p).wait_recv()

        for name in ("zh", "xr0", "xl0", "c_own"):
            start(hop(name, p))
    for sub in range(4):
        start(weights(sub))

    rs_base = index("rs", 48)
    ag_base = index("ag", 48)

    def rs(kind, p, s):
        q = 2 * p + (kind in ("far_l", "nr_raw", "nl_rel"))
        at = quarter(q)
        src, dst, to = {
            "fa": lambda: (psend.at[0, s, at, :], prelay.at[s, at, :], yr if kind == "far_r" else yl),
            "nr": lambda: (psend.at[1, s, at, :], precv.at[0, s, at, :], yr),
            "nl": lambda: (psend.at[2, s, at, :], precv.at[1, s, at, :], yl),
        }[kind[:2]]()
        return copy_at(rs_base + (p * 4 + s) * 6 + RS_KINDS.index(kind), src, dst, y=to)

    def logit(r):
        to = (yo, yr, yl)[r]
        return copy(("lg", r), lsend.at[r], lrecv.at[r], y=to)

    def pre_send(p, j):
        for kind in RS_KINDS[:4]:
            for s in (2 * j, 2 * j + 1):
                rs(kind, p, s).start()

    def pre(p, j, held=False):
        s0, s1 = 2 * j, 2 * j + 1

        def one(n, carry):
            r = jnp.where(n == 0, 2, jnp.where(n == 1, 1, jnp.where(n == 2, 3, 0)))
            t = (y + r) % 4
            at = pl.ds(pl.multiple_of(t * CAP + P0[p], 16), PN[p])
            x_in = rows[0, at, :]
            g0 = dot_f32(x_in, wgt[s0, :, : 2 * PART], ((1,), (0,)))
            g1 = dot_f32(x_in, wgt[s1, :, : 2 * PART], ((1,), (0,)))
            w_d = jnp.concatenate([wgt[s0, :, 2 * PART :], wgt[s1, :, 2 * PART :]], axis=1)
            d = dot_f32(rows[1, at, :], w_d, ((1,), (0,)))

            @pl.when(n < 3)
            def _():
                psend[n, s0, part(p), : 2 * PART] = g0.astype(BF16)
                psend[n, s1, part(p), : 2 * PART] = g1.astype(BF16)
                psend[n, s0, part(p), 2 * PART :] = d[:, :PART].astype(BF16)
                psend[n, s1, part(p), 2 * PART :] = d[:, PART:].astype(BF16)

            @pl.when(n == 3)
            def _():
                pown[s0, part(p), : 2 * PART] = g0
                pown[s1, part(p), : 2 * PART] = g1
                pown[s0, part(p), 2 * PART :] = d[:, :PART]
                pown[s1, part(p), 2 * PART :] = d[:, PART:]

            for m, kinds in () if held else ((0, ("far_r", "far_l")), (1, ("nr_raw",)), (2, ("nl_raw",))):

                @pl.when(n == m)
                def _():
                    for s in (s0, s1):
                        for kind in kinds:
                            rs(kind, p, s).start()

            return carry

        lax.fori_loop(0, 4, one, 0)

    def logits():
        cols = router[:, pl.ds(pl.multiple_of(y * D, 128), D)]

        def one(n, carry):
            t = (y + jnp.where(n == 0, 2, jnp.where(n == 1, 1, jnp.where(n == 2, 3, 0)))) % 4
            at = pl.ds(pl.multiple_of(t * CAP, 16), CAP)
            lsend[n, :, :CAP] = dot_f32(cols, rows[0, at, :], ((1,), (1,)))
            return carry

        lax.fori_loop(0, 4, one, 0)
        for r in range(3):
            start(logit(r))

    def relay(p, s):
        for side, slot, rel in (("far_r", 1, "nr_rel"), ("far_l", 2, "nl_rel")):
            at = quarter(2 * p + (side == "far_l"))
            rs(side, p, s).wait_recv()
            total = psend[slot, s, at, :].astype(F32) + prelay[s, at, :].astype(F32)
            psend[slot, s, at, :] = total.astype(BF16)
            rs(rel, p, s).start()

    def gates():
        for r in range(3):
            logit(r).wait_recv()
        total = (lsend[3] + lrecv[0]) + (lrecv[1] + lrecv[2])
        label = labels[:8] - 1.0
        experts = lax.broadcasted_iota(jnp.int32, (8, 512), 0).astype(F32)
        picked = jnp.sum(jnp.where(label == experts, total, 0.0), axis=0, keepdims=True)
        margin = total[:1] - picked
        row = jnp.where(label[:1] > -0.5, jax.nn.sigmoid(margin), 0.0)
        gate[...] = jnp.transpose(jnp.broadcast_to(row, (PART, 512)))
        sacc[...] = jnp.zeros_like(sacc)

    def ag(kind, p, s):
        q = 2 * p + (kind in ("own_r1", "own_l1", "fwd_l"))
        t = {"own": y, "fwd": yl if kind == "fwd_r" else yr}[kind[:3]]
        to = yr if kind[4] == "r" else yl
        at = mids.at[s, pl.ds(pl.multiple_of(t * CAP + Q0[q], 16), QN[q]), :]
        return copy_at(ag_base + (p * 4 + s) * 6 + AG_KINDS.index(kind), at, at, y=to)

    def pointwise(p, s):
        for kind in RS_KINDS[2:]:
            rs(kind, p, s).wait_recv()
        for q in (2 * p, 2 * p + 1):
            at = quarter(q)
            near = precv[0, s, at, :].astype(F32) + precv[1, s, at, :].astype(F32)
            now = pown[s, at, :] + near
            g, up, raw = now[:, :PART], now[:, PART : 2 * PART], now[:, 2 * PART :]
            sigma = jax.nn.sigmoid(g)
            active = g * sigma
            slope = sigma * (1.0 + g * (1.0 - sigma))
            product = active * up
            scale = gate[at, :]
            sacc[at, :] += product * raw
            upstream = scale * raw
            to = pl.ds(pl.multiple_of(y * CAP + Q0[q], 16), QN[q])
            mids[s, to, :PART] = (upstream * up * slope).astype(BF16)
            mids[s, to, PART : 2 * PART] = (upstream * active).astype(BF16)
            mids[s, to, 2 * PART :] = (scale * product).astype(BF16)
        for kind in AG_KINDS[:4]:
            ag(kind, p, s).start()

    def forward(p, s):
        for kind, fwd in (("own_r0", "fwd_r"), ("own_l1", "fwd_l")):
            ag(kind, p, s).wait_recv()
            ag(fwd, p, s).start()

    def near(p, s):
        ag("own_r1", p, s).wait_recv()
        ag("own_l0", p, s).wait_recv()

    def far(p, s):
        ag("fwd_r", p, s).wait_recv()
        ag("fwd_l", p, s).wait_recv()

    def exchange(s, half=None):
        at = pl.ds(0, own) if half is None else pl.ds(half * (own // 4), own // 4)
        return copy(("gz", s, half), gsend.at[s, at, :], grecv.at[s, at, :], zl=1 - zl)

    def grads_tile(s, at):
        gu = dot_f32(rows[0, :, pl.ds(at, 256)], mids[s, :, : 2 * PART], ((0,), (0,)))
        return gu, dot_f32(rows[1, :, pl.ds(at, 256)], mids[s, :, 2 * PART :], ((0,), (0,)))

    def grads_theirs(s):
        def one(i, carry):
            gu, d = grads_tile(s, pl.multiple_of((1 - zl) * own + i * 256, 256))
            to = pl.ds(pl.multiple_of(i * 256, 256), 256)
            gsend[s, to, : 2 * PART] = gu.astype(BF16)
            gsend[s, to, 2 * PART :] = d.astype(BF16)
            return carry

        lax.fori_loop(0, own // 256, one, 0)

    def grads_mine(s):
        def one(i, carry):
            gu, d = grads_tile(s, pl.multiple_of(zl * own + i * 256, 256))
            to = pl.ds(pl.multiple_of(i * 256, 256), 256)
            for g in range(2):
                acc[3 * s + g, to, :] = gu[:, PART * g : PART * (g + 1)]
            acc[3 * s + 2, to, :] = d
            return carry

        lax.fori_loop(0, own // 256, one, 0)

    def add_grads(s, half=None):
        exchange(s, half).wait_recv()

        def one(i, carry):
            at = pl.ds(pl.multiple_of(i * 64, 16), 64)
            got = grecv[s, at, :].astype(F32)
            for g in range(3):
                acc[3 * s + g, at, :] += got[:, PART * g : PART * (g + 1)]
            return carry

        count = own // 64
        if half is None:
            lax.fori_loop(0, count, one, 0)
        else:
            lax.fori_loop(half * (count // 4), (half + 1) * (count // 4), one, 0)
        at = pl.ds(0, own) if half is None else pl.ds(half * (own // 4), own // 4)
        put_out(acc.at[pl.ds(3 * s, 3), at, :], acc_out.at[pl.ds(3 * s, 3), at, :])

    def score(key):
        src, dst, to = {
            "c": (0, 0, dict(c=1 - c)), "zh": (1, 1, dict(zh=1 - zh)),
            "x0": (2, 2, dict(x=xr)), "x1": (2, 3, dict(x=xl)), "x2": (2, 4, dict(x=xo)),
        }[key]
        return copy(("sc", key), srow.at[src], srecv.at[dst], **to)

    def scores():
        summed = jnp.sum(jnp.transpose(sacc[...]), axis=0, keepdims=True)
        srow[0] = jnp.broadcast_to(summed, (8, 512))
        start(score("c"))

    def scores_zh():
        score("c").wait_recv()
        srow[1] = srow[0] + srecv[0]
        start(score("zh"))

    def scores_x():
        score("zh").wait_recv()
        srow[2] = srow[1] + srecv[1]
        for key in ("x0", "x1", "x2"):
            start(score(key))

    def scores_end():
        for key in ("x0", "x1", "x2"):
            score(key).wait_recv()
        exact = ((srow[2] + srecv[2]) + (srecv[3] + srecv[4]))[0:1, :CAP]
        high = exact.astype(BF16).astype(F32)
        middle = (exact - high).astype(BF16).astype(F32)
        at = lax.broadcasted_iota(jnp.int32, (16, CAP), 0)
        split = jnp.where(at == 0, high, jnp.where(at == 1, middle, exact - high - middle))
        split = jnp.where(at < 3, split, 0.0).astype(BF16)
        parts = dot_f32(split, select[...], ((1,), (0,)))
        value = parts[0:1] + (parts[1:2] + parts[2:3])
        column = lax.broadcasted_iota(jnp.int32, (8, total), 0)
        chosen = jnp.where(column == 0, meta[2:3, :], meta[3:4, :])
        comb[...] = jnp.where(chosen > 0, value, 0.0)
        put_out(comb, comb_out)

    pair_base = index("pair", 16)

    def pair(p, i):
        src = psend.at[i // 4, i % 4, part(p), :]
        return copy_at(pair_base + p * 8 + i, src, brecv.at[i, part(p), :], c=1 - c)

    def ring(kind, half, p):
        at = part(p)
        src, dst, to = {
            "far_r": lambda: (bown.at[xo, half, at, :], xrelay.at[0, at, :], xr),
            "far_l": lambda: (bown.at[xo, half, at, :], xrelay.at[1, at, :], xl),
            "near_r": lambda: (bown.at[xr, half, at, :], xrecv.at[0, half, at, :], xr),
            "near_l": lambda: (bown.at[xl, half, at, :], xrecv.at[1, half, at, :], xl),
        }[kind]()
        return copy(("bx", kind, half, p), src, dst, x=to)

    def last(p):
        return copy(("bz", p), zsend.at[part(p), :], zrecv.at[part(p), :], zh=1 - zh)

    def home(p):
        return copy(("home", p), fsend.at[part(p), :], fin.at[part(p), :], **swap)

    def add_rows(p, out, refs):
        for q in (2 * p, 2 * p + 1):
            at = quarter(q)
            total = refs[0][at, :].astype(F32)
            for ref in refs[1:]:
                total = total + ref[at, :].astype(F32)
            out[at, :] = total.astype(out.dtype)

    def back_blocks(*blocks):
        def one(b, carry):
            col = pl.multiple_of(b * 2 * SUB, 128)
            lines = []
            for p, t in blocks:
                at = pl.ds(pl.multiple_of(t * CAP + P0[p], 16), PN[p])
                lines.append(jnp.concatenate([mids[sub, at, : 2 * PART] for sub in range(4)], axis=1))
            m = jnp.concatenate(lines, axis=0)
            w = jnp.concatenate([wgt[sub, pl.ds(col, 2 * SUB), : 2 * PART] for sub in range(4)], axis=1)
            piece = dot_f32(m, w, ((1,), (1,)))
            low, high = piece[:, :SUB], piece[:, SUB:]
            mine = jnp.where(c == 0, low, high).astype(BF16)
            theirs = jnp.where(c == 0, high, low).astype(BF16)
            base = 0
            for p, t in blocks:
                k = t // 2
                x_ = 2 * (t % 2) + b
                i = x_ * 2 + k
                bown[x_, k, part(p), :] = mine[base : base + PN[p]]
                psend[i // 4, i % 4, part(p), :] = theirs[base : base + PN[p]]
                base += PN[p]
                pair(p, i).start()
            return carry

        lax.fori_loop(0, 2, one, 0)

    def back_sum(p, t):
        k = t // 2

        def one(b, carry):
            x_ = 2 * (t % 2) + b
            i = x_ * 2 + k
            r = (x_ - x + 4) % 4
            pair(p, i).wait_recv()
            add_rows(p, bown.at[x_, k], [bown.at[x_, k], brecv.at[i]])
            for r_, k_, kind in ((2, 0, "far_r"), (2, 1, "far_l"), (1, 1, "near_r"), (3, 0, "near_l")):

                @pl.when(jnp.logical_and(r == r_, k == k_))
                def _():
                    ring(kind, k_, p).start()

            return carry

        lax.fori_loop(0, 2, one, 0)

    def ring_relay(p):
        ring("far_r", 0, p).wait_recv()
        add_rows(p, bown.at[xr, 0], [bown.at[xr, 0], xrelay.at[0]])
        ring("near_r", 0, p).start()
        ring("far_l", 1, p).wait_recv()
        add_rows(p, bown.at[xl, 1], [bown.at[xl, 1], xrelay.at[1]])
        ring("near_l", 1, p).start()

    def ring_end(p):
        for half in range(2):
            for kind in ("near_r", "near_l"):
                ring(kind, half, p).wait_recv()
        add_rows(p, zsend, [bown.at[x, 1 - zh], xrecv.at[0, 1 - zh], xrecv.at[1, 1 - zh]])
        start(last(p))

    def go_home(p):
        last(p).wait_recv()
        add_rows(p, fsend, [bown.at[x, zh], xrecv.at[0, zh], xrecv.at[1, zh], zrecv])

        @pl.when(fixed)
        def _():
            fin[part(p), :] = fsend[part(p), :]

        @pl.when(moves)
        def _():
            home(p).start()

    arrive("xr0", 0, "xro", "c_xr0")
    arrive("xl0", 0, "c_xl0")
    arrive("zh", 0, "xr1", "xl1", "c_zh")
    arrive("xr0", 1, "xro", "c_xr0")
    arrive("xl0", 1, "c_xl0")
    arrive("zh", 1, "xr1", "xl1", "c_zh")
    arrive("xl1", 0, "xlo", "c_xl1")
    arrive("xro", 0, "c_xro")
    arrive("xr1", 0, "c_xr1")
    arrive("xl1", 1, "xlo", "c_xl1")
    arrive("xlo", 0, "c_xlo")
    weights(0).wait_recv()
    weights(1).wait_recv()
    all_cores(0)
    pre(0, 0)
    arrive("xro", 1, "c_xro")
    arrive("xr1", 1, "c_xr1")
    arrive("xlo", 1, "c_xlo")
    all_cores(1)
    pre(1, 0)
    logits()
    for p in range(2):
        for s in range(2):
            relay(p, s)
    gates()
    pointwise(0, 0)
    pointwise(0, 1)
    pointwise(1, 0)
    pointwise(1, 1)
    forward(0, 0)
    forward(0, 1)
    weights(2).wait_recv()
    weights(3).wait_recv()
    pre(0, 1, held=True)
    forward(1, 0)
    forward(1, 1)
    pre_send(0, 1)
    pre(1, 1)
    for p in range(2):
        near(p, 0)
        far(p, 0)
    grads_theirs(0)
    start(exchange(0))
    relay(0, 2)
    relay(0, 3)
    for p in range(2):
        near(p, 1)
        far(p, 1)
    grads_theirs(1)
    start(exchange(1))
    relay(1, 2)
    relay(1, 3)
    grads_mine(0)
    pointwise(0, 2)
    pointwise(1, 2)
    forward(0, 2)
    pointwise(0, 3)
    forward(1, 2)
    pointwise(1, 3)
    for kind in RS_KINDS:
        for p in range(2):
            for s in range(4):
                rs(kind, p, s).wait_send()
    scores()
    back_blocks((0, y), (1, y))
    forward(0, 3)
    for p in range(2):
        near(p, 2)
        far(p, 2)
    grads_theirs(2)
    start(exchange(2))
    scores_zh()
    forward(1, 3)
    near(0, 3)
    back_blocks((0, yr), (0, yl))
    far(0, 3)
    back_blocks((0, yo),)
    back_sum(0, y)
    back_sum(0, yr)
    back_sum(0, yl)
    back_sum(0, yo)
    near(1, 3)
    back_blocks((1, yr), (1, yl))
    far(1, 3)
    grads_theirs(3)
    start(exchange(3, 0))
    start(exchange(3, 1))
    back_blocks((1, yo),)
    back_sum(1, y)
    back_sum(1, yr)
    back_sum(1, yl)
    back_sum(1, yo)
    ring_relay(0)
    ring_relay(1)
    ring_end(0)
    start(exchange(3, 2))
    scores_x()
    grads_mine(1)
    ring_end(1)
    start(exchange(3, 3))
    add_grads(0)
    add_grads(1)
    go_home(0)
    grads_mine(2)
    add_grads(2)
    scores_end()
    go_home(1)
    grads_mine(3)
    for quarter_ in range(4):
        add_grads(3, quarter_)

    @pl.when(moves)
    def _():
        home(0).wait_recv()
        home(1).wait_recv()

    put_out(fin, fin_out)

    @pl.when(moves)
    def _():
        for p in range(2):
            move(p).wait_send()
            home(p).wait_send()

    for kind in AG_KINDS:
        for p in range(2):
            for s in range(4):
                ag(kind, p, s).wait_send()
    for key in number:
        if key[0] == "bx":
            ring(*key[1:]).wait_send()
    for p in range(2):
        for i in range(8):
            pair(p, i).wait_send()
    for cp in started:
        cp.wait_send()
    for cp in leave:
        cp.wait()


def finish(ranks, fin, combine, sums):
    total, own = ranks.shape[1], sums.shape[1]
    steps = 4
    tile, deep = total // steps, own // steps

    def body(ranks_ref, fin_ref, comb_ref, sums_ref, gtok_ref, comb_out, gu_out, down_out):
        for s in range(4):
            for g in range(2):
                gu_out[pl.ds(2 * s + g, deep, stride=8), :] = sums_ref[3 * s + g]
            down_out[:, PART * s : PART * (s + 1)] = sums_ref[3 * s + 2]
        comb_out[...] = comb_ref[0:2, :]
        slots = lax.broadcasted_iota(jnp.int32, (CAP, tile), 0)
        select = jnp.where(slots == ranks_ref[0:1, :], 1.0, 0.0).astype(BF16)
        gtok_ref[...] = dot_f32(select, fin_ref[...], ((0,), (0,))).astype(BF16)

    cols = lambda n: pl.BlockSpec((n, tile), lambda i: (0, i))
    rows = lambda n, m: pl.BlockSpec((n, m), lambda i: (i, 0))
    return pl.pallas_call(
        body,
        grid=(steps,),
        out_shape=(
            jax.ShapeDtypeStruct((total, SUB), BF16),
            jax.ShapeDtypeStruct((2, total), F32),
            jax.ShapeDtypeStruct((own * 8, PART), F32),
            jax.ShapeDtypeStruct((own, 4 * PART), F32),
        ),
        in_specs=[
            cols(8),
            pl.BlockSpec(fin.shape, lambda i: (0, 0)),
            cols(8),
            pl.BlockSpec((12, deep, PART), lambda i: (0, i, 0)),
        ],
        out_specs=[rows(tile, SUB), cols(2), rows(deep * 8, PART), rows(deep, 4 * PART)],
        cost_estimate=pl.CostEstimate(flops=2 * total * CAP * SUB, bytes_accessed=12 << 20, transcendentals=0),
    )(ranks, fin, combine, sums)


def exchange_and_compute(tokens, cotangent, gate_up, down_w, router, choice):
    own = down_w.shape[0]
    rows_all = 4 * CAP
    vm = pltpu.VMEM
    piece = (CAP, SUB)
    flops = 2 * rows_all * 2 * own * 4 * SUB * 8 // 3
    return pl.pallas_call(
        kernel,
        out_shape=(
            jax.ShapeDtypeStruct(piece, BF16),
            jax.ShapeDtypeStruct((8, tokens.shape[0]), F32),
            jax.ShapeDtypeStruct((8, tokens.shape[0]), jnp.int32),
            jax.ShapeDtypeStruct((12, own, PART), F32),
        ),
        in_specs=[pl.BlockSpec(memory_space=vm)] * 6,
        out_specs=[pl.BlockSpec(memory_space=pl.ANY)] * 4,
        scratch_shapes=[
            vm((CAP, tokens.shape[0]), BF16),
            vm((2,) + piece, BF16),
            vm((2, rows_all, 2 * own), BF16),
            vm((4, 2 * own, SUB), BF16),
            vm((3, 4) + piece, BF16),
            vm((4,) + piece, F32),
            vm((4,) + piece, BF16),
            vm((2, 4) + piece, BF16),
            vm((4, 8, 512), F32),
            vm((3, 8, 512), F32),
            vm((512, PART), F32),
            vm((512, PART), F32),
            vm((4, rows_all, SUB), BF16),
            vm((4, own, SUB), BF16),
            vm((4, own, SUB), BF16),
            vm((4, 2) + piece, BF16),
            vm((8,) + piece, BF16),
            vm((2,) + piece, BF16),
            vm((2, 2) + piece, BF16),
            vm(piece, BF16),
            vm(piece, BF16),
            vm(piece, BF16),
            vm(piece, BF16),
            vm((3, 8, 512), F32),
            vm((5, 8, 512), F32),
            vm((16, 512), F32),
            vm((8, tokens.shape[0]), jnp.int32),
            vm((16, PART), F32),
            vm((8, tokens.shape[0]), F32),
            vm((12, own, PART), F32),
            pltpu.SemaphoreType.DMA((192,)),
            pltpu.SemaphoreType.DMA((192,)),
            pltpu.SemaphoreType.DMA((12,)),
        ],
        cost_estimate=pl.CostEstimate(flops=flops, bytes_accessed=20 << 20, transcendentals=CAP * 512),
        compiler_params=pltpu.CompilerParams(
            collective_id=0, has_side_effects=True, vmem_limit_bytes=67043328
        ),
    )(tokens, cotangent, gate_up, down_w, router, choice)


def local(tokens, cotangent, expert_choice, router, gate_up, w_down):
    own, hid = w_down.shape
    fin, combine, ranks, sums = exchange_and_compute(
        tokens, cotangent, gate_up.reshape(own, 2 * hid), w_down, router, expert_choice.T
    )
    grad_tokens, combine, d_gu, d_down = finish(ranks, fin, combine, sums)
    d_gate_up = d_gu.reshape(own, hid // PART, 2, PART).transpose(0, 2, 1, 3).reshape(own, 2, hid)
    return (grad_tokens, combine.T, d_gate_up, d_down)


def solution(mesh):
    split = Mesh(mesh.devices.reshape(4, 2, 2, 4, 2), ALL)
    return jax.shard_map(
        local,
        mesh=split,
        in_specs=(
            P(TOK, HID),
            P(TOK, HID),
            P(TOK, None),
            P(),
            P(TOK, None, HID),
            P(TOK, HID),
        ),
        out_specs=(P(TOK, HID), P(TOK, None), P(TOK, None, HID), P(TOK, HID)),
        check_vma=False,
    )
```

```python
import jax
import jax.numpy as jnp
from jax import lax
from jax.experimental import pallas as pl
from jax.experimental.pallas import tpu as pltpu
from jax.sharding import Mesh
from jax.sharding import PartitionSpec as P

CAP = 432
SUB = 384
PART = 128
TOK = ("y", "zl")
HID = ("zh", "x", "c")
ALL = TOK + HID
MESH = pl.DeviceIdType.MESH
F32 = jnp.float32
BF16 = jnp.bfloat16


def dot_f32(left, right, dims):
    return lax.dot_general(left, right, ((dims[0], dims[1]), ((), ())), preferred_element_type=F32)


P0, PN = (0, 224), (224, 208)
Q0, QN = (0, 112, 224, 336), (112, 112, 112, 96)
RS_KINDS = ("far_r", "far_l", "nr_raw", "nl_raw", "nr_rel", "nl_rel")
AG_KINDS = ("own_r0", "own_l1", "own_r1", "own_l0", "fwd_r", "fwd_l")


def kernel(
    tokens, cotangent, gate_up, down_w, router, choice,
    fin_out, comb_out, rank_out, acc_out,
    select, xin, rows, wgt, psend, pown, prelay, precv, lsend, lrecv, gate, sacc, mids,
    gsend, grecv, bown, brecv, xrelay, xrecv, fsend, fin2, fin, srow, srecv, labels, meta, flags, comb, acc,
    ssem, rsem, osem,
):
    y, zl, zh, x, c = (lax.axis_index(a) for a in ALL)
    yr, yl, yo = (y + 1) % 4, (y + 3) % 4, (y + 2) % 4
    xr, xl, xo = (x + 1) % 4, (x + 3) % 4, (x + 2) % 4
    D = rows.shape[2]
    own = D // 2
    swap_y, swap_zh, swap_x = 2 * zh + x // 2, y // 2, 2 * (y % 2) + x % 2
    fixed = swap_y == y
    moves = jnp.logical_not(fixed)
    swap = dict(y=swap_y, zh=swap_zh, x=swap_x)

    number = {}
    started = []

    def index(key, n=1):
        if key not in number:
            number[key] = number.get("next", 0)
            number["next"] = number[key] + n
        return number[key]

    def copy_at(i, src, dst, **to):
        return pltpu.make_async_remote_copy(
            src_ref=src, dst_ref=dst, send_sem=ssem.at[i], recv_sem=rsem.at[i],
            device_id=to, device_id_type=MESH,
        )

    def copy(key, src, dst, **to):
        return copy_at(index(key), src, dst, **to)

    def start(cp):
        cp.start()
        started.append(cp)
        return cp

    barrier = pltpu.get_barrier_semaphore()
    peers = (
        dict(y=yr), dict(y=yl), dict(y=yo), dict(zl=1 - zl), dict(zh=1 - zh),
        dict(x=xr), dict(x=xl), dict(x=xo), dict(c=1 - c),
        dict(y=2 * (1 - zh) + x // 2, zh=swap_zh, x=swap_x), dict(y=swap_y, zh=1 - swap_zh, x=swap_x),
    )
    for peer in peers:
        pl.semaphore_signal(barrier, inc=1, device_id=peer, device_id_type=MESH)

    @pl.when(moves)
    def _():
        pl.semaphore_signal(barrier, inc=1, device_id=swap, device_id_type=MESH)

    def place(p, zh_, x_, c_):
        row = pl.multiple_of((2 * zh_ + x_ // 2) * CAP + P0[p], 16)
        col = pl.multiple_of((2 * (x_ % 2) + c_) * SUB, 128)
        return rows.at[:, pl.ds(row, PN[p]), pl.ds(col, SUB)]

    def weights(sub):
        at = wgt.at[sub, pl.ds(pl.multiple_of(zl * own, 16), own), :]
        return copy(("w", sub), at, at, zl=1 - zl)

    def part(p):
        return pl.ds(P0[p], PN[p])

    def quarter(q):
        return pl.ds(Q0[q], QN[q])

    def move(p):
        return copy(("move", p), xin.at[:, part(p), :], place(p, swap_zh, swap_x, c), **swap)

    total = tokens.shape[0]
    first, second = choice[0:1, :], choice[1:2, :]
    routed = jnp.logical_or(first == 0, second == 0)
    hits = jnp.where(routed, 1.0, 0.0)
    flags[...] = jnp.zeros_like(flags)
    for i in range(total // PART):
        flags[i : i + 1, :] = hits[:, PART * i : PART * (i + 1)]
    lane = lax.broadcasted_iota(jnp.int32, (PART, PART), 0)
    before = jnp.where(lane < lax.broadcasted_iota(jnp.int32, (PART, PART), 1), 1.0, 0.0)
    line = lax.broadcasted_iota(jnp.int32, (16, 16), 0)
    above = jnp.where(line > lax.broadcasted_iota(jnp.int32, (16, 16), 1), 1.0, 0.0)
    marks = flags[...].astype(BF16)
    within = dot_f32(marks, before.astype(BF16), ((1,), (0,)))
    counts = dot_f32(marks, jnp.ones((PART, PART), BF16), ((1,), (0,)))
    flags[...] = within + dot_f32(above.astype(BF16), counts.astype(BF16), ((1,), (0,)))
    for i in range(total // PART):
        at = slice(PART * i, PART * (i + 1))
        rank = flags[i : i + 1, :].astype(jnp.int32)
        meta[0:1, at] = jnp.where(routed[:, at], rank, -1)
    meta[1:2, :] = first + second + 1
    meta[2:3, :] = jnp.where(first == 0, 1, 0)
    meta[3:4, :] = jnp.where(second == 0, 1, 0)
    meta[4:8, :] = jnp.zeros((4, total), jnp.int32)
    leave = []

    def put_out(src, dst):
        cp = pltpu.make_async_copy(src, dst, osem.at[len(leave)])
        cp.start()
        leave.append(cp)

    put_out(meta, rank_out)

    def dispatch(p):
        slots = lax.broadcasted_iota(jnp.int32, (PN[p], total), 0) + P0[p]
        select[part(p), :] = jnp.where(slots == meta[0:1, :], 1.0, 0.0).astype(BF16)
        xin[0, part(p), :] = dot_f32(select[part(p), :], tokens[...], ((1,), (0,))).astype(BF16)
        xin[1, part(p), :] = dot_f32(select[part(p), :], cotangent[...], ((1,), (0,))).astype(BF16)

    def send(p):
        @pl.when(fixed)
        def _():
            place(p, zh, x, c)[...] = xin[:, part(p), :]

        @pl.when(moves)
        def _():
            move(p).start()

    dispatch(0)

    @pl.when(moves)
    def _():
        pl.semaphore_wait(barrier, len(peers) + 1)

    @pl.when(fixed)
    def _():
        pl.semaphore_wait(barrier, len(peers))

    send(0)
    dispatch(1)
    send(1)

    def put_weights(i, carry):
        at = pl.ds(pl.multiple_of(zl * own + i * 96, 16), 96)
        of = pl.ds(pl.multiple_of(i * 96, 16), 96)
        for sub in range(4):
            for n, (ref, base) in enumerate(((gate_up, 0), (gate_up, 512), (down_w, 0))):
                wgt[sub, at, PART * n : PART * (n + 1)] = ref[of, base + PART * sub : base + PART * (sub + 1)]
        return carry

    lax.fori_loop(0, own // 96, put_weights, 0)
    named = jnp.broadcast_to(meta[1:2, :].astype(F32).astype(BF16), (16, tokens.shape[0]))
    labels[:, :CAP] = dot_f32(named, select[...], ((1,), (1,)))

    steps = {
        "zh": (lambda p: place(p, zh, x, c), dict(zh=1 - zh)),
        "xr0": (lambda p: place(p, zh, x, c), dict(x=xr)),
        "xl0": (lambda p: place(p, zh, x, c), dict(x=xl)),
        "xro": (lambda p: place(p, zh, xl, c), dict(x=xr)),
        "xr1": (lambda p: place(p, 1 - zh, x, c), dict(x=xr)),
        "xl1": (lambda p: place(p, 1 - zh, x, c), dict(x=xl)),
        "xlo": (lambda p: place(p, 1 - zh, xr, c), dict(x=xl)),
        "c_own": (lambda p: place(p, zh, x, c), dict(c=1 - c)),
        "c_zh": (lambda p: place(p, 1 - zh, x, c), dict(c=1 - c)),
        "c_xr0": (lambda p: place(p, zh, xl, c), dict(c=1 - c)),
        "c_xl0": (lambda p: place(p, zh, xr, c), dict(c=1 - c)),
        "c_xr1": (lambda p: place(p, 1 - zh, xl, c), dict(c=1 - c)),
        "c_xl1": (lambda p: place(p, 1 - zh, xr, c), dict(c=1 - c)),
        "c_xro": (lambda p: place(p, zh, xo, c), dict(c=1 - c)),
        "c_xlo": (lambda p: place(p, 1 - zh, xo, c), dict(c=1 - c)),
    }

    def hop(name, p):
        at, to = steps[name]
        return copy((name, p), at(p), at(p), **to)

    def arrive(name, p, *then):
        hop(name, p).wait_recv()
        for follow in then:
            start(hop(follow, p))

    def all_cores(p):
        for name in steps:
            if name.startswith("c_"):
                hop(name, p).wait_recv()

    for p in range(2):

        @pl.when(moves)
        def _():
            move(p).wait_recv()

        for name in ("zh", "xr0", "xl0", "c_own"):
            start(hop(name, p))
    for sub in range(4):
        start(weights(sub))

    rs_base = index("rs", 48)
    ag_base = index("ag", 48)

    def rs(kind, p, s):
        q = 2 * p + (kind in ("far_l", "nr_raw", "nl_rel"))
        at = quarter(q)
        src, dst, to = {
            "fa": lambda: (psend.at[0, s, at, :], prelay.at[s, at, :], yr if kind == "far_r" else yl),
            "nr": lambda: (psend.at[1, s, at, :], precv.at[0, s, at, :], yr),
            "nl": lambda: (psend.at[2, s, at, :], precv.at[1, s, at, :], yl),
        }[kind[:2]]()
        return copy_at(rs_base + (p * 4 + s) * 6 + RS_KINDS.index(kind), src, dst, y=to)

    def logit(r):
        to = (yo, yr, yl)[r]
        return copy(("lg", r), lsend.at[r], lrecv.at[r], y=to)

    def pre_send(p, s):
        for kind in RS_KINDS[:4]:
            rs(kind, p, s).start()

    def pre(p, s, held=False):
        def one(n, carry):
            r = jnp.where(n == 0, 2, jnp.where(n == 1, 1, jnp.where(n == 2, 3, 0)))
            t = (y + r) % 4
            at = pl.ds(pl.multiple_of(t * CAP + P0[p], 16), PN[p])
            g = dot_f32(rows[0, at, :], wgt[s, :, : 2 * PART], ((1,), (0,)))
            d = dot_f32(rows[1, at, :], wgt[s, :, 2 * PART :], ((1,), (0,)))

            @pl.when(n < 3)
            def _():
                psend[n, s, part(p), : 2 * PART] = g.astype(BF16)
                psend[n, s, part(p), 2 * PART :] = d.astype(BF16)

            @pl.when(n == 3)
            def _():
                pown[s, part(p), : 2 * PART] = g
                pown[s, part(p), 2 * PART :] = d

            for m, kinds in () if held else ((0, ("far_r", "far_l")), (1, ("nr_raw",)), (2, ("nl_raw",))):

                @pl.when(n == m)
                def _():
                    for kind in kinds:
                        rs(kind, p, s).start()

            return carry

        lax.fori_loop(0, 4, one, 0)

    def logits():
        cols = router[:, pl.ds(pl.multiple_of(y * D, 128), D)]

        def one(n, carry):
            t = (y + jnp.where(n == 0, 2, jnp.where(n == 1, 1, jnp.where(n == 2, 3, 0)))) % 4
            at = pl.ds(pl.multiple_of(t * CAP, 16), CAP)
            lsend[n, :, :CAP] = dot_f32(cols, rows[0, at, :], ((1,), (1,)))
            return carry

        lax.fori_loop(0, 4, one, 0)
        for r in range(3):
            start(logit(r))

    def relay(p, s):
        for side, slot, rel in (("far_r", 1, "nr_rel"), ("far_l", 2, "nl_rel")):
            at = quarter(2 * p + (side == "far_l"))
            rs(side, p, s).wait_recv()
            total = psend[slot, s, at, :].astype(F32) + prelay[s, at, :].astype(F32)
            psend[slot, s, at, :] = total.astype(BF16)
            rs(rel, p, s).start()

    def gates():
        for r in range(3):
            logit(r).wait_recv()
        total = (lsend[3] + lrecv[0]) + (lrecv[1] + lrecv[2])
        label = labels[:8] - 1.0
        experts = lax.broadcasted_iota(jnp.int32, (8, 512), 0).astype(F32)
        picked = jnp.sum(jnp.where(label == experts, total, 0.0), axis=0, keepdims=True)
        margin = total[:1] - picked
        row = jnp.where(label[:1] > -0.5, jax.nn.sigmoid(margin), 0.0)
        gate[...] = jnp.transpose(jnp.broadcast_to(row, (PART, 512)))
        sacc[...] = jnp.zeros_like(sacc)

    def ag(kind, p, s):
        q = 2 * p + (kind in ("own_r1", "own_l1", "fwd_l"))
        t = {"own": y, "fwd": yl if kind == "fwd_r" else yr}[kind[:3]]
        to = yr if kind[4] == "r" else yl
        at = mids.at[s, pl.ds(pl.multiple_of(t * CAP + Q0[q], 16), QN[q]), :]
        return copy_at(ag_base + (p * 4 + s) * 6 + AG_KINDS.index(kind), at, at, y=to)

    def pointwise(p, s):
        for kind in RS_KINDS[2:]:
            rs(kind, p, s).wait_recv()
        for q in (2 * p, 2 * p + 1):
            at = quarter(q)
            near = precv[0, s, at, :].astype(F32) + precv[1, s, at, :].astype(F32)
            now = pown[s, at, :] + near
            g, up, raw = now[:, :PART], now[:, PART : 2 * PART], now[:, 2 * PART :]
            sigma = jax.nn.sigmoid(g)
            active = g * sigma
            slope = sigma * (1.0 + g * (1.0 - sigma))
            product = active * up
            scale = gate[at, :]
            sacc[at, :] += product * raw
            upstream = scale * raw
            to = pl.ds(pl.multiple_of(y * CAP + Q0[q], 16), QN[q])
            mids[s, to, :PART] = (upstream * up * slope).astype(BF16)
            mids[s, to, PART : 2 * PART] = (upstream * active).astype(BF16)
            mids[s, to, 2 * PART :] = (scale * product).astype(BF16)
        for kind in AG_KINDS[:4]:
            ag(kind, p, s).start()

    def forward(p, s):
        for kind, fwd in (("own_r0", "fwd_r"), ("own_l1", "fwd_l")):
            ag(kind, p, s).wait_recv()
            ag(fwd, p, s).start()

    def near(p, s):
        ag("own_r1", p, s).wait_recv()
        ag("own_l0", p, s).wait_recv()

    def far(p, s):
        ag("fwd_r", p, s).wait_recv()
        ag("fwd_l", p, s).wait_recv()

    def exchange(s, half=None):
        at = pl.ds(0, own) if half is None else pl.ds(half * (own // 4), own // 4)
        return copy(("gz", s, half), gsend.at[s, at, :], grecv.at[s, at, :], zl=1 - zl)

    def grads_tile(s, at):
        gu = dot_f32(rows[0, :, pl.ds(at, 256)], mids[s, :, : 2 * PART], ((0,), (0,)))
        return gu, dot_f32(rows[1, :, pl.ds(at, 256)], mids[s, :, 2 * PART :], ((0,), (0,)))

    def grads_theirs(s):
        def one(i, carry):
            gu, d = grads_tile(s, pl.multiple_of((1 - zl) * own + i * 256, 256))
            to = pl.ds(pl.multiple_of(i * 256, 256), 256)
            gsend[s, to, : 2 * PART] = gu.astype(BF16)
            gsend[s, to, 2 * PART :] = d.astype(BF16)
            return carry

        lax.fori_loop(0, own // 256, one, 0)

    def grads_mine(s):
        def one(i, carry):
            gu, d = grads_tile(s, pl.multiple_of(zl * own + i * 256, 256))
            to = pl.ds(pl.multiple_of(i * 256, 256), 256)
            for g in range(2):
                acc[3 * s + g, to, :] = gu[:, PART * g : PART * (g + 1)]
            acc[3 * s + 2, to, :] = d
            return carry

        lax.fori_loop(0, own // 256, one, 0)

    def add_grads(s, half=None):
        exchange(s, half).wait_recv()

        def one(i, carry):
            at = pl.ds(pl.multiple_of(i * 64, 16), 64)
            got = grecv[s, at, :].astype(F32)
            for g in range(3):
                acc[3 * s + g, at, :] += got[:, PART * g : PART * (g + 1)]
            return carry

        count = own // 64
        if half is None:
            lax.fori_loop(0, count, one, 0)
        else:
            lax.fori_loop(half * (count // 4), (half + 1) * (count // 4), one, 0)
        at = pl.ds(0, own) if half is None else pl.ds(half * (own // 4), own // 4)
        put_out(acc.at[pl.ds(3 * s, 3), at, :], acc_out.at[pl.ds(3 * s, 3), at, :])

    def score(key):
        src, dst, to = {
            "c": (0, 0, dict(c=1 - c)), "zh": (1, 1, dict(zh=1 - zh)),
            "x0": (2, 2, dict(x=xr)), "x1": (2, 3, dict(x=xl)), "x2": (2, 4, dict(x=xo)),
        }[key]
        return copy(("sc", key), srow.at[src], srecv.at[dst], **to)

    def scores():
        summed = jnp.sum(jnp.transpose(sacc[...]), axis=0, keepdims=True)
        srow[0] = jnp.broadcast_to(summed, (8, 512))
        start(score("c"))

    def scores_zh():
        score("c").wait_recv()
        srow[1] = srow[0] + srecv[0]
        start(score("zh"))

    def scores_x():
        score("zh").wait_recv()
        srow[2] = srow[1] + srecv[1]
        for key in ("x0", "x1", "x2"):
            start(score(key))

    def scores_end():
        for key in ("x0", "x1", "x2"):
            score(key).wait_recv()
        exact = ((srow[2] + srecv[2]) + (srecv[3] + srecv[4]))[0:1, :CAP]
        high = exact.astype(BF16).astype(F32)
        middle = (exact - high).astype(BF16).astype(F32)
        at = lax.broadcasted_iota(jnp.int32, (16, CAP), 0)
        split = jnp.where(at == 0, high, jnp.where(at == 1, middle, exact - high - middle))
        split = jnp.where(at < 3, split, 0.0).astype(BF16)
        parts = dot_f32(split, select[...], ((1,), (0,)))
        value = parts[0:1] + (parts[1:2] + parts[2:3])
        column = lax.broadcasted_iota(jnp.int32, (8, total), 0)
        chosen = jnp.where(column == 0, meta[2:3, :], meta[3:4, :])
        comb[...] = jnp.where(chosen > 0, value, 0.0)
        put_out(comb, comb_out)

    pair_base = index("pair", 16)

    def pair(p, i):
        src = psend.at[i // 4, i % 4, part(p), :]
        return copy_at(pair_base + p * 8 + i, src, brecv.at[i, part(p), :], c=1 - c)

    def ring(kind, half, p):
        at = part(p)
        src, dst, to = {
            "far_r": lambda: (bown.at[xo, half, at, :], xrelay.at[0, at, :], xr),
            "far_l": lambda: (bown.at[xo, half, at, :], xrelay.at[1, at, :], xl),
            "near_r": lambda: (bown.at[xr, half, at, :], xrecv.at[0, half, at, :], xr),
            "near_l": lambda: (bown.at[xl, half, at, :], xrecv.at[1, half, at, :], xl),
        }[kind]()
        return copy(("bx", kind, half, p), src, dst, x=to)

    def home(p, near_plane):
        to = swap if near_plane else dict(y=2 * (1 - zh) + x // 2, zh=swap_zh, x=swap_x)
        src = fsend.at[0 if near_plane else 1, part(p), :]
        return copy(("home", p, near_plane), src, fin2.at[zh, part(p), :], **to)

    def owned(p):
        home(p, False).wait_recv()

        @pl.when(moves)
        def _():
            home(p, True).wait_recv()

        add_rows(p, fin, [fin2.at[0], fin2.at[1]])

    def add_rows(p, out, refs):
        for q in (2 * p, 2 * p + 1):
            at = quarter(q)
            total = refs[0][at, :].astype(F32)
            for ref in refs[1:]:
                total = total + ref[at, :].astype(F32)
            out[at, :] = total.astype(out.dtype)

    def back_blocks(*blocks):
        def one(b, carry):
            col = pl.multiple_of(b * 2 * SUB, 128)
            lines = []
            for p, t in blocks:
                at = pl.ds(pl.multiple_of(t * CAP + P0[p], 16), PN[p])
                lines.append(jnp.concatenate([mids[sub, at, : 2 * PART] for sub in range(4)], axis=1))
            m = jnp.concatenate(lines, axis=0)
            w = jnp.concatenate([wgt[sub, pl.ds(col, 2 * SUB), : 2 * PART] for sub in range(4)], axis=1)
            piece = dot_f32(m, w, ((1,), (1,)))
            low, high = piece[:, :SUB], piece[:, SUB:]
            mine = jnp.where(c == 0, low, high).astype(BF16)
            theirs = jnp.where(c == 0, high, low).astype(BF16)
            base = 0
            for p, t in blocks:
                k = t // 2
                x_ = 2 * (t % 2) + b
                i = x_ * 2 + k
                bown[x_, k, part(p), :] = mine[base : base + PN[p]]
                psend[i // 4, i % 4, part(p), :] = theirs[base : base + PN[p]]
                base += PN[p]
                pair(p, i).start()
            return carry

        lax.fori_loop(0, 2, one, 0)

    def back_sum(p, t):
        k = t // 2

        def one(b, carry):
            x_ = 2 * (t % 2) + b
            i = x_ * 2 + k
            r = (x_ - x + 4) % 4
            pair(p, i).wait_recv()
            add_rows(p, bown.at[x_, k], [bown.at[x_, k], brecv.at[i]])
            for r_, k_, kind in ((2, 0, "far_r"), (2, 1, "far_l"), (1, 1, "near_r"), (3, 0, "near_l")):

                @pl.when(jnp.logical_and(r == r_, k == k_))
                def _():
                    ring(kind, k_, p).start()

            return carry

        lax.fori_loop(0, 2, one, 0)

    def ring_relay(p):
        ring("far_r", 0, p).wait_recv()
        add_rows(p, bown.at[xr, 0], [bown.at[xr, 0], xrelay.at[0]])
        ring("near_r", 0, p).start()
        ring("far_l", 1, p).wait_recv()
        add_rows(p, bown.at[xl, 1], [bown.at[xl, 1], xrelay.at[1]])
        ring("near_l", 1, p).start()

    def ring_end(p):
        for half in range(2):
            for kind in ("near_r", "near_l"):
                ring(kind, half, p).wait_recv()
        add_rows(p, fsend.at[1], [bown.at[x, 1 - zh], xrecv.at[0, 1 - zh], xrecv.at[1, 1 - zh]])
        add_rows(p, fsend.at[0], [bown.at[x, zh], xrecv.at[0, zh], xrecv.at[1, zh]])

    def go_home(p):
        start(home(p, False))

        @pl.when(fixed)
        def _():
            fin2[zh, part(p), :] = fsend[0, part(p), :]

        @pl.when(moves)
        def _():
            home(p, True).start()

    arrive("xr0", 0, "xro", "c_xr0")
    arrive("xl0", 0, "c_xl0")
    arrive("zh", 0, "xr1", "xl1", "c_zh")
    arrive("xr0", 1, "xro", "c_xr0")
    arrive("xl0", 1, "c_xl0")
    arrive("zh", 1, "xr1", "xl1", "c_zh")
    arrive("xl1", 0, "xlo", "c_xl1")
    arrive("xro", 0, "c_xro")
    arrive("xr1", 0, "c_xr1")
    arrive("xl1", 1, "xlo", "c_xl1")
    arrive("xlo", 0, "c_xlo")
    all_cores(0)
    weights(0).wait_recv()
    pre(0, 0)
    weights(1).wait_recv()
    pre(0, 1)
    arrive("xro", 1, "c_xro")
    arrive("xr1", 1, "c_xr1")
    arrive("xlo", 1, "c_xlo")
    all_cores(1)
    pre(1, 0)
    pre(1, 1)
    logits()
    for p in range(2):
        for s in range(2):
            relay(p, s)
    gates()
    pointwise(0, 0)
    pointwise(0, 1)
    pointwise(1, 0)
    pointwise(1, 1)
    forward(0, 0)
    forward(0, 1)
    weights(2).wait_recv()
    pre(0, 2, held=True)
    forward(1, 0)
    forward(1, 1)
    pre_send(0, 2)
    weights(3).wait_recv()
    pre(0, 3)
    pre(1, 2)
    pre(1, 3)
    for p in range(2):
        near(p, 0)
        far(p, 0)
    grads_theirs(0)
    start(exchange(0))
    relay(0, 2)
    relay(0, 3)
    for p in range(2):
        near(p, 1)
        far(p, 1)
    grads_theirs(1)
    start(exchange(1))
    relay(1, 2)
    relay(1, 3)
    grads_mine(0)
    pointwise(0, 2)
    pointwise(0, 3)
    forward(0, 2)
    pointwise(1, 2)
    forward(0, 3)
    pointwise(1, 3)
    scores()
    for kind in RS_KINDS:
        for p in range(2):
            for s in range(4):
                rs(kind, p, s).wait_send()
    back_blocks((0, y), (1, y))
    scores_zh()
    for s in range(2, 4):
        near(0, s)
    back_blocks((0, yr), (0, yl))
    forward(1, 2)
    for s in range(2, 4):
        far(0, s)
    back_blocks((0, yo),)
    back_sum(0, y)
    back_sum(0, yr)
    back_sum(0, yl)
    forward(1, 3)
    back_sum(0, yo)
    near(1, 2)
    far(1, 2)
    grads_theirs(2)
    start(exchange(2))
    near(1, 3)
    back_blocks((1, yr), (1, yl))
    ring_relay(0)
    far(1, 3)
    grads_theirs(3)
    start(exchange(3))
    back_blocks((1, yo),)
    back_sum(1, y)
    back_sum(1, yr)
    back_sum(1, yl)
    back_sum(1, yo)
    scores_x()
    ring_relay(1)
    grads_mine(1)
    ring_end(0)
    ring_end(1)
    go_home(0)
    go_home(1)
    grads_mine(2)
    add_grads(0)
    add_grads(1)
    add_grads(2)
    grads_mine(3)
    scores_end()
    owned(0)
    add_grads(3)
    owned(1)
    put_out(fin, fin_out)

    @pl.when(moves)
    def _():
        for p in range(2):
            move(p).wait_send()
            home(p, True).wait_send()

    for kind in AG_KINDS:
        for p in range(2):
            for s in range(4):
                ag(kind, p, s).wait_send()
    for key in number:
        if key[0] == "bx":
            ring(*key[1:]).wait_send()
    for p in range(2):
        for i in range(8):
            pair(p, i).wait_send()
    for cp in started:
        cp.wait_send()
    for cp in leave:
        cp.wait()


def finish(ranks, fin, combine, sums):
    total, own = ranks.shape[1], sums.shape[1]
    steps = 2
    tile, deep = total // steps, own // steps

    def body(ranks_ref, fin_ref, comb_ref, sums_ref, gtok_ref, comb_out, gu_out, down_out):
        for s in range(4):
            for g in range(2):
                gu_out[pl.ds(2 * s + g, deep, stride=8), :] = sums_ref[3 * s + g]
            down_out[:, PART * s : PART * (s + 1)] = sums_ref[3 * s + 2]
        comb_out[...] = comb_ref[0:2, :]
        slots = lax.broadcasted_iota(jnp.int32, (CAP, tile), 0)
        select = jnp.where(slots == ranks_ref[0:1, :], 1.0, 0.0).astype(BF16)
        gtok_ref[...] = dot_f32(select, fin_ref[...], ((0,), (0,))).astype(BF16)

    cols = lambda n: pl.BlockSpec((n, tile), lambda i: (0, i))
    rows = lambda n, m: pl.BlockSpec((n, m), lambda i: (i, 0))
    return pl.pallas_call(
        body,
        grid=(steps,),
        out_shape=(
            jax.ShapeDtypeStruct((total, SUB), BF16),
            jax.ShapeDtypeStruct((2, total), F32),
            jax.ShapeDtypeStruct((own * 8, PART), F32),
            jax.ShapeDtypeStruct((own, 4 * PART), F32),
        ),
        in_specs=[
            cols(8),
            pl.BlockSpec(fin.shape, lambda i: (0, 0)),
            cols(8),
            pl.BlockSpec((12, deep, PART), lambda i: (0, i, 0)),
        ],
        out_specs=[rows(tile, SUB), cols(2), rows(deep * 8, PART), rows(deep, 4 * PART)],
        cost_estimate=pl.CostEstimate(flops=2 * total * CAP * SUB, bytes_accessed=12 << 20, transcendentals=0),
    )(ranks, fin, combine, sums)


def exchange_and_compute(tokens, cotangent, gate_up, down_w, router, choice):
    own = down_w.shape[0]
    rows_all = 4 * CAP
    vm = pltpu.VMEM
    piece = (CAP, SUB)
    flops = 2 * rows_all * 2 * own * 4 * SUB * 8 // 3
    return pl.pallas_call(
        kernel,
        out_shape=(
            jax.ShapeDtypeStruct(piece, BF16),
            jax.ShapeDtypeStruct((8, tokens.shape[0]), F32),
            jax.ShapeDtypeStruct((8, tokens.shape[0]), jnp.int32),
            jax.ShapeDtypeStruct((12, own, PART), F32),
        ),
        in_specs=[pl.BlockSpec(memory_space=vm)] * 6,
        out_specs=[pl.BlockSpec(memory_space=pl.ANY)] * 4,
        scratch_shapes=[
            vm((CAP, tokens.shape[0]), BF16),
            vm((2,) + piece, BF16),
            vm((2, rows_all, 2 * own), BF16),
            vm((4, 2 * own, SUB), BF16),
            vm((3, 4) + piece, BF16),
            vm((4,) + piece, F32),
            vm((4,) + piece, BF16),
            vm((2, 4) + piece, BF16),
            vm((4, 8, 512), F32),
            vm((3, 8, 512), F32),
            vm((512, PART), F32),
            vm((512, PART), F32),
            vm((4, rows_all, SUB), BF16),
            vm((4, own, SUB), BF16),
            vm((4, own, SUB), BF16),
            vm((4, 2) + piece, BF16),
            vm((8,) + piece, BF16),
            vm((2,) + piece, BF16),
            vm((2, 2) + piece, BF16),
            vm((2,) + piece, BF16),
            vm((2,) + piece, BF16),
            vm(piece, BF16),
            vm((3, 8, 512), F32),
            vm((5, 8, 512), F32),
            vm((16, 512), F32),
            vm((8, tokens.shape[0]), jnp.int32),
            vm((16, PART), F32),
            vm((8, tokens.shape[0]), F32),
            vm((12, own, PART), F32),
            pltpu.SemaphoreType.DMA((192,)),
            pltpu.SemaphoreType.DMA((192,)),
            pltpu.SemaphoreType.DMA((12,)),
        ],
        cost_estimate=pl.CostEstimate(flops=flops, bytes_accessed=20 << 20, transcendentals=CAP * 512),
        compiler_params=pltpu.CompilerParams(
            collective_id=0, has_side_effects=True, vmem_limit_bytes=67043328
        ),
    )(tokens, cotangent, gate_up, down_w, router, choice)


def local(tokens, cotangent, expert_choice, router, gate_up, w_down):
    own, hid = w_down.shape
    fin, combine, ranks, sums = exchange_and_compute(
        tokens, cotangent, gate_up.reshape(own, 2 * hid), w_down, router, expert_choice.T
    )
    grad_tokens, combine, d_gu, d_down = finish(ranks, fin, combine, sums)
    d_gate_up = d_gu.reshape(own, hid // PART, 2, PART).transpose(0, 2, 1, 3).reshape(own, 2, hid)
    return (grad_tokens, combine.T, d_gate_up, d_down)


def solution(mesh):
    split = Mesh(mesh.devices.reshape(4, 2, 2, 4, 2), ALL)
    return jax.shard_map(
        local,
        mesh=split,
        in_specs=(
            P(TOK, HID),
            P(TOK, HID),
            P(TOK, None),
            P(),
            P(TOK, None, HID),
            P(TOK, HID),
        ),
        out_specs=(P(TOK, HID), P(TOK, None), P(TOK, None, HID), P(TOK, HID)),
        check_vma=False,
    )
```

```python
import jax
import jax.numpy as jnp
from jax import lax
from jax.experimental import pallas as pl
from jax.experimental.pallas import tpu as pltpu
from jax.sharding import Mesh
from jax.sharding import PartitionSpec as P

CAP = 432
SUB = 384
PART = 128
TOK = ("y", "zl")
HID = ("zh", "x", "c")
ALL = TOK + HID
MESH = pl.DeviceIdType.MESH
F32 = jnp.float32
BF16 = jnp.bfloat16


def dot_f32(left, right, dims):
    return lax.dot_general(left, right, ((dims[0], dims[1]), ((), ())), preferred_element_type=F32)


P0, PN = (0, 224), (224, 208)
Q0, QN = (0, 112, 224, 336), (112, 112, 112, 96)
RS_KINDS = ("far_r", "far_l", "nr_raw", "nl_raw", "nr_rel", "nl_rel")
AG_KINDS = ("own_r0", "own_l1", "own_r1", "own_l0", "fwd_r", "fwd_l")


def kernel(
    tokens, cotangent, gate_up, down_w, router, choice,
    fin_out, comb_out, rank_out, acc_out,
    select, xin, rows, wgt, psend, pown, prelay, precv, lsend, lrecv, gate, sacc, mids,
    gsend, grecv, bown, brecv, xrelay, xrecv, fsend, fin2, fin, srow, srecv, labels, meta, flags, comb, acc,
    ssem, rsem, osem,
):
    y, zl, zh, x, c = (lax.axis_index(a) for a in ALL)
    yr, yl, yo = (y + 1) % 4, (y + 3) % 4, (y + 2) % 4
    xr, xl, xo = (x + 1) % 4, (x + 3) % 4, (x + 2) % 4
    D = rows.shape[2]
    own = D // 2
    swap_y, swap_zh, swap_x = 2 * zh + x // 2, y // 2, 2 * (y % 2) + x % 2
    fixed = swap_y == y
    moves = jnp.logical_not(fixed)
    swap = dict(y=swap_y, zh=swap_zh, x=swap_x)

    number = {}
    started = []

    def index(key, n=1):
        if key not in number:
            number[key] = number.get("next", 0)
            number["next"] = number[key] + n
        return number[key]

    def copy_at(i, src, dst, **to):
        return pltpu.make_async_remote_copy(
            src_ref=src, dst_ref=dst, send_sem=ssem.at[i], recv_sem=rsem.at[i],
            device_id=to, device_id_type=MESH,
        )

    def copy(key, src, dst, **to):
        return copy_at(index(key), src, dst, **to)

    def start(cp):
        cp.start()
        started.append(cp)
        return cp

    barrier = pltpu.get_barrier_semaphore()
    peers = (
        dict(y=yr), dict(y=yl), dict(y=yo), dict(zl=1 - zl), dict(zh=1 - zh),
        dict(x=xr), dict(x=xl), dict(x=xo), dict(c=1 - c),
        dict(y=2 * (1 - zh) + x // 2, zh=swap_zh, x=swap_x), dict(y=swap_y, zh=1 - swap_zh, x=swap_x),
    )
    for peer in peers:
        pl.semaphore_signal(barrier, inc=1, device_id=peer, device_id_type=MESH)

    @pl.when(moves)
    def _():
        pl.semaphore_signal(barrier, inc=1, device_id=swap, device_id_type=MESH)

    def place(p, zh_, x_, c_):
        row = pl.multiple_of((2 * zh_ + x_ // 2) * CAP + P0[p], 16)
        col = pl.multiple_of((2 * (x_ % 2) + c_) * SUB, 128)
        return rows.at[:, pl.ds(row, PN[p]), pl.ds(col, SUB)]

    def weights(sub):
        at = wgt.at[sub, pl.ds(pl.multiple_of(zl * own, 16), own), :]
        return copy(("w", sub), at, at, zl=1 - zl)

    def part(p):
        return pl.ds(P0[p], PN[p])

    def quarter(q):
        return pl.ds(Q0[q], QN[q])

    def move(p):
        return copy(("move", p), xin.at[:, part(p), :], place(p, swap_zh, swap_x, c), **swap)

    total = tokens.shape[0]
    first, second = choice[0:1, :], choice[1:2, :]
    routed = jnp.logical_or(first == 0, second == 0)
    hits = jnp.where(routed, 1.0, 0.0)
    flags[...] = jnp.zeros_like(flags)
    for i in range(total // PART):
        flags[i : i + 1, :] = hits[:, PART * i : PART * (i + 1)]
    lane = lax.broadcasted_iota(jnp.int32, (PART, PART), 0)
    before = jnp.where(lane < lax.broadcasted_iota(jnp.int32, (PART, PART), 1), 1.0, 0.0)
    line = lax.broadcasted_iota(jnp.int32, (16, 16), 0)
    above = jnp.where(line > lax.broadcasted_iota(jnp.int32, (16, 16), 1), 1.0, 0.0)
    marks = flags[...].astype(BF16)
    within = dot_f32(marks, before.astype(BF16), ((1,), (0,)))
    counts = dot_f32(marks, jnp.ones((PART, PART), BF16), ((1,), (0,)))
    flags[...] = within + dot_f32(above.astype(BF16), counts.astype(BF16), ((1,), (0,)))
    for i in range(total // PART):
        at = slice(PART * i, PART * (i + 1))
        rank = flags[i : i + 1, :].astype(jnp.int32)
        meta[0:1, at] = jnp.where(routed[:, at], rank, -1)
    meta[1:2, :] = first + second + 1
    meta[2:3, :] = jnp.where(first == 0, 1, 0)
    meta[3:4, :] = jnp.where(second == 0, 1, 0)
    meta[4:8, :] = jnp.zeros((4, total), jnp.int32)
    leave = []

    def put_out(src, dst):
        cp = pltpu.make_async_copy(src, dst, osem.at[len(leave)])
        cp.start()
        leave.append(cp)

    put_out(meta, rank_out)

    def dispatch(p):
        slots = lax.broadcasted_iota(jnp.int32, (PN[p], total), 0) + P0[p]
        select[part(p), :] = jnp.where(slots == meta[0:1, :], 1.0, 0.0).astype(BF16)
        xin[0, part(p), :] = dot_f32(select[part(p), :], tokens[...], ((1,), (0,))).astype(BF16)
        xin[1, part(p), :] = dot_f32(select[part(p), :], cotangent[...], ((1,), (0,))).astype(BF16)

    def send(p):
        @pl.when(fixed)
        def _():
            place(p, zh, x, c)[...] = xin[:, part(p), :]

        @pl.when(moves)
        def _():
            move(p).start()

    dispatch(0)

    @pl.when(moves)
    def _():
        pl.semaphore_wait(barrier, len(peers) + 1)

    @pl.when(fixed)
    def _():
        pl.semaphore_wait(barrier, len(peers))

    send(0)
    dispatch(1)
    send(1)

    def put_weights(i, carry):
        at = pl.ds(pl.multiple_of(zl * own + i * 96, 16), 96)
        of = pl.ds(pl.multiple_of(i * 96, 16), 96)
        for sub in range(4):
            cut = slice(PART * sub, PART * (sub + 1))
            wgt[sub, at, :PART] = gate_up[of, 0, cut]
            wgt[sub, at, PART : 2 * PART] = gate_up[of, 1, cut]
            wgt[sub, at, 2 * PART :] = down_w[of, cut]
        return carry

    lax.fori_loop(0, own // 96, put_weights, 0)
    named = jnp.broadcast_to(meta[1:2, :].astype(F32).astype(BF16), (16, tokens.shape[0]))
    labels[:, :CAP] = dot_f32(named, select[...], ((1,), (1,)))

    steps = {
        "zh": (lambda p: place(p, zh, x, c), dict(zh=1 - zh)),
        "xr0": (lambda p: place(p, zh, x, c), dict(x=xr)),
        "xl0": (lambda p: place(p, zh, x, c), dict(x=xl)),
        "xro": (lambda p: place(p, zh, xl, c), dict(x=xr)),
        "xr1": (lambda p: place(p, 1 - zh, x, c), dict(x=xr)),
        "xl1": (lambda p: place(p, 1 - zh, x, c), dict(x=xl)),
        "xlo": (lambda p: place(p, 1 - zh, xr, c), dict(x=xl)),
        "c_own": (lambda p: place(p, zh, x, c), dict(c=1 - c)),
        "c_zh": (lambda p: place(p, 1 - zh, x, c), dict(c=1 - c)),
        "c_xr0": (lambda p: place(p, zh, xl, c), dict(c=1 - c)),
        "c_xl0": (lambda p: place(p, zh, xr, c), dict(c=1 - c)),
        "c_xr1": (lambda p: place(p, 1 - zh, xl, c), dict(c=1 - c)),
        "c_xl1": (lambda p: place(p, 1 - zh, xr, c), dict(c=1 - c)),
        "c_xro": (lambda p: place(p, zh, xo, c), dict(c=1 - c)),
        "c_xlo": (lambda p: place(p, 1 - zh, xo, c), dict(c=1 - c)),
    }

    def hop(name, p):
        at, to = steps[name]
        return copy((name, p), at(p), at(p), **to)

    def arrive(name, p, *then):
        hop(name, p).wait_recv()
        for follow in then:
            start(hop(follow, p))

    def all_cores(p):
        for name in steps:
            if name.startswith("c_"):
                hop(name, p).wait_recv()

    for p in range(2):

        @pl.when(moves)
        def _():
            move(p).wait_recv()

        for name in ("zh", "xr0", "xl0", "c_own"):
            start(hop(name, p))
    for sub in range(4):
        start(weights(sub))

    rs_base = index("rs", 48)
    ag_base = index("ag", 48)

    def rs(kind, p, s):
        q = 2 * p + (kind in ("far_l", "nr_raw", "nl_rel"))
        at = quarter(q)
        src, dst, to = {
            "fa": lambda: (psend.at[0, s, at, :], prelay.at[s, at, :], yr if kind == "far_r" else yl),
            "nr": lambda: (psend.at[1, s, at, :], precv.at[0, s, at, :], yr),
            "nl": lambda: (psend.at[2, s, at, :], precv.at[1, s, at, :], yl),
        }[kind[:2]]()
        return copy_at(rs_base + (p * 4 + s) * 6 + RS_KINDS.index(kind), src, dst, y=to)

    def logit(r):
        to = (yo, yr, yl)[r]
        return copy(("lg", r), lsend.at[r], lrecv.at[r], y=to)

    def pre_send(p, s):
        for kind in RS_KINDS[:4]:
            rs(kind, p, s).start()

    def pre(p, s, held=False):
        def one(n, carry):
            r = jnp.where(n == 0, 2, jnp.where(n == 1, 1, jnp.where(n == 2, 3, 0)))
            t = (y + r) % 4
            at = pl.ds(pl.multiple_of(t * CAP + P0[p], 16), PN[p])
            g = dot_f32(rows[0, at, :], wgt[s, :, : 2 * PART], ((1,), (0,)))
            d = dot_f32(rows[1, at, :], wgt[s, :, 2 * PART :], ((1,), (0,)))

            @pl.when(n < 3)
            def _():
                psend[n, s, part(p), : 2 * PART] = g.astype(BF16)
                psend[n, s, part(p), 2 * PART :] = d.astype(BF16)

            @pl.when(n == 3)
            def _():
                pown[s, part(p), : 2 * PART] = g
                pown[s, part(p), 2 * PART :] = d

            for m, kinds in () if held else ((0, ("far_r", "far_l")), (1, ("nr_raw",)), (2, ("nl_raw",))):

                @pl.when(n == m)
                def _():
                    for kind in kinds:
                        rs(kind, p, s).start()

            return carry

        lax.fori_loop(0, 4, one, 0)

    def logits():
        cols = router[:, pl.ds(pl.multiple_of(y * D, 128), D)]

        def one(n, carry):
            t = (y + jnp.where(n == 0, 2, jnp.where(n == 1, 1, jnp.where(n == 2, 3, 0)))) % 4
            at = pl.ds(pl.multiple_of(t * CAP, 16), CAP)
            lsend[n, :, :CAP] = dot_f32(cols, rows[0, at, :], ((1,), (1,)))
            return carry

        lax.fori_loop(0, 4, one, 0)
        for r in range(3):
            start(logit(r))

    def relay(p, s):
        for side, slot, rel in (("far_r", 1, "nr_rel"), ("far_l", 2, "nl_rel")):
            at = quarter(2 * p + (side == "far_l"))
            rs(side, p, s).wait_recv()
            total = psend[slot, s, at, :].astype(F32) + prelay[s, at, :].astype(F32)
            psend[slot, s, at, :] = total.astype(BF16)
            rs(rel, p, s).start()

    def gates():
        for r in range(3):
            logit(r).wait_recv()
        total = (lsend[3] + lrecv[0]) + (lrecv[1] + lrecv[2])
        label = labels[:8] - 1.0
        experts = lax.broadcasted_iota(jnp.int32, (8, 512), 0).astype(F32)
        picked = jnp.sum(jnp.where(label == experts, total, 0.0), axis=0, keepdims=True)
        margin = total[:1] - picked
        row = jnp.where(label[:1] > -0.5, jax.nn.sigmoid(margin), 0.0)
        gate[...] = jnp.transpose(jnp.broadcast_to(row, (PART, 512)))
        sacc[...] = jnp.zeros_like(sacc)

    def ag(kind, p, s):
        q = 2 * p + (kind in ("own_r1", "own_l1", "fwd_l"))
        t = {"own": y, "fwd": yl if kind == "fwd_r" else yr}[kind[:3]]
        to = yr if kind[4] == "r" else yl
        at = mids.at[s, pl.ds(pl.multiple_of(t * CAP + Q0[q], 16), QN[q]), :]
        return copy_at(ag_base + (p * 4 + s) * 6 + AG_KINDS.index(kind), at, at, y=to)

    def pointwise(p, s):
        for kind in RS_KINDS[2:]:
            rs(kind, p, s).wait_recv()
        for q in (2 * p, 2 * p + 1):
            at = quarter(q)
            near = precv[0, s, at, :].astype(F32) + precv[1, s, at, :].astype(F32)
            now = pown[s, at, :] + near
            g, up, raw = now[:, :PART], now[:, PART : 2 * PART], now[:, 2 * PART :]
            sigma = jax.nn.sigmoid(g)
            active = g * sigma
            slope = sigma * (1.0 + g * (1.0 - sigma))
            product = active * up
            scale = gate[at, :]
            sacc[at, :] += product * raw
            upstream = scale * raw
            to = pl.ds(pl.multiple_of(y * CAP + Q0[q], 16), QN[q])
            mids[s, to, :PART] = (upstream * up * slope).astype(BF16)
            mids[s, to, PART : 2 * PART] = (upstream * active).astype(BF16)
            mids[s, to, 2 * PART :] = (scale * product).astype(BF16)
        for kind in AG_KINDS[:4]:
            ag(kind, p, s).start()

    def forward(p, s):
        for kind, fwd in (("own_r0", "fwd_r"), ("own_l1", "fwd_l")):
            ag(kind, p, s).wait_recv()
            ag(fwd, p, s).start()

    def near(p, s):
        ag("own_r1", p, s).wait_recv()
        ag("own_l0", p, s).wait_recv()

    def far(p, s):
        ag("fwd_r", p, s).wait_recv()
        ag("fwd_l", p, s).wait_recv()

    def exchange(s, half=None):
        at = pl.ds(0, own) if half is None else pl.ds(half * (own // 4), own // 4)
        return copy(("gz", s, half), gsend.at[s, at, :], grecv.at[s, at, :], zl=1 - zl)

    def grads_tile(s, at):
        gu = dot_f32(rows[0, :, pl.ds(at, 256)], mids[s, :, : 2 * PART], ((0,), (0,)))
        return gu, dot_f32(rows[1, :, pl.ds(at, 256)], mids[s, :, 2 * PART :], ((0,), (0,)))

    def grads_theirs(s):
        def one(i, carry):
            gu, d = grads_tile(s, pl.multiple_of((1 - zl) * own + i * 256, 256))
            to = pl.ds(pl.multiple_of(i * 256, 256), 256)
            gsend[s, to, : 2 * PART] = gu.astype(BF16)
            gsend[s, to, 2 * PART :] = d.astype(BF16)
            return carry

        lax.fori_loop(0, own // 256, one, 0)

    def grads_mine(s):
        def one(i, carry):
            gu, d = grads_tile(s, pl.multiple_of(zl * own + i * 256, 256))
            to = pl.ds(pl.multiple_of(i * 256, 256), 256)
            for g in range(2):
                acc[3 * s + g, to, :] = gu[:, PART * g : PART * (g + 1)]
            acc[3 * s + 2, to, :] = d
            return carry

        lax.fori_loop(0, own // 256, one, 0)

    def add_grads(s, half=None):
        exchange(s, half).wait_recv()

        def one(i, carry):
            at = pl.ds(pl.multiple_of(i * 64, 16), 64)
            got = grecv[s, at, :].astype(F32)
            for g in range(3):
                acc[3 * s + g, at, :] += got[:, PART * g : PART * (g + 1)]
            return carry

        count = own // 64
        if half is None:
            lax.fori_loop(0, count, one, 0)
        else:
            lax.fori_loop(half * (count // 4), (half + 1) * (count // 4), one, 0)
        at = pl.ds(0, own) if half is None else pl.ds(half * (own // 4), own // 4)
        put_out(acc.at[pl.ds(3 * s, 3), at, :], acc_out.at[pl.ds(3 * s, 3), at, :])

    def score(key):
        src, dst, to = {
            "c": (0, 0, dict(c=1 - c)), "zh": (1, 1, dict(zh=1 - zh)),
            "x0": (2, 2, dict(x=xr)), "x1": (2, 3, dict(x=xl)), "x2": (2, 4, dict(x=xo)),
        }[key]
        return copy(("sc", key), srow.at[src], srecv.at[dst], **to)

    def scores():
        summed = jnp.sum(jnp.transpose(sacc[...]), axis=0, keepdims=True)
        srow[0] = jnp.broadcast_to(summed, (8, 512))
        start(score("c"))

    def scores_zh():
        score("c").wait_recv()
        srow[1] = srow[0] + srecv[0]
        start(score("zh"))

    def scores_x():
        score("zh").wait_recv()
        srow[2] = srow[1] + srecv[1]
        for key in ("x0", "x1", "x2"):
            start(score(key))

    def scores_end():
        for key in ("x0", "x1", "x2"):
            score(key).wait_recv()
        exact = ((srow[2] + srecv[2]) + (srecv[3] + srecv[4]))[0:1, :CAP]
        high = exact.astype(BF16).astype(F32)
        middle = (exact - high).astype(BF16).astype(F32)
        at = lax.broadcasted_iota(jnp.int32, (16, CAP), 0)
        split = jnp.where(at == 0, high, jnp.where(at == 1, middle, exact - high - middle))
        split = jnp.where(at < 3, split, 0.0).astype(BF16)
        parts = dot_f32(split, select[...], ((1,), (0,)))
        value = parts[0:1] + (parts[1:2] + parts[2:3])
        column = lax.broadcasted_iota(jnp.int32, (8, total), 0)
        chosen = jnp.where(column == 0, meta[2:3, :], meta[3:4, :])
        comb[...] = jnp.where(chosen > 0, value, 0.0)
        put_out(comb, comb_out)

    pair_base = index("pair", 16)

    def pair(p, i):
        src = psend.at[i // 4, i % 4, part(p), :]
        return copy_at(pair_base + p * 8 + i, src, brecv.at[i, part(p), :], c=1 - c)

    def ring(kind, half, p):
        at = part(p)
        src, dst, to = {
            "far_r": lambda: (bown.at[xo, half, at, :], xrelay.at[0, at, :], xr),
            "far_l": lambda: (bown.at[xo, half, at, :], xrelay.at[1, at, :], xl),
            "near_r": lambda: (bown.at[xr, half, at, :], xrecv.at[0, half, at, :], xr),
            "near_l": lambda: (bown.at[xl, half, at, :], xrecv.at[1, half, at, :], xl),
        }[kind]()
        return copy(("bx", kind, half, p), src, dst, x=to)

    def home(p, near_plane):
        to = swap if near_plane else dict(y=2 * (1 - zh) + x // 2, zh=swap_zh, x=swap_x)
        src = fsend.at[0 if near_plane else 1, part(p), :]
        return copy(("home", p, near_plane), src, fin2.at[zh, part(p), :], **to)

    def owned(p):
        home(p, False).wait_recv()

        @pl.when(moves)
        def _():
            home(p, True).wait_recv()

        add_rows(p, fin, [fin2.at[0], fin2.at[1]])

    def add_rows(p, out, refs):
        for q in (2 * p, 2 * p + 1):
            at = quarter(q)
            total = refs[0][at, :].astype(F32)
            for ref in refs[1:]:
                total = total + ref[at, :].astype(F32)
            out[at, :] = total.astype(out.dtype)

    def back_blocks(*blocks):
        def one(b, carry):
            col = pl.multiple_of(b * 2 * SUB, 128)
            lines = []
            for p, t in blocks:
                at = pl.ds(pl.multiple_of(t * CAP + P0[p], 16), PN[p])
                lines.append(jnp.concatenate([mids[sub, at, : 2 * PART] for sub in range(4)], axis=1))
            m = jnp.concatenate(lines, axis=0)
            w = jnp.concatenate([wgt[sub, pl.ds(col, 2 * SUB), : 2 * PART] for sub in range(4)], axis=1)
            piece = dot_f32(m, w, ((1,), (1,)))
            low, high = piece[:, :SUB], piece[:, SUB:]
            mine = jnp.where(c == 0, low, high).astype(BF16)
            theirs = jnp.where(c == 0, high, low).astype(BF16)
            base = 0
            for p, t in blocks:
                k = t // 2
                x_ = 2 * (t % 2) + b
                i = x_ * 2 + k
                bown[x_, k, part(p), :] = mine[base : base + PN[p]]
                psend[i // 4, i % 4, part(p), :] = theirs[base : base + PN[p]]
                base += PN[p]
                pair(p, i).start()
            return carry

        lax.fori_loop(0, 2, one, 0)

    def back_sum(p, t):
        k = t // 2

        def one(b, carry):
            x_ = 2 * (t % 2) + b
            i = x_ * 2 + k
            r = (x_ - x + 4) % 4
            pair(p, i).wait_recv()
            add_rows(p, bown.at[x_, k], [bown.at[x_, k], brecv.at[i]])
            for r_, k_, kind in ((2, 0, "far_r"), (2, 1, "far_l"), (1, 1, "near_r"), (3, 0, "near_l")):

                @pl.when(jnp.logical_and(r == r_, k == k_))
                def _():
                    ring(kind, k_, p).start()

            return carry

        lax.fori_loop(0, 2, one, 0)

    def ring_relay(p):
        ring("far_r", 0, p).wait_recv()
        add_rows(p, bown.at[xr, 0], [bown.at[xr, 0], xrelay.at[0]])
        ring("near_r", 0, p).start()
        ring("far_l", 1, p).wait_recv()
        add_rows(p, bown.at[xl, 1], [bown.at[xl, 1], xrelay.at[1]])
        ring("near_l", 1, p).start()

    def ring_end(p):
        for half in range(2):
            for kind in ("near_r", "near_l"):
                ring(kind, half, p).wait_recv()
        add_rows(p, fsend.at[1], [bown.at[x, 1 - zh], xrecv.at[0, 1 - zh], xrecv.at[1, 1 - zh]])
        add_rows(p, fsend.at[0], [bown.at[x, zh], xrecv.at[0, zh], xrecv.at[1, zh]])

    def go_home(p):
        home(p, False).start()

        @pl.when(fixed)
        def _():
            fin2[zh, part(p), :] = fsend[0, part(p), :]

        @pl.when(moves)
        def _():
            home(p, True).start()

    arrive("xr0", 0, "xro", "c_xr0")
    arrive("xl0", 0, "c_xl0")
    arrive("zh", 0, "xr1", "xl1", "c_zh")
    arrive("xr0", 1, "xro", "c_xr0")
    arrive("xl0", 1, "c_xl0")
    arrive("zh", 1, "xr1", "xl1", "c_zh")
    arrive("xl1", 0, "xlo", "c_xl1")
    arrive("xro", 0, "c_xro")
    arrive("xr1", 0, "c_xr1")
    arrive("xl1", 1, "xlo", "c_xl1")
    arrive("xlo", 0, "c_xlo")
    all_cores(0)
    weights(0).wait_recv()
    pre(0, 0)
    weights(1).wait_recv()
    pre(0, 1)
    arrive("xro", 1, "c_xro")
    arrive("xr1", 1, "c_xr1")
    arrive("xlo", 1, "c_xlo")
    all_cores(1)
    pre(1, 0)
    pre(1, 1)
    logits()
    for p in range(2):
        for s in range(2):
            relay(p, s)
    gates()
    pointwise(0, 0)
    pointwise(0, 1)
    pointwise(1, 0)
    pointwise(1, 1)
    forward(0, 0)
    forward(0, 1)
    weights(2).wait_recv()
    pre(0, 2, held=True)
    forward(1, 0)
    forward(1, 1)
    pre_send(0, 2)
    weights(3).wait_recv()
    pre(0, 3)
    pre(1, 2)
    pre(1, 3)
    for p in range(2):
        near(p, 0)
        far(p, 0)
    grads_theirs(0)
    start(exchange(0))
    relay(0, 2)
    relay(0, 3)
    for p in range(2):
        near(p, 1)
        far(p, 1)
    grads_theirs(1)
    start(exchange(1))
    relay(1, 2)
    relay(1, 3)
    grads_mine(0)
    pointwise(0, 2)
    pointwise(0, 3)
    forward(0, 2)
    pointwise(1, 2)
    forward(0, 3)
    pointwise(1, 3)
    scores()
    for kind in RS_KINDS:
        for p in range(2):
            for s in range(4):
                rs(kind, p, s).wait_send()
    back_blocks((0, y), (1, y))
    scores_zh()
    for s in range(2, 4):
        near(0, s)
    back_blocks((0, yr), (0, yl))
    forward(1, 2)
    for s in range(2, 4):
        far(0, s)
    back_blocks((0, yo),)
    back_sum(0, y)
    back_sum(0, yr)
    back_sum(0, yl)
    forward(1, 3)
    back_sum(0, yo)
    near(1, 2)
    far(1, 2)
    grads_theirs(2)
    start(exchange(2))
    near(1, 3)
    back_blocks((1, yr), (1, yl))
    ring_relay(0)
    far(1, 3)
    grads_theirs(3)
    start(exchange(3))
    back_blocks((1, yo),)
    back_sum(1, y)
    back_sum(1, yr)
    back_sum(1, yl)
    back_sum(1, yo)
    scores_x()
    ring_relay(1)
    grads_mine(1)
    ring_end(0)
    ring_end(1)
    go_home(0)
    go_home(1)
    grads_mine(2)
    add_grads(0)
    add_grads(1)
    add_grads(2)
    grads_mine(3)
    scores_end()

    @pl.when(moves)
    def _():
        for p in range(2):
            move(p).wait_send()

    for kind in AG_KINDS:
        for p in range(2):
            for s in range(4):
                ag(kind, p, s).wait_send()
    for key in number:
        if key[0] == "bx":
            ring(*key[1:]).wait_send()
    for p in range(2):
        for i in range(8):
            pair(p, i).wait_send()
    for cp in started:
        cp.wait_send()
    owned(0)
    add_grads(3)
    owned(1)
    put_out(fin, fin_out)

    for p in range(2):
        home(p, False).wait_send()

    @pl.when(moves)
    def _():
        for p in range(2):
            home(p, True).wait_send()

    for cp in leave:
        cp.wait()


def finish(ranks, fin, combine, sums):
    total, own = ranks.shape[1], sums.shape[1]
    steps = 2
    tile, deep = total // steps, own // steps

    def body(ranks_ref, fin_ref, comb_ref, sums_ref, gtok_ref, comb_out, gu_out, down_out):
        for s in range(4):
            for g in range(2):
                gu_out[pl.ds(2 * s + g, deep, stride=8), :] = sums_ref[3 * s + g]
            down_out[:, PART * s : PART * (s + 1)] = sums_ref[3 * s + 2]
        comb_out[...] = comb_ref[0:2, :]
        slots = lax.broadcasted_iota(jnp.int32, (CAP, tile), 0)
        select = jnp.where(slots == ranks_ref[0:1, :], 1.0, 0.0).astype(BF16)
        gtok_ref[...] = dot_f32(select, fin_ref[...], ((0,), (0,))).astype(BF16)

    cols = lambda n: pl.BlockSpec((n, tile), lambda i: (0, i))
    rows = lambda n, m: pl.BlockSpec((n, m), lambda i: (i, 0))
    return pl.pallas_call(
        body,
        grid=(steps,),
        out_shape=(
            jax.ShapeDtypeStruct((total, SUB), BF16),
            jax.ShapeDtypeStruct((2, total), F32),
            jax.ShapeDtypeStruct((own * 8, PART), F32),
            jax.ShapeDtypeStruct((own, 4 * PART), F32),
        ),
        in_specs=[
            cols(8),
            pl.BlockSpec(fin.shape, lambda i: (0, 0)),
            cols(8),
            pl.BlockSpec((12, deep, PART), lambda i: (0, i, 0)),
        ],
        out_specs=[rows(tile, SUB), cols(2), rows(deep * 8, PART), rows(deep, 4 * PART)],
        cost_estimate=pl.CostEstimate(flops=2 * total * CAP * SUB, bytes_accessed=12 << 20, transcendentals=0),
    )(ranks, fin, combine, sums)


def exchange_and_compute(tokens, cotangent, gate_up, down_w, router, choice):
    own = down_w.shape[0]
    rows_all = 4 * CAP
    vm = pltpu.VMEM
    piece = (CAP, SUB)
    flops = 2 * rows_all * 2 * own * 4 * SUB * 8 // 3
    return pl.pallas_call(
        kernel,
        out_shape=(
            jax.ShapeDtypeStruct(piece, BF16),
            jax.ShapeDtypeStruct((8, tokens.shape[0]), F32),
            jax.ShapeDtypeStruct((8, tokens.shape[0]), jnp.int32),
            jax.ShapeDtypeStruct((12, own, PART), F32),
        ),
        in_specs=[pl.BlockSpec(memory_space=vm)] * 6,
        out_specs=[pl.BlockSpec(memory_space=pl.ANY)] * 4,
        scratch_shapes=[
            vm((CAP, tokens.shape[0]), BF16),
            vm((2,) + piece, BF16),
            vm((2, rows_all, 2 * own), BF16),
            vm((4, 2 * own, SUB), BF16),
            vm((3, 4) + piece, BF16),
            vm((4,) + piece, F32),
            vm((4,) + piece, BF16),
            vm((2, 4) + piece, BF16),
            vm((4, 8, 512), F32),
            vm((3, 8, 512), F32),
            vm((512, PART), F32),
            vm((512, PART), F32),
            vm((4, rows_all, SUB), BF16),
            vm((4, own, SUB), BF16),
            vm((4, own, SUB), BF16),
            vm((4, 2) + piece, BF16),
            vm((8,) + piece, BF16),
            vm((2,) + piece, BF16),
            vm((2, 2) + piece, BF16),
            vm((2,) + piece, BF16),
            vm((2,) + piece, BF16),
            vm(piece, BF16),
            vm((3, 8, 512), F32),
            vm((5, 8, 512), F32),
            vm((16, 512), F32),
            vm((8, tokens.shape[0]), jnp.int32),
            vm((16, PART), F32),
            vm((8, tokens.shape[0]), F32),
            vm((12, own, PART), F32),
            pltpu.SemaphoreType.DMA((192,)),
            pltpu.SemaphoreType.DMA((192,)),
            pltpu.SemaphoreType.DMA((12,)),
        ],
        cost_estimate=pl.CostEstimate(flops=flops, bytes_accessed=20 << 20, transcendentals=CAP * 512),
        compiler_params=pltpu.CompilerParams(
            collective_id=0, has_side_effects=True, vmem_limit_bytes=67043328
        ),
    )(tokens, cotangent, gate_up, down_w, router, choice)


def local(tokens, cotangent, expert_choice, router, gate_up, w_down):
    own, hid = w_down.shape
    fin, combine, ranks, sums = exchange_and_compute(
        tokens, cotangent, gate_up, w_down, router, expert_choice.T
    )
    grad_tokens, combine, d_gu, d_down = finish(ranks, fin, combine, sums)
    d_gate_up = d_gu.reshape(own, hid // PART, 2, PART).transpose(0, 2, 1, 3).reshape(own, 2, hid)
    return (grad_tokens, combine.T, d_gate_up, d_down)


def solution(mesh):
    split = Mesh(mesh.devices.reshape(4, 2, 2, 4, 2), ALL)
    return jax.shard_map(
        local,
        mesh=split,
        in_specs=(
            P(TOK, HID),
            P(TOK, HID),
            P(TOK, None),
            P(),
            P(TOK, None, HID),
            P(TOK, HID),
        ),
        out_specs=(P(TOK, HID), P(TOK, None), P(TOK, None, HID), P(TOK, HID)),
        check_vma=False,
    )
```

```python
import jax
import jax.numpy as jnp
from jax import lax
from jax.experimental import pallas as pl
from jax.experimental.pallas import tpu as pltpu
from jax.sharding import Mesh
from jax.sharding import PartitionSpec as P

CAP = 432
SUB = 384
PART = 128
TOK = ("y", "zl")
HID = ("zh", "x", "c")
ALL = TOK + HID
MESH = pl.DeviceIdType.MESH
F32 = jnp.float32
BF16 = jnp.bfloat16


def dot_f32(left, right, dims):
    return lax.dot_general(left, right, ((dims[0], dims[1]), ((), ())), preferred_element_type=F32)


P0, PN = (0, 224), (224, 208)
Q0, QN = (0, 112, 224, 336), (112, 112, 112, 96)
RS_KINDS = ("far_r", "far_l", "nr_raw", "nl_raw", "nr_rel", "nl_rel")
AG_KINDS = ("own_r0", "own_l1", "own_r1", "own_l0", "fwd_r", "fwd_l")


def kernel(
    tokens, cotangent, gate_up, down_w, router, choice,
    fin_out, comb_out, rank_out, acc_out,
    select, xin, rows, wgt, psend, pown, prelay, precv, lsend, lrecv, gate, sacc, mids,
    gsend, grecv, bown, brecv, xrelay, xrecv, fsend, fin2, fin, srow, srecv, labels, meta, flags, comb, acc,
    ssem, rsem, osem,
):
    y, zl, zh, x, c = (lax.axis_index(a) for a in ALL)
    yr, yl, yo = (y + 1) % 4, (y + 3) % 4, (y + 2) % 4
    xr, xl, xo = (x + 1) % 4, (x + 3) % 4, (x + 2) % 4
    D = rows.shape[2]
    own = D // 2
    swap_y, swap_zh, swap_x = 2 * zh + x // 2, y // 2, 2 * (y % 2) + x % 2
    fixed = swap_y == y
    moves = jnp.logical_not(fixed)
    swap = dict(y=swap_y, zh=swap_zh, x=swap_x)

    number = {}
    started = []

    def index(key, n=1):
        if key not in number:
            number[key] = number.get("next", 0)
            number["next"] = number[key] + n
        return number[key]

    def copy_at(i, src, dst, **to):
        return pltpu.make_async_remote_copy(
            src_ref=src, dst_ref=dst, send_sem=ssem.at[i], recv_sem=rsem.at[i],
            device_id=to, device_id_type=MESH,
        )

    def copy(key, src, dst, **to):
        return copy_at(index(key), src, dst, **to)

    def start(cp):
        cp.start()
        started.append(cp)
        return cp

    barrier = pltpu.get_barrier_semaphore()
    peers = (
        dict(y=yr), dict(y=yl), dict(y=yo), dict(zl=1 - zl), dict(zh=1 - zh),
        dict(x=xr), dict(x=xl), dict(x=xo), dict(c=1 - c),
        dict(y=2 * (1 - zh) + x // 2, zh=swap_zh, x=swap_x), dict(y=swap_y, zh=1 - swap_zh, x=swap_x),
    )
    for peer in peers:
        pl.semaphore_signal(barrier, inc=1, device_id=peer, device_id_type=MESH)

    @pl.when(moves)
    def _():
        pl.semaphore_signal(barrier, inc=1, device_id=swap, device_id_type=MESH)

    def place(p, zh_, x_, c_):
        row = pl.multiple_of((2 * zh_ + x_ // 2) * CAP + P0[p], 16)
        col = pl.multiple_of((2 * (x_ % 2) + c_) * SUB, 128)
        return rows.at[:, pl.ds(row, PN[p]), pl.ds(col, SUB)]

    def weights(sub):
        at = wgt.at[sub, pl.ds(pl.multiple_of(zl * own, 16), own), :]
        return copy(("w", sub), at, at, zl=1 - zl)

    def part(p):
        return pl.ds(P0[p], PN[p])

    def quarter(q):
        return pl.ds(Q0[q], QN[q])

    def move(p):
        return copy(("move", p), xin.at[:, part(p), :], place(p, swap_zh, swap_x, c), **swap)

    total = tokens.shape[0]
    first, second = choice[0:1, :], choice[1:2, :]
    routed = jnp.logical_or(first == 0, second == 0)
    hits = jnp.where(routed, 1.0, 0.0)
    flags[...] = jnp.zeros_like(flags)
    for i in range(total // PART):
        flags[i : i + 1, :] = hits[:, PART * i : PART * (i + 1)]
    lane = lax.broadcasted_iota(jnp.int32, (PART, PART), 0)
    before = jnp.where(lane < lax.broadcasted_iota(jnp.int32, (PART, PART), 1), 1.0, 0.0)
    line = lax.broadcasted_iota(jnp.int32, (16, 16), 0)
    above = jnp.where(line > lax.broadcasted_iota(jnp.int32, (16, 16), 1), 1.0, 0.0)
    marks = flags[...].astype(BF16)
    within = dot_f32(marks, before.astype(BF16), ((1,), (0,)))
    counts = dot_f32(marks, jnp.ones((PART, PART), BF16), ((1,), (0,)))
    flags[...] = within + dot_f32(above.astype(BF16), counts.astype(BF16), ((1,), (0,)))
    for i in range(total // PART):
        at = slice(PART * i, PART * (i + 1))
        rank = flags[i : i + 1, :].astype(jnp.int32)
        meta[0:1, at] = jnp.where(routed[:, at], rank, -1)
    meta[1:2, :] = first + second + 1
    meta[2:3, :] = jnp.where(first == 0, 1, 0)
    meta[3:4, :] = jnp.where(second == 0, 1, 0)
    meta[4:8, :] = jnp.zeros((4, total), jnp.int32)
    leave = []

    def put_out(src, dst):
        cp = pltpu.make_async_copy(src, dst, osem.at[len(leave)])
        cp.start()
        leave.append(cp)

    put_out(meta, rank_out)

    def dispatch(p):
        slots = lax.broadcasted_iota(jnp.int32, (PN[p], total), 0) + P0[p]
        select[part(p), :] = jnp.where(slots == meta[0:1, :], 1.0, 0.0).astype(BF16)
        xin[0, part(p), :] = dot_f32(select[part(p), :], tokens[...], ((1,), (0,))).astype(BF16)
        xin[1, part(p), :] = dot_f32(select[part(p), :], cotangent[...], ((1,), (0,))).astype(BF16)

    def send(p):
        @pl.when(fixed)
        def _():
            place(p, zh, x, c)[...] = xin[:, part(p), :]

        @pl.when(moves)
        def _():
            move(p).start()

    dispatch(0)

    @pl.when(moves)
    def _():
        pl.semaphore_wait(barrier, len(peers) + 1)

    @pl.when(fixed)
    def _():
        pl.semaphore_wait(barrier, len(peers))

    send(0)
    dispatch(1)
    send(1)

    def put_weights(i, carry):
        at = pl.ds(pl.multiple_of(zl * own + i * 96, 16), 96)
        of = pl.ds(pl.multiple_of(i * 96, 16), 96)
        for sub in range(4):
            cut = slice(PART * sub, PART * (sub + 1))
            wgt[sub, at, :PART] = gate_up[of, 0, cut]
            wgt[sub, at, PART : 2 * PART] = gate_up[of, 1, cut]
            wgt[sub, at, 2 * PART :] = down_w[of, cut]
        return carry

    lax.fori_loop(0, own // 96, put_weights, 0)
    named = jnp.broadcast_to(meta[1:2, :].astype(F32).astype(BF16), (16, tokens.shape[0]))
    labels[:, :CAP] = dot_f32(named, select[...], ((1,), (1,)))

    steps = {
        "zh": (lambda p: place(p, zh, x, c), dict(zh=1 - zh)),
        "xr0": (lambda p: place(p, zh, x, c), dict(x=xr)),
        "xl0": (lambda p: place(p, zh, x, c), dict(x=xl)),
        "xro": (lambda p: place(p, zh, xl, c), dict(x=xr)),
        "xr1": (lambda p: place(p, 1 - zh, x, c), dict(x=xr)),
        "xl1": (lambda p: place(p, 1 - zh, x, c), dict(x=xl)),
        "xlo": (lambda p: place(p, 1 - zh, xr, c), dict(x=xl)),
        "c_own": (lambda p: place(p, zh, x, c), dict(c=1 - c)),
        "c_zh": (lambda p: place(p, 1 - zh, x, c), dict(c=1 - c)),
        "c_xr0": (lambda p: place(p, zh, xl, c), dict(c=1 - c)),
        "c_xl0": (lambda p: place(p, zh, xr, c), dict(c=1 - c)),
        "c_xr1": (lambda p: place(p, 1 - zh, xl, c), dict(c=1 - c)),
        "c_xl1": (lambda p: place(p, 1 - zh, xr, c), dict(c=1 - c)),
        "c_xro": (lambda p: place(p, zh, xo, c), dict(c=1 - c)),
        "c_xlo": (lambda p: place(p, 1 - zh, xo, c), dict(c=1 - c)),
    }

    def hop(name, p):
        at, to = steps[name]
        return copy((name, p), at(p), at(p), **to)

    def arrive(name, p, *then):
        hop(name, p).wait_recv()
        for follow in then:
            start(hop(follow, p))

    def all_cores(p):
        for name in steps:
            if name.startswith("c_"):
                hop(name, p).wait_recv()

    for p in range(2):

        @pl.when(moves)
        def _():
            move(p).wait_recv()

        for name in ("zh", "xr0", "xl0", "c_own"):
            start(hop(name, p))
    for sub in range(4):
        start(weights(sub))

    rs_base = index("rs", 48)
    ag_base = index("ag", 48)

    def rs(kind, p, s):
        q = 2 * p + (kind in ("far_l", "nr_raw", "nl_rel"))
        at = quarter(q)
        src, dst, to = {
            "fa": lambda: (psend.at[0, s, at, :], prelay.at[s, at, :], yr if kind == "far_r" else yl),
            "nr": lambda: (psend.at[1, s, at, :], precv.at[0, s, at, :], yr),
            "nl": lambda: (psend.at[2, s, at, :], precv.at[1, s, at, :], yl),
        }[kind[:2]]()
        return copy_at(rs_base + (p * 4 + s) * 6 + RS_KINDS.index(kind), src, dst, y=to)

    def logit(r):
        to = (yo, yr, yl)[r]
        return copy(("lg", r), lsend.at[r], lrecv.at[r], y=to)

    def pre_send(p, s):
        for kind in RS_KINDS[:4]:
            rs(kind, p, s).start()

    def pre(p, s, held=False):
        def one(n, carry):
            r = jnp.where(n == 0, 2, jnp.where(n == 1, 1, jnp.where(n == 2, 3, 0)))
            t = (y + r) % 4
            at = pl.ds(pl.multiple_of(t * CAP + P0[p], 16), PN[p])
            g = dot_f32(rows[0, at, :], wgt[s, :, : 2 * PART], ((1,), (0,)))
            d = dot_f32(rows[1, at, :], wgt[s, :, 2 * PART :], ((1,), (0,)))

            @pl.when(n < 3)
            def _():
                psend[n, s, part(p), : 2 * PART] = g.astype(BF16)
                psend[n, s, part(p), 2 * PART :] = d.astype(BF16)

            @pl.when(n == 3)
            def _():
                pown[s, part(p), : 2 * PART] = g
                pown[s, part(p), 2 * PART :] = d

            for m, kinds in () if held else ((0, ("far_r", "far_l")), (1, ("nr_raw",)), (2, ("nl_raw",))):

                @pl.when(n == m)
                def _():
                    for kind in kinds:
                        rs(kind, p, s).start()

            return carry

        lax.fori_loop(0, 4, one, 0)

    def logits():
        cols = router[:, pl.ds(pl.multiple_of(y * D, 128), D)]

        def one(n, carry):
            t = (y + jnp.where(n == 0, 2, jnp.where(n == 1, 1, jnp.where(n == 2, 3, 0)))) % 4
            at = pl.ds(pl.multiple_of(t * CAP, 16), CAP)
            lsend[n, :, :CAP] = dot_f32(cols, rows[0, at, :], ((1,), (1,)))
            return carry

        lax.fori_loop(0, 4, one, 0)
        for r in range(3):
            start(logit(r))

    def relay(p, s):
        for side, slot, rel in (("far_r", 1, "nr_rel"), ("far_l", 2, "nl_rel")):
            at = quarter(2 * p + (side == "far_l"))
            rs(side, p, s).wait_recv()
            total = psend[slot, s, at, :].astype(F32) + prelay[s, at, :].astype(F32)
            psend[slot, s, at, :] = total.astype(BF16)
            rs(rel, p, s).start()

    def gates():
        for r in range(3):
            logit(r).wait_recv()
        total = (lsend[3] + lrecv[0]) + (lrecv[1] + lrecv[2])
        label = labels[:8] - 1.0
        experts = lax.broadcasted_iota(jnp.int32, (8, 512), 0).astype(F32)
        picked = jnp.sum(jnp.where(label == experts, total, 0.0), axis=0, keepdims=True)
        margin = total[:1] - picked
        row = jnp.where(label[:1] > -0.5, jax.nn.sigmoid(margin), 0.0)
        gate[...] = jnp.transpose(jnp.broadcast_to(row, (PART, 512)))
        sacc[...] = jnp.zeros_like(sacc)

    def ag(kind, p, s):
        q = 2 * p + (kind in ("own_r1", "own_l1", "fwd_l"))
        t = {"own": y, "fwd": yl if kind == "fwd_r" else yr}[kind[:3]]
        to = yr if kind[4] == "r" else yl
        at = mids.at[s, pl.ds(pl.multiple_of(t * CAP + Q0[q], 16), QN[q]), :]
        return copy_at(ag_base + (p * 4 + s) * 6 + AG_KINDS.index(kind), at, at, y=to)

    def pointwise(p, s):
        for kind in RS_KINDS[2:]:
            rs(kind, p, s).wait_recv()
        for q in (2 * p, 2 * p + 1):
            at = quarter(q)
            near = precv[0, s, at, :].astype(F32) + precv[1, s, at, :].astype(F32)
            now = pown[s, at, :] + near
            g, up, raw = now[:, :PART], now[:, PART : 2 * PART], now[:, 2 * PART :]
            sigma = jax.nn.sigmoid(g)
            active = g * sigma
            slope = sigma * (1.0 + g * (1.0 - sigma))
            product = active * up
            scale = gate[at, :]
            sacc[at, :] += product * raw
            upstream = scale * raw
            to = pl.ds(pl.multiple_of(y * CAP + Q0[q], 16), QN[q])
            mids[s, to, :PART] = (upstream * up * slope).astype(BF16)
            mids[s, to, PART : 2 * PART] = (upstream * active).astype(BF16)
            mids[s, to, 2 * PART :] = (scale * product).astype(BF16)
        for kind in AG_KINDS[:4]:
            ag(kind, p, s).start()

    def forward(p, s):
        for kind, fwd in (("own_r0", "fwd_r"), ("own_l1", "fwd_l")):
            ag(kind, p, s).wait_recv()
            ag(fwd, p, s).start()

    def near(p, s):
        ag("own_r1", p, s).wait_recv()
        ag("own_l0", p, s).wait_recv()

    def far(p, s):
        ag("fwd_r", p, s).wait_recv()
        ag("fwd_l", p, s).wait_recv()

    def exchange(s, half=None):
        at = pl.ds(0, own) if half is None else pl.ds(half * (own // 4), own // 4)
        return copy(("gz", s, half), gsend.at[s, at, :], grecv.at[s, at, :], zl=1 - zl)

    def grads_tile(s, at):
        gu = dot_f32(rows[0, :, pl.ds(at, 256)], mids[s, :, : 2 * PART], ((0,), (0,)))
        return gu, dot_f32(rows[1, :, pl.ds(at, 256)], mids[s, :, 2 * PART :], ((0,), (0,)))

    def grads_theirs(s):
        def one(i, carry):
            gu, d = grads_tile(s, pl.multiple_of((1 - zl) * own + i * 256, 256))
            to = pl.ds(pl.multiple_of(i * 256, 256), 256)
            gsend[s, to, : 2 * PART] = gu.astype(BF16)
            gsend[s, to, 2 * PART :] = d.astype(BF16)
            return carry

        lax.fori_loop(0, own // 256, one, 0)

    def grads_mine(s):
        def one(i, carry):
            gu, d = grads_tile(s, pl.multiple_of(zl * own + i * 256, 256))
            to = pl.ds(pl.multiple_of(i * 256, 256), 256)
            for g in range(2):
                acc[3 * s + g, to, :] = gu[:, PART * g : PART * (g + 1)]
            acc[3 * s + 2, to, :] = d
            return carry

        lax.fori_loop(0, own // 256, one, 0)

    def add_grads(s, half=None):
        exchange(s, half).wait_recv()

        def one(i, carry):
            at = pl.ds(pl.multiple_of(i * 64, 16), 64)
            got = grecv[s, at, :].astype(F32)
            for g in range(3):
                acc[3 * s + g, at, :] += got[:, PART * g : PART * (g + 1)]
            return carry

        count = own // 64
        if half is None:
            lax.fori_loop(0, count, one, 0)
        else:
            lax.fori_loop(half * (count // 4), (half + 1) * (count // 4), one, 0)
        at = pl.ds(0, own) if half is None else pl.ds(half * (own // 4), own // 4)
        put_out(acc.at[pl.ds(3 * s, 3), at, :], acc_out.at[pl.ds(3 * s, 3), at, :])

    def score(key):
        src, dst, to = {
            "c": (0, 0, dict(c=1 - c)), "zh": (1, 1, dict(zh=1 - zh)),
            "x0": (2, 2, dict(x=xr)), "x1": (2, 3, dict(x=xl)), "x2": (2, 4, dict(x=xo)),
        }[key]
        return copy(("sc", key), srow.at[src], srecv.at[dst], **to)

    def scores():
        summed = jnp.sum(jnp.transpose(sacc[...]), axis=0, keepdims=True)
        srow[0] = jnp.broadcast_to(summed, (8, 512))
        start(score("c"))

    def scores_zh():
        score("c").wait_recv()
        srow[1] = srow[0] + srecv[0]
        start(score("zh"))

    def scores_x():
        score("zh").wait_recv()
        srow[2] = srow[1] + srecv[1]
        for key in ("x0", "x1", "x2"):
            start(score(key))

    def scores_end():
        for key in ("x0", "x1", "x2"):
            score(key).wait_recv()
        exact = ((srow[2] + srecv[2]) + (srecv[3] + srecv[4]))[0:1, :CAP]
        high = exact.astype(BF16).astype(F32)
        middle = (exact - high).astype(BF16).astype(F32)
        at = lax.broadcasted_iota(jnp.int32, (16, CAP), 0)
        split = jnp.where(at == 0, high, jnp.where(at == 1, middle, exact - high - middle))
        split = jnp.where(at < 3, split, 0.0).astype(BF16)
        parts = dot_f32(split, select[...], ((1,), (0,)))
        value = parts[0:1] + (parts[1:2] + parts[2:3])
        column = lax.broadcasted_iota(jnp.int32, (8, total), 0)
        chosen = jnp.where(column == 0, meta[2:3, :], meta[3:4, :])
        comb[...] = jnp.where(chosen > 0, value, 0.0)
        put_out(comb, comb_out)

    pair_base = index("pair", 16)

    def pair(p, i):
        src = psend.at[i // 4, i % 4, part(p), :]
        return copy_at(pair_base + p * 8 + i, src, brecv.at[i, part(p), :], c=1 - c)

    def ring(kind, half, p):
        at = part(p)
        src, dst, to = {
            "far_r": lambda: (bown.at[xo, half, at, :], xrelay.at[0, at, :], xr),
            "far_l": lambda: (bown.at[xo, half, at, :], xrelay.at[1, at, :], xl),
            "near_r": lambda: (bown.at[xr, half, at, :], xrecv.at[0, half, at, :], xr),
            "near_l": lambda: (bown.at[xl, half, at, :], xrecv.at[1, half, at, :], xl),
        }[kind]()
        return copy(("bx", kind, half, p), src, dst, x=to)

    def home(p, near_plane):
        to = swap if near_plane else dict(y=2 * (1 - zh) + x // 2, zh=swap_zh, x=swap_x)
        src = fsend.at[0 if near_plane else 1, part(p), :]
        return copy(("home", p, near_plane), src, fin2.at[zh, part(p), :], **to)

    def owned(p):
        home(p, False).wait_recv()

        @pl.when(moves)
        def _():
            home(p, True).wait_recv()

        add_rows(p, fin, [fin2.at[0], fin2.at[1]])

    def add_rows(p, out, refs):
        for q in (2 * p, 2 * p + 1):
            at = quarter(q)
            total = refs[0][at, :].astype(F32)
            for ref in refs[1:]:
                total = total + ref[at, :].astype(F32)
            out[at, :] = total.astype(out.dtype)

    def back_blocks(*blocks):
        def one(b, carry):
            col = pl.multiple_of(b * 2 * SUB, 128)
            lines = []
            for p, t in blocks:
                at = pl.ds(pl.multiple_of(t * CAP + P0[p], 16), PN[p])
                lines.append(jnp.concatenate([mids[sub, at, : 2 * PART] for sub in range(4)], axis=1))
            m = jnp.concatenate(lines, axis=0)
            w = jnp.concatenate([wgt[sub, pl.ds(col, 2 * SUB), : 2 * PART] for sub in range(4)], axis=1)
            piece = dot_f32(m, w, ((1,), (1,)))
            low, high = piece[:, :SUB], piece[:, SUB:]
            mine = jnp.where(c == 0, low, high).astype(BF16)
            theirs = jnp.where(c == 0, high, low).astype(BF16)
            base = 0
            for p, t in blocks:
                k = t // 2
                x_ = 2 * (t % 2) + b
                i = x_ * 2 + k
                bown[x_, k, part(p), :] = mine[base : base + PN[p]]
                psend[i // 4, i % 4, part(p), :] = theirs[base : base + PN[p]]
                base += PN[p]
                pair(p, i).start()
            return carry

        lax.fori_loop(0, 2, one, 0)

    def back_sum(p, t):
        k = t // 2

        def one(b, carry):
            x_ = 2 * (t % 2) + b
            i = x_ * 2 + k
            r = (x_ - x + 4) % 4
            pair(p, i).wait_recv()
            add_rows(p, bown.at[x_, k], [bown.at[x_, k], brecv.at[i]])
            for r_, k_, kind in ((2, 0, "far_r"), (2, 1, "far_l"), (1, 1, "near_r"), (3, 0, "near_l")):

                @pl.when(jnp.logical_and(r == r_, k == k_))
                def _():
                    ring(kind, k_, p).start()

            return carry

        lax.fori_loop(0, 2, one, 0)

    def ring_relay(p):
        ring("far_r", 0, p).wait_recv()
        add_rows(p, bown.at[xr, 0], [bown.at[xr, 0], xrelay.at[0]])
        ring("near_r", 0, p).start()
        ring("far_l", 1, p).wait_recv()
        add_rows(p, bown.at[xl, 1], [bown.at[xl, 1], xrelay.at[1]])
        ring("near_l", 1, p).start()

    def ring_end(p):
        for half in range(2):
            for kind in ("near_r", "near_l"):
                ring(kind, half, p).wait_recv()
        add_rows(p, fsend.at[1], [bown.at[x, 1 - zh], xrecv.at[0, 1 - zh], xrecv.at[1, 1 - zh]])
        add_rows(p, fsend.at[0], [bown.at[x, zh], xrecv.at[0, zh], xrecv.at[1, zh]])

    def go_home(p):
        @pl.when(fixed)
        def _():
            fin2[zh, part(p), :] = fsend[0, part(p), :]

        @pl.when(moves)
        def _():
            home(p, True).start()

        home(p, False).start()

    arrive("xr0", 0, "xro", "c_xr0")
    arrive("xl0", 0, "c_xl0")
    arrive("zh", 0, "xr1", "xl1", "c_zh")
    arrive("xr0", 1, "xro", "c_xr0")
    arrive("xl0", 1, "c_xl0")
    arrive("zh", 1, "xr1", "xl1", "c_zh")
    arrive("xl1", 0, "xlo", "c_xl1")
    arrive("xro", 0, "c_xro")
    arrive("xr1", 0, "c_xr1")
    arrive("xl1", 1, "xlo", "c_xl1")
    arrive("xlo", 0, "c_xlo")
    all_cores(0)
    weights(0).wait_recv()
    pre(0, 0)
    weights(1).wait_recv()
    pre(0, 1)
    arrive("xro", 1, "c_xro")
    arrive("xr1", 1, "c_xr1")
    arrive("xlo", 1, "c_xlo")
    all_cores(1)
    pre(1, 0)
    pre(1, 1)
    logits()
    for p in range(2):
        for s in range(2):
            relay(p, s)
    gates()
    pointwise(0, 0)
    pointwise(0, 1)
    pointwise(1, 0)
    pointwise(1, 1)
    forward(0, 0)
    forward(0, 1)
    weights(2).wait_recv()
    pre(0, 2, held=True)
    forward(1, 0)
    forward(1, 1)
    pre_send(0, 2)
    weights(3).wait_recv()
    pre(0, 3)
    pre(1, 2)
    pre(1, 3)
    for p in range(2):
        near(p, 0)
        far(p, 0)
    grads_theirs(0)
    start(exchange(0))
    relay(0, 2)
    relay(0, 3)
    for p in range(2):
        near(p, 1)
        far(p, 1)
    grads_theirs(1)
    start(exchange(1))
    relay(1, 2)
    relay(1, 3)
    grads_mine(0)
    pointwise(0, 2)
    pointwise(0, 3)
    forward(0, 2)
    pointwise(1, 2)
    forward(0, 3)
    pointwise(1, 3)
    scores()
    for kind in RS_KINDS:
        for p in range(2):
            for s in range(4):
                rs(kind, p, s).wait_send()
    back_blocks((0, y), (1, y))
    scores_zh()
    for s in range(2, 4):
        near(0, s)
    back_blocks((0, yr), (0, yl))
    back_sum(0, y)
    forward(1, 2)
    back_sum(0, yr)
    back_sum(0, yl)
    for s in range(2, 4):
        far(0, s)
    back_blocks((0, yo),)
    forward(1, 3)
    back_sum(0, yo)
    near(1, 2)
    far(1, 2)
    grads_theirs(2)
    start(exchange(2))
    near(1, 3)
    back_blocks((1, yr), (1, yl))
    ring_relay(0)
    far(1, 3)
    grads_theirs(3)
    start(exchange(3))
    back_blocks((1, yo),)
    back_sum(1, y)
    back_sum(1, yr)
    back_sum(1, yl)
    back_sum(1, yo)
    scores_x()
    ring_relay(1)
    grads_mine(1)
    ring_end(0)
    ring_end(1)
    go_home(0)
    go_home(1)
    grads_mine(2)
    add_grads(0)
    add_grads(1)
    add_grads(2)
    grads_mine(3)
    scores_end()

    @pl.when(moves)
    def _():
        for p in range(2):
            move(p).wait_send()

    for kind in AG_KINDS:
        for p in range(2):
            for s in range(4):
                ag(kind, p, s).wait_send()
    for key in number:
        if key[0] == "bx":
            ring(*key[1:]).wait_send()
    for p in range(2):
        for i in range(8):
            pair(p, i).wait_send()
    for cp in started:
        cp.wait_send()
    owned(0)
    add_grads(3)
    owned(1)
    put_out(fin, fin_out)

    for p in range(2):
        home(p, False).wait_send()

    @pl.when(moves)
    def _():
        for p in range(2):
            home(p, True).wait_send()

    for cp in leave:
        cp.wait()


def finish(ranks, fin, combine, sums):
    total, own = ranks.shape[1], sums.shape[1]
    steps = 2
    tile, deep = total // steps, own // steps

    def body(ranks_ref, fin_ref, comb_ref, sums_ref, gtok_ref, comb_out, gu_out, down_out):
        for s in range(4):
            for g in range(2):
                gu_out[pl.ds(2 * s + g, deep, stride=8), :] = sums_ref[3 * s + g]
            down_out[:, PART * s : PART * (s + 1)] = sums_ref[3 * s + 2]
        comb_out[...] = comb_ref[0:2, :]
        slots = lax.broadcasted_iota(jnp.int32, (CAP, tile), 0)
        select = jnp.where(slots == ranks_ref[0:1, :], 1.0, 0.0).astype(BF16)
        gtok_ref[...] = dot_f32(select, fin_ref[...], ((0,), (0,))).astype(BF16)

    cols = lambda n: pl.BlockSpec((n, tile), lambda i: (0, i))
    rows = lambda n, m: pl.BlockSpec((n, m), lambda i: (i, 0))
    return pl.pallas_call(
        body,
        grid=(steps,),
        out_shape=(
            jax.ShapeDtypeStruct((total, SUB), BF16),
            jax.ShapeDtypeStruct((2, total), F32),
            jax.ShapeDtypeStruct((own * 8, PART), F32),
            jax.ShapeDtypeStruct((own, 4 * PART), F32),
        ),
        in_specs=[
            cols(8),
            pl.BlockSpec(fin.shape, lambda i: (0, 0)),
            cols(8),
            pl.BlockSpec((12, deep, PART), lambda i: (0, i, 0)),
        ],
        out_specs=[rows(tile, SUB), cols(2), rows(deep * 8, PART), rows(deep, 4 * PART)],
        cost_estimate=pl.CostEstimate(flops=2 * total * CAP * SUB, bytes_accessed=12 << 20, transcendentals=0),
    )(ranks, fin, combine, sums)


def exchange_and_compute(tokens, cotangent, gate_up, down_w, router, choice):
    own = down_w.shape[0]
    rows_all = 4 * CAP
    vm = pltpu.VMEM
    piece = (CAP, SUB)
    flops = 2 * rows_all * 2 * own * 4 * SUB * 8 // 3
    return pl.pallas_call(
        kernel,
        out_shape=(
            jax.ShapeDtypeStruct(piece, BF16),
            jax.ShapeDtypeStruct((8, tokens.shape[0]), F32),
            jax.ShapeDtypeStruct((8, tokens.shape[0]), jnp.int32),
            jax.ShapeDtypeStruct((12, own, PART), F32),
        ),
        in_specs=[pl.BlockSpec(memory_space=vm)] * 6,
        out_specs=[pl.BlockSpec(memory_space=pl.ANY)] * 4,
        scratch_shapes=[
            vm((CAP, tokens.shape[0]), BF16),
            vm((2,) + piece, BF16),
            vm((2, rows_all, 2 * own), BF16),
            vm((4, 2 * own, SUB), BF16),
            vm((3, 4) + piece, BF16),
            vm((4,) + piece, F32),
            vm((4,) + piece, BF16),
            vm((2, 4) + piece, BF16),
            vm((4, 8, 512), F32),
            vm((3, 8, 512), F32),
            vm((512, PART), F32),
            vm((512, PART), F32),
            vm((4, rows_all, SUB), BF16),
            vm((4, own, SUB), BF16),
            vm((4, own, SUB), BF16),
            vm((4, 2) + piece, BF16),
            vm((8,) + piece, BF16),
            vm((2,) + piece, BF16),
            vm((2, 2) + piece, BF16),
            vm((2,) + piece, BF16),
            vm((2,) + piece, BF16),
            vm(piece, BF16),
            vm((3, 8, 512), F32),
            vm((5, 8, 512), F32),
            vm((16, 512), F32),
            vm((8, tokens.shape[0]), jnp.int32),
            vm((16, PART), F32),
            vm((8, tokens.shape[0]), F32),
            vm((12, own, PART), F32),
            pltpu.SemaphoreType.DMA((192,)),
            pltpu.SemaphoreType.DMA((192,)),
            pltpu.SemaphoreType.DMA((12,)),
        ],
        cost_estimate=pl.CostEstimate(flops=flops, bytes_accessed=20 << 20, transcendentals=CAP * 512),
        compiler_params=pltpu.CompilerParams(
            collective_id=0, has_side_effects=True, vmem_limit_bytes=67043328
        ),
    )(tokens, cotangent, gate_up, down_w, router, choice)


def local(tokens, cotangent, expert_choice, router, gate_up, w_down):
    own, hid = w_down.shape
    fin, combine, ranks, sums = exchange_and_compute(
        tokens, cotangent, gate_up, w_down, router, expert_choice.T
    )
    grad_tokens, combine, d_gu, d_down = finish(ranks, fin, combine, sums)
    d_gate_up = d_gu.reshape(own, hid // PART, 2, PART).transpose(0, 2, 1, 3).reshape(own, 2, hid)
    return (grad_tokens, combine.T, d_gate_up, d_down)


def solution(mesh):
    split = Mesh(mesh.devices.reshape(4, 2, 2, 4, 2), ALL)
    return jax.shard_map(
        local,
        mesh=split,
        in_specs=(
            P(TOK, HID),
            P(TOK, HID),
            P(TOK, None),
            P(),
            P(TOK, None, HID),
            P(TOK, HID),
        ),
        out_specs=(P(TOK, HID), P(TOK, None), P(TOK, None, HID), P(TOK, HID)),
        check_vma=False,
    )
```

```python
import jax
import jax.numpy as jnp
from jax import lax
from jax.experimental import pallas as pl
from jax.experimental.pallas import tpu as pltpu
from jax.sharding import Mesh
from jax.sharding import PartitionSpec as P

CAP = 432
SUB = 384
PART = 128
TOK = ("y", "zl")
HID = ("zh", "x", "c")
ALL = TOK + HID
MESH = pl.DeviceIdType.MESH
F32 = jnp.float32
BF16 = jnp.bfloat16


def dot_f32(left, right, dims):
    return lax.dot_general(left, right, ((dims[0], dims[1]), ((), ())), preferred_element_type=F32)


P0, PN = (0, 224), (224, 208)
Q0, QN = (0, 112, 224, 336), (112, 112, 112, 96)
RS_KINDS = ("far_r", "far_l", "nr_raw", "nl_raw", "nr_rel", "nl_rel")
AG_KINDS = ("own_r0", "own_l1", "own_r1", "own_l0", "fwd_r", "fwd_l")


def kernel(
    tokens, cotangent, gate_up, down_w, router, choice,
    fin_out, comb_out, rank_out, acc_out,
    select, xin, rows, wgt, psend, pown, prelay, precv, lsend, lrecv, gate, sacc, mids,
    gsend, grecv, bown, brecv, xrelay, xrecv, fsend, fin2, fin, srow, srecv, labels, meta, flags, comb, acc,
    ssem, rsem, osem,
):
    y, zl, zh, x, c = (lax.axis_index(a) for a in ALL)
    yr, yl, yo = (y + 1) % 4, (y + 3) % 4, (y + 2) % 4
    xr, xl, xo = (x + 1) % 4, (x + 3) % 4, (x + 2) % 4
    D = rows.shape[2]
    own = D // 2
    swap_y, swap_zh, swap_x = 2 * zh + x // 2, y // 2, 2 * (y % 2) + x % 2
    fixed = swap_y == y
    moves = jnp.logical_not(fixed)
    swap = dict(y=swap_y, zh=swap_zh, x=swap_x)

    number = {}
    started = []

    def index(key, n=1):
        if key not in number:
            number[key] = number.get("next", 0)
            number["next"] = number[key] + n
        return number[key]

    def copy_at(i, src, dst, **to):
        return pltpu.make_async_remote_copy(
            src_ref=src, dst_ref=dst, send_sem=ssem.at[i], recv_sem=rsem.at[i],
            device_id=to, device_id_type=MESH,
        )

    def copy(key, src, dst, **to):
        return copy_at(index(key), src, dst, **to)

    def start(cp):
        cp.start()
        started.append(cp)
        return cp

    barrier = pltpu.get_barrier_semaphore()
    peers = (
        dict(y=yr), dict(y=yl), dict(y=yo), dict(zl=1 - zl), dict(zh=1 - zh),
        dict(x=xr), dict(x=xl), dict(x=xo), dict(c=1 - c),
        dict(y=2 * (1 - zh) + x // 2, zh=swap_zh, x=swap_x), dict(y=swap_y, zh=1 - swap_zh, x=swap_x),
    )
    for peer in peers:
        pl.semaphore_signal(barrier, inc=1, device_id=peer, device_id_type=MESH)

    @pl.when(moves)
    def _():
        pl.semaphore_signal(barrier, inc=1, device_id=swap, device_id_type=MESH)

    def place(p, zh_, x_, c_):
        row = pl.multiple_of((2 * zh_ + x_ // 2) * CAP + P0[p], 16)
        col = pl.multiple_of((2 * (x_ % 2) + c_) * SUB, 128)
        return rows.at[:, pl.ds(row, PN[p]), pl.ds(col, SUB)]

    def weights(sub):
        at = wgt.at[sub, pl.ds(pl.multiple_of(zl * own, 16), own), :]
        return copy(("w", sub), at, at, zl=1 - zl)

    def part(p):
        return pl.ds(P0[p], PN[p])

    def quarter(q):
        return pl.ds(Q0[q], QN[q])

    def move(p):
        return copy(("move", p), xin.at[:, part(p), :], place(p, swap_zh, swap_x, c), **swap)

    total = tokens.shape[0]
    first, second = choice[0:1, :], choice[1:2, :]
    routed = jnp.logical_or(first == 0, second == 0)
    hits = jnp.where(routed, 1.0, 0.0)
    flags[...] = jnp.zeros_like(flags)
    for i in range(total // PART):
        flags[i : i + 1, :] = hits[:, PART * i : PART * (i + 1)]
    lane = lax.broadcasted_iota(jnp.int32, (PART, PART), 0)
    before = jnp.where(lane < lax.broadcasted_iota(jnp.int32, (PART, PART), 1), 1.0, 0.0)
    line = lax.broadcasted_iota(jnp.int32, (16, 16), 0)
    above = jnp.where(line > lax.broadcasted_iota(jnp.int32, (16, 16), 1), 1.0, 0.0)
    marks = flags[...].astype(BF16)
    within = dot_f32(marks, before.astype(BF16), ((1,), (0,)))
    counts = dot_f32(marks, jnp.ones((PART, PART), BF16), ((1,), (0,)))
    flags[...] = within + dot_f32(above.astype(BF16), counts.astype(BF16), ((1,), (0,)))
    for i in range(total // PART):
        at = slice(PART * i, PART * (i + 1))
        rank = flags[i : i + 1, :].astype(jnp.int32)
        meta[0:1, at] = jnp.where(routed[:, at], rank, -1)
    meta[1:2, :] = first + second + 1
    meta[2:3, :] = jnp.where(first == 0, 1, 0)
    meta[3:4, :] = jnp.where(second == 0, 1, 0)
    meta[4:8, :] = jnp.zeros((4, total), jnp.int32)
    leave = []

    def put_out(src, dst):
        cp = pltpu.make_async_copy(src, dst, osem.at[len(leave)])
        cp.start()
        leave.append(cp)

    put_out(meta, rank_out)

    def dispatch(p):
        slots = lax.broadcasted_iota(jnp.int32, (PN[p], total), 0) + P0[p]
        select[part(p), :] = jnp.where(slots == meta[0:1, :], 1.0, 0.0).astype(BF16)
        xin[0, part(p), :] = dot_f32(select[part(p), :], tokens[...], ((1,), (0,))).astype(BF16)
        xin[1, part(p), :] = dot_f32(select[part(p), :], cotangent[...], ((1,), (0,))).astype(BF16)

    def send(p):
        @pl.when(fixed)
        def _():
            place(p, zh, x, c)[...] = xin[:, part(p), :]

        @pl.when(moves)
        def _():
            move(p).start()

    dispatch(0)

    @pl.when(moves)
    def _():
        pl.semaphore_wait(barrier, len(peers) + 1)

    @pl.when(fixed)
    def _():
        pl.semaphore_wait(barrier, len(peers))

    send(0)
    dispatch(1)
    send(1)

    def put_weights(i, carry):
        at = pl.ds(pl.multiple_of(zl * own + i * 96, 16), 96)
        of = pl.ds(pl.multiple_of(i * 96, 16), 96)
        for sub in range(4):
            cut = slice(PART * sub, PART * (sub + 1))
            wgt[sub, at, :PART] = gate_up[of, 0, cut]
            wgt[sub, at, PART : 2 * PART] = gate_up[of, 1, cut]
            wgt[sub, at, 2 * PART :] = down_w[of, cut]
        return carry

    lax.fori_loop(0, own // 96, put_weights, 0)
    named = jnp.broadcast_to(meta[1:2, :].astype(F32).astype(BF16), (16, tokens.shape[0]))
    labels[:, :CAP] = dot_f32(named, select[...], ((1,), (1,)))

    steps = {
        "zh": (lambda p: place(p, zh, x, c), dict(zh=1 - zh)),
        "xr0": (lambda p: place(p, zh, x, c), dict(x=xr)),
        "xl0": (lambda p: place(p, zh, x, c), dict(x=xl)),
        "xro": (lambda p: place(p, zh, xl, c), dict(x=xr)),
        "xr1": (lambda p: place(p, 1 - zh, x, c), dict(x=xr)),
        "xl1": (lambda p: place(p, 1 - zh, x, c), dict(x=xl)),
        "xlo": (lambda p: place(p, 1 - zh, xr, c), dict(x=xl)),
        "c_own": (lambda p: place(p, zh, x, c), dict(c=1 - c)),
        "c_zh": (lambda p: place(p, 1 - zh, x, c), dict(c=1 - c)),
        "c_xr0": (lambda p: place(p, zh, xl, c), dict(c=1 - c)),
        "c_xl0": (lambda p: place(p, zh, xr, c), dict(c=1 - c)),
        "c_xr1": (lambda p: place(p, 1 - zh, xl, c), dict(c=1 - c)),
        "c_xl1": (lambda p: place(p, 1 - zh, xr, c), dict(c=1 - c)),
        "c_xro": (lambda p: place(p, zh, xo, c), dict(c=1 - c)),
        "c_xlo": (lambda p: place(p, 1 - zh, xo, c), dict(c=1 - c)),
    }

    def hop(name, p):
        at, to = steps[name]
        return copy((name, p), at(p), at(p), **to)

    def arrive(name, p, *then):
        hop(name, p).wait_recv()
        for follow in then:
            start(hop(follow, p))

    def all_cores(p):
        for name in steps:
            if name.startswith("c_"):
                hop(name, p).wait_recv()

    for p in range(2):

        @pl.when(moves)
        def _():
            move(p).wait_recv()

        for name in ("zh", "xr0", "xl0", "c_own"):
            start(hop(name, p))
    for sub in range(4):
        start(weights(sub))

    rs_base = index("rs", 48)
    ag_base = index("ag", 48)

    def rs(kind, p, s):
        q = 2 * p + (kind in ("far_l", "nr_raw", "nl_rel"))
        at = quarter(q)
        src, dst, to = {
            "fa": lambda: (psend.at[0, s, at, :], prelay.at[s, at, :], yr if kind == "far_r" else yl),
            "nr": lambda: (psend.at[1, s, at, :], precv.at[0, s, at, :], yr),
            "nl": lambda: (psend.at[2, s, at, :], precv.at[1, s, at, :], yl),
        }[kind[:2]]()
        return copy_at(rs_base + (p * 4 + s) * 6 + RS_KINDS.index(kind), src, dst, y=to)

    def logit(r):
        to = (yo, yr, yl)[r]
        return copy(("lg", r), lsend.at[r], lrecv.at[r], y=to)

    def pre_send(p, s):
        for kind in RS_KINDS[:4]:
            rs(kind, p, s).start()

    def pre(p, s, held=False):
        def one(n, carry):
            r = jnp.where(n == 0, 2, jnp.where(n == 1, 1, jnp.where(n == 2, 3, 0)))
            t = (y + r) % 4
            at = pl.ds(pl.multiple_of(t * CAP + P0[p], 16), PN[p])
            g = dot_f32(rows[0, at, :], wgt[s, :, : 2 * PART], ((1,), (0,)))
            d = dot_f32(rows[1, at, :], wgt[s, :, 2 * PART :], ((1,), (0,)))

            @pl.when(n < 3)
            def _():
                psend[n, s, part(p), : 2 * PART] = g.astype(BF16)
                psend[n, s, part(p), 2 * PART :] = d.astype(BF16)

            @pl.when(n == 3)
            def _():
                pown[s, part(p), : 2 * PART] = g
                pown[s, part(p), 2 * PART :] = d

            for m, kinds in () if held else ((0, ("far_r", "far_l")), (1, ("nr_raw",)), (2, ("nl_raw",))):

                @pl.when(n == m)
                def _():
                    for kind in kinds:
                        rs(kind, p, s).start()

            return carry

        lax.fori_loop(0, 4, one, 0)

    def logits():
        cols = router[:, pl.ds(pl.multiple_of(y * D, 128), D)]

        def one(n, carry):
            t = (y + jnp.where(n == 0, 2, jnp.where(n == 1, 1, jnp.where(n == 2, 3, 0)))) % 4
            at = pl.ds(pl.multiple_of(t * CAP, 16), CAP)
            lsend[n, :, :CAP] = dot_f32(cols, rows[0, at, :], ((1,), (1,)))
            return carry

        lax.fori_loop(0, 4, one, 0)
        for r in range(3):
            start(logit(r))

    def relay(p, s):
        for side, slot, rel in (("far_r", 1, "nr_rel"), ("far_l", 2, "nl_rel")):
            at = quarter(2 * p + (side == "far_l"))
            rs(side, p, s).wait_recv()
            total = psend[slot, s, at, :].astype(F32) + prelay[s, at, :].astype(F32)
            psend[slot, s, at, :] = total.astype(BF16)
            rs(rel, p, s).start()

    def gates():
        for r in range(3):
            logit(r).wait_recv()
        total = (lsend[3] + lrecv[0]) + (lrecv[1] + lrecv[2])
        label = labels[:8] - 1.0
        experts = lax.broadcasted_iota(jnp.int32, (8, 512), 0).astype(F32)
        picked = jnp.sum(jnp.where(label == experts, total, 0.0), axis=0, keepdims=True)
        margin = total[:1] - picked
        row = jnp.where(label[:1] > -0.5, jax.nn.sigmoid(margin), 0.0)
        gate[...] = jnp.transpose(jnp.broadcast_to(row, (PART, 512)))
        sacc[...] = jnp.zeros_like(sacc)

    def ag(kind, p, s):
        q = 2 * p + (kind in ("own_r1", "own_l1", "fwd_l"))
        t = {"own": y, "fwd": yl if kind == "fwd_r" else yr}[kind[:3]]
        to = yr if kind[4] == "r" else yl
        at = mids.at[s, pl.ds(pl.multiple_of(t * CAP + Q0[q], 16), QN[q]), :]
        return copy_at(ag_base + (p * 4 + s) * 6 + AG_KINDS.index(kind), at, at, y=to)

    def pointwise(p, s):
        for kind in RS_KINDS[2:]:
            rs(kind, p, s).wait_recv()
        for q in (2 * p, 2 * p + 1):
            at = quarter(q)
            near = precv[0, s, at, :].astype(F32) + precv[1, s, at, :].astype(F32)
            now = pown[s, at, :] + near
            g, up, raw = now[:, :PART], now[:, PART : 2 * PART], now[:, 2 * PART :]
            sigma = jax.nn.sigmoid(g)
            active = g * sigma
            slope = sigma * (1.0 + g * (1.0 - sigma))
            product = active * up
            scale = gate[at, :]
            sacc[at, :] += product * raw
            upstream = scale * raw
            to = pl.ds(pl.multiple_of(y * CAP + Q0[q], 16), QN[q])
            mids[s, to, :PART] = (upstream * up * slope).astype(BF16)
            mids[s, to, PART : 2 * PART] = (upstream * active).astype(BF16)
            mids[s, to, 2 * PART :] = (scale * product).astype(BF16)
        for kind in AG_KINDS[:4]:
            ag(kind, p, s).start()

    def forward(p, s):
        for kind, fwd in (("own_r0", "fwd_r"), ("own_l1", "fwd_l")):
            ag(kind, p, s).wait_recv()
            ag(fwd, p, s).start()

    def near(p, s):
        ag("own_r1", p, s).wait_recv()
        ag("own_l0", p, s).wait_recv()

    def far(p, s):
        ag("fwd_r", p, s).wait_recv()
        ag("fwd_l", p, s).wait_recv()

    gz_base = index("gz", 12)

    def exchange(s, i):
        at = pl.ds(pl.multiple_of(i * 256, 256), 256)
        return copy_at(gz_base + s * 3 + i, gsend.at[s, at, :], grecv.at[s, at, :], zl=1 - zl)

    def grads_tile(s, at):
        gu = dot_f32(rows[0, :, pl.ds(at, 256)], mids[s, :, : 2 * PART], ((0,), (0,)))
        return gu, dot_f32(rows[1, :, pl.ds(at, 256)], mids[s, :, 2 * PART :], ((0,), (0,)))

    def grads_theirs(s):
        def one(i, carry):
            gu, d = grads_tile(s, pl.multiple_of((1 - zl) * own + i * 256, 256))
            to = pl.ds(pl.multiple_of(i * 256, 256), 256)
            gsend[s, to, : 2 * PART] = gu.astype(BF16)
            gsend[s, to, 2 * PART :] = d.astype(BF16)
            exchange(s, i).start()
            return carry

        lax.fori_loop(0, own // 256, one, 0)

    def grads_mine(s):
        def one(i, carry):
            gu, d = grads_tile(s, pl.multiple_of(zl * own + i * 256, 256))
            to = pl.ds(pl.multiple_of(i * 256, 256), 256)
            for g in range(2):
                acc[3 * s + g, to, :] = gu[:, PART * g : PART * (g + 1)]
            acc[3 * s + 2, to, :] = d
            return carry

        lax.fori_loop(0, own // 256, one, 0)

    def add_grads(s):
        for i in range(own // 256):
            exchange(s, i).wait_recv()

        def one(i, carry):
            at = pl.ds(pl.multiple_of(i * 64, 16), 64)
            got = grecv[s, at, :].astype(F32)
            for g in range(3):
                acc[3 * s + g, at, :] += got[:, PART * g : PART * (g + 1)]
            return carry

        lax.fori_loop(0, own // 64, one, 0)
        put_out(acc.at[pl.ds(3 * s, 3)], acc_out.at[pl.ds(3 * s, 3)])

    def score(key):
        src, dst, to = {
            "c": (0, 0, dict(c=1 - c)), "zh": (1, 1, dict(zh=1 - zh)),
            "x0": (2, 2, dict(x=xr)), "x1": (2, 3, dict(x=xl)), "x2": (2, 4, dict(x=xo)),
        }[key]
        return copy(("sc", key), srow.at[src], srecv.at[dst], **to)

    def scores():
        summed = jnp.sum(jnp.transpose(sacc[...]), axis=0, keepdims=True)
        srow[0] = jnp.broadcast_to(summed, (8, 512))
        start(score("c"))

    def scores_zh():
        score("c").wait_recv()
        srow[1] = srow[0] + srecv[0]
        start(score("zh"))

    def scores_x():
        score("zh").wait_recv()
        srow[2] = srow[1] + srecv[1]
        for key in ("x0", "x1", "x2"):
            start(score(key))

    def scores_end():
        for key in ("x0", "x1", "x2"):
            score(key).wait_recv()
        exact = ((srow[2] + srecv[2]) + (srecv[3] + srecv[4]))[0:1, :CAP]
        high = exact.astype(BF16).astype(F32)
        middle = (exact - high).astype(BF16).astype(F32)
        at = lax.broadcasted_iota(jnp.int32, (16, CAP), 0)
        split = jnp.where(at == 0, high, jnp.where(at == 1, middle, exact - high - middle))
        split = jnp.where(at < 3, split, 0.0).astype(BF16)
        parts = dot_f32(split, select[...], ((1,), (0,)))
        value = parts[0:1] + (parts[1:2] + parts[2:3])
        column = lax.broadcasted_iota(jnp.int32, (8, total), 0)
        chosen = jnp.where(column == 0, meta[2:3, :], meta[3:4, :])
        comb[...] = jnp.where(chosen > 0, value, 0.0)
        put_out(comb, comb_out)

    pair_base = index("pair", 16)

    def pair(p, i):
        src = psend.at[i // 4, i % 4, part(p), :]
        return copy_at(pair_base + p * 8 + i, src, brecv.at[i, part(p), :], c=1 - c)

    def ring(kind, half, p):
        at = part(p)
        src, dst, to = {
            "far_r": lambda: (bown.at[xo, half, at, :], xrelay.at[0, at, :], xr),
            "far_l": lambda: (bown.at[xo, half, at, :], xrelay.at[1, at, :], xl),
            "near_r": lambda: (bown.at[xr, half, at, :], xrecv.at[0, half, at, :], xr),
            "near_l": lambda: (bown.at[xl, half, at, :], xrecv.at[1, half, at, :], xl),
        }[kind]()
        return copy(("bx", kind, half, p), src, dst, x=to)

    def home(p, near_plane):
        to = swap if near_plane else dict(y=2 * (1 - zh) + x // 2, zh=swap_zh, x=swap_x)
        src = fsend.at[0 if near_plane else 1, part(p), :]
        return copy(("home", p, near_plane), src, fin2.at[zh, part(p), :], **to)

    def owned(p):
        home(p, False).wait_recv()

        @pl.when(moves)
        def _():
            home(p, True).wait_recv()

        add_rows(p, fin, [fin2.at[0], fin2.at[1]])

    def add_rows(p, out, refs):
        for q in (2 * p, 2 * p + 1):
            at = quarter(q)
            total = refs[0][at, :].astype(F32)
            for ref in refs[1:]:
                total = total + ref[at, :].astype(F32)
            out[at, :] = total.astype(out.dtype)

    def back_blocks(*blocks):
        def one(b, carry):
            col = pl.multiple_of(b * 2 * SUB, 128)
            lines = []
            for p, t in blocks:
                at = pl.ds(pl.multiple_of(t * CAP + P0[p], 16), PN[p])
                lines.append(jnp.concatenate([mids[sub, at, : 2 * PART] for sub in range(4)], axis=1))
            m = jnp.concatenate(lines, axis=0)
            w = jnp.concatenate([wgt[sub, pl.ds(col, 2 * SUB), : 2 * PART] for sub in range(4)], axis=1)
            piece = dot_f32(m, w, ((1,), (1,)))
            low, high = piece[:, :SUB], piece[:, SUB:]
            mine = jnp.where(c == 0, low, high).astype(BF16)
            theirs = jnp.where(c == 0, high, low).astype(BF16)
            base = 0
            for p, t in blocks:
                k = t // 2
                x_ = 2 * (t % 2) + b
                i = x_ * 2 + k
                bown[x_, k, part(p), :] = mine[base : base + PN[p]]
                psend[i // 4, i % 4, part(p), :] = theirs[base : base + PN[p]]
                base += PN[p]
                pair(p, i).start()
            return carry

        lax.fori_loop(0, 2, one, 0)

    def back_sum(p, t):
        k = t // 2

        def one(b, carry):
            x_ = 2 * (t % 2) + b
            i = x_ * 2 + k
            r = (x_ - x + 4) % 4
            pair(p, i).wait_recv()
            add_rows(p, bown.at[x_, k], [bown.at[x_, k], brecv.at[i]])
            for r_, k_, kind in ((2, 0, "far_r"), (2, 1, "far_l"), (1, 1, "near_r"), (3, 0, "near_l")):

                @pl.when(jnp.logical_and(r == r_, k == k_))
                def _():
                    ring(kind, k_, p).start()

            return carry

        lax.fori_loop(0, 2, one, 0)

    def ring_relay(p):
        ring("far_r", 0, p).wait_recv()
        add_rows(p, bown.at[xr, 0], [bown.at[xr, 0], xrelay.at[0]])
        ring("near_r", 0, p).start()
        ring("far_l", 1, p).wait_recv()
        add_rows(p, bown.at[xl, 1], [bown.at[xl, 1], xrelay.at[1]])
        ring("near_l", 1, p).start()

    def ring_end(p):
        for half in range(2):
            for kind in ("near_r", "near_l"):
                ring(kind, half, p).wait_recv()
        add_rows(p, fsend.at[1], [bown.at[x, 1 - zh], xrecv.at[0, 1 - zh], xrecv.at[1, 1 - zh]])
        add_rows(p, fsend.at[0], [bown.at[x, zh], xrecv.at[0, zh], xrecv.at[1, zh]])

    def go_home(p):
        @pl.when(fixed)
        def _():
            fin2[zh, part(p), :] = fsend[0, part(p), :]

        @pl.when(moves)
        def _():
            home(p, True).start()

        home(p, False).start()

    arrive("xr0", 0, "xro", "c_xr0")
    arrive("xl0", 0, "c_xl0")
    arrive("zh", 0, "xr1", "xl1", "c_zh")
    arrive("xr0", 1, "xro", "c_xr0")
    arrive("xl0", 1, "c_xl0")
    arrive("zh", 1, "xr1", "xl1", "c_zh")
    arrive("xl1", 0, "xlo", "c_xl1")
    arrive("xro", 0, "c_xro")
    arrive("xr1", 0, "c_xr1")
    arrive("xl1", 1, "xlo", "c_xl1")
    arrive("xlo", 0, "c_xlo")
    all_cores(0)
    weights(0).wait_recv()
    pre(0, 0)
    weights(1).wait_recv()
    pre(0, 1)
    arrive("xro", 1, "c_xro")
    arrive("xr1", 1, "c_xr1")
    arrive("xlo", 1, "c_xlo")
    all_cores(1)
    pre(1, 0)
    pre(1, 1)
    logits()
    for p in range(2):
        for s in range(2):
            relay(p, s)
    gates()
    pointwise(0, 0)
    pointwise(0, 1)
    pointwise(1, 0)
    pointwise(1, 1)
    forward(0, 0)
    forward(0, 1)
    weights(2).wait_recv()
    pre(0, 2, held=True)
    forward(1, 0)
    forward(1, 1)
    pre_send(0, 2)
    weights(3).wait_recv()
    pre(0, 3)
    pre(1, 2)
    pre(1, 3)
    for p in range(2):
        near(p, 0)
        far(p, 0)
    grads_theirs(0)
    relay(0, 2)
    relay(0, 3)
    for p in range(2):
        near(p, 1)
        far(p, 1)
    grads_theirs(1)
    relay(1, 2)
    relay(1, 3)
    grads_mine(0)
    pointwise(0, 2)
    pointwise(0, 3)
    forward(0, 2)
    pointwise(1, 2)
    forward(0, 3)
    pointwise(1, 3)
    scores()
    for kind in RS_KINDS:
        for p in range(2):
            for s in range(4):
                rs(kind, p, s).wait_send()
    back_blocks((0, y), (1, y))
    scores_zh()
    for s in range(2, 4):
        near(0, s)
    back_blocks((0, yr), (0, yl))
    back_sum(0, y)
    forward(1, 2)
    back_sum(0, yr)
    back_sum(0, yl)
    for s in range(2, 4):
        far(0, s)
    back_blocks((0, yo),)
    forward(1, 3)
    back_sum(0, yo)
    near(1, 2)
    far(1, 2)
    grads_theirs(2)
    near(1, 3)
    back_blocks((1, yr), (1, yl))
    ring_relay(0)
    far(1, 3)
    back_sum(1, yr)
    back_sum(1, yl)
    grads_theirs(3)
    back_sum(1, y)
    back_blocks((1, yo),)
    back_sum(1, yo)
    scores_x()
    ring_relay(1)
    grads_mine(1)
    ring_end(0)
    ring_end(1)
    go_home(0)
    go_home(1)
    grads_mine(2)
    add_grads(0)
    add_grads(1)
    add_grads(2)
    grads_mine(3)
    scores_end()

    @pl.when(moves)
    def _():
        for p in range(2):
            move(p).wait_send()

    for kind in AG_KINDS:
        for p in range(2):
            for s in range(4):
                ag(kind, p, s).wait_send()
    for key in number:
        if key[0] == "bx":
            ring(*key[1:]).wait_send()
    for p in range(2):
        for i in range(8):
            pair(p, i).wait_send()
    for s in range(4):
        for i in range(own // 256):
            exchange(s, i).wait_send()
    for cp in started:
        cp.wait_send()
    owned(0)
    add_grads(3)
    owned(1)
    put_out(fin, fin_out)

    for p in range(2):
        home(p, False).wait_send()

    @pl.when(moves)
    def _():
        for p in range(2):
            home(p, True).wait_send()

    for cp in leave:
        cp.wait()


def finish(ranks, fin, combine, sums):
    total, own = ranks.shape[1], sums.shape[1]
    steps = 2
    tile, deep = total // steps, own // steps

    def body(ranks_ref, fin_ref, comb_ref, sums_ref, gtok_ref, comb_out, gu_out, down_out):
        for s in range(4):
            for g in range(2):
                gu_out[pl.ds(2 * s + g, deep, stride=8), :] = sums_ref[3 * s + g]
            down_out[:, PART * s : PART * (s + 1)] = sums_ref[3 * s + 2]
        comb_out[...] = comb_ref[0:2, :]
        slots = lax.broadcasted_iota(jnp.int32, (CAP, tile), 0)
        select = jnp.where(slots == ranks_ref[0:1, :], 1.0, 0.0).astype(BF16)
        gtok_ref[...] = dot_f32(select, fin_ref[...], ((0,), (0,))).astype(BF16)

    cols = lambda n: pl.BlockSpec((n, tile), lambda i: (0, i))
    rows = lambda n, m: pl.BlockSpec((n, m), lambda i: (i, 0))
    return pl.pallas_call(
        body,
        grid=(steps,),
        out_shape=(
            jax.ShapeDtypeStruct((total, SUB), BF16),
            jax.ShapeDtypeStruct((2, total), F32),
            jax.ShapeDtypeStruct((own * 8, PART), F32),
            jax.ShapeDtypeStruct((own, 4 * PART), F32),
        ),
        in_specs=[
            cols(8),
            pl.BlockSpec(fin.shape, lambda i: (0, 0)),
            cols(8),
            pl.BlockSpec((12, deep, PART), lambda i: (0, i, 0)),
        ],
        out_specs=[rows(tile, SUB), cols(2), rows(deep * 8, PART), rows(deep, 4 * PART)],
        cost_estimate=pl.CostEstimate(flops=2 * total * CAP * SUB, bytes_accessed=12 << 20, transcendentals=0),
    )(ranks, fin, combine, sums)


def exchange_and_compute(tokens, cotangent, gate_up, down_w, router, choice):
    own = down_w.shape[0]
    rows_all = 4 * CAP
    vm = pltpu.VMEM
    piece = (CAP, SUB)
    flops = 2 * rows_all * 2 * own * 4 * SUB * 8 // 3
    return pl.pallas_call(
        kernel,
        out_shape=(
            jax.ShapeDtypeStruct(piece, BF16),
            jax.ShapeDtypeStruct((8, tokens.shape[0]), F32),
            jax.ShapeDtypeStruct((8, tokens.shape[0]), jnp.int32),
            jax.ShapeDtypeStruct((12, own, PART), F32),
        ),
        in_specs=[pl.BlockSpec(memory_space=vm)] * 6,
        out_specs=[pl.BlockSpec(memory_space=pl.ANY)] * 4,
        scratch_shapes=[
            vm((CAP, tokens.shape[0]), BF16),
            vm((2,) + piece, BF16),
            vm((2, rows_all, 2 * own), BF16),
            vm((4, 2 * own, SUB), BF16),
            vm((3, 4) + piece, BF16),
            vm((4,) + piece, F32),
            vm((4,) + piece, BF16),
            vm((2, 4) + piece, BF16),
            vm((4, 8, 512), F32),
            vm((3, 8, 512), F32),
            vm((512, PART), F32),
            vm((512, PART), F32),
            vm((4, rows_all, SUB), BF16),
            vm((4, own, SUB), BF16),
            vm((4, own, SUB), BF16),
            vm((4, 2) + piece, BF16),
            vm((8,) + piece, BF16),
            vm((2,) + piece, BF16),
            vm((2, 2) + piece, BF16),
            vm((2,) + piece, BF16),
            vm((2,) + piece, BF16),
            vm(piece, BF16),
            vm((3, 8, 512), F32),
            vm((5, 8, 512), F32),
            vm((16, 512), F32),
            vm((8, tokens.shape[0]), jnp.int32),
            vm((16, PART), F32),
            vm((8, tokens.shape[0]), F32),
            vm((12, own, PART), F32),
            pltpu.SemaphoreType.DMA((192,)),
            pltpu.SemaphoreType.DMA((192,)),
            pltpu.SemaphoreType.DMA((12,)),
        ],
        cost_estimate=pl.CostEstimate(flops=flops, bytes_accessed=20 << 20, transcendentals=CAP * 512),
        compiler_params=pltpu.CompilerParams(
            collective_id=0, has_side_effects=True, vmem_limit_bytes=67043328
        ),
    )(tokens, cotangent, gate_up, down_w, router, choice)


def local(tokens, cotangent, expert_choice, router, gate_up, w_down):
    own, hid = w_down.shape
    fin, combine, ranks, sums = exchange_and_compute(
        tokens, cotangent, gate_up, w_down, router, expert_choice.T
    )
    grad_tokens, combine, d_gu, d_down = finish(ranks, fin, combine, sums)
    d_gate_up = d_gu.reshape(own, hid // PART, 2, PART).transpose(0, 2, 1, 3).reshape(own, 2, hid)
    return (grad_tokens, combine.T, d_gate_up, d_down)


def solution(mesh):
    split = Mesh(mesh.devices.reshape(4, 2, 2, 4, 2), ALL)
    return jax.shard_map(
        local,
        mesh=split,
        in_specs=(
            P(TOK, HID),
            P(TOK, HID),
            P(TOK, None),
            P(),
            P(TOK, None, HID),
            P(TOK, HID),
        ),
        out_specs=(P(TOK, HID), P(TOK, None), P(TOK, None, HID), P(TOK, HID)),
        check_vma=False,
    )
```
